32 devices in a mesh: data: 32 (over z, y, x, core).
Axes of the slice: x: 2, y: 2, z: 4, core: 2. Of those that a mesh axis runs over, the one named last changes fastest.
Arguments:
- x_in: bfloat16 [256, 512, 1280], P('data')
- dy_out: bfloat16 [256, 512, 1280], P('data')
- lengths: int32 [128, 2], P('data')
- w_in: bfloat16 [1, 1280, 5120], replicated
- w_out: bfloat16 [1, 5120, 1280], replicated
Outputs:
- output 1: bfloat16 [1, 1280, 5120], replicated
- output 2: bfloat16 [1, 5120, 1280], replicated
- output 3: bfloat16 [256, 512, 1280], P('data')
All inputs are finite; a program needn't handle non-finite values.
Results may differ from the reference program's by a relative error of at most 0.0159579.
Values are sent between devices in bfloat16 or wider.
A program may use at most 1 GiB of HBM per device.

```python
import math
import jax
import jax.numpy as jnp
from jax import lax

DATA_DEVICES = 32
MICRO_STEPS = 4
BATCH_ROWS = 2
SEQ_LEN = 512
D_MODEL = 1280
D_FF = 5120
LAYERS = 1

GELU_SCALE = math.sqrt(2.0 / math.pi)
GELU_CUBIC = 0.044715


def gelu_value(pre_act):
    return 0.5 * pre_act * (1.0 + jnp.tanh(GELU_SCALE * (pre_act + GELU_CUBIC * pre_act * pre_act * pre_act)))


def gelu_slope(pre_act):
    inner = jnp.tanh(GELU_SCALE * (pre_act + GELU_CUBIC * pre_act * pre_act * pre_act))
    return 0.5 * (1.0 + inner) + 0.5 * pre_act * (1.0 - inner * inner) * GELU_SCALE * (1.0 + 3.0 * GELU_CUBIC * pre_act * pre_act)


def setup_inputs(seed: int = 0) -> dict:
    key = jax.random.key(seed)
    key_x, key_dy, key_len, key_win, key_wout = jax.random.split(key, 5)
    total_rows = DATA_DEVICES * MICRO_STEPS * BATCH_ROWS
    total_micro = DATA_DEVICES * MICRO_STEPS
    shape = (total_rows, SEQ_LEN, D_MODEL)
    x_in = jax.random.normal(key_x, shape, jnp.float32).astype(jnp.bfloat16)
    dy_out = jax.random.normal(key_dy, shape, jnp.float32).astype(jnp.bfloat16)
    lengths = jax.random.randint(key_len, (total_micro, BATCH_ROWS), 1, SEQ_LEN + 1, dtype=jnp.int32)
    lengths = lengths.at[0, 0].set(SEQ_LEN).at[total_micro - 1, BATCH_ROWS - 1].set(1)
    w_in = (jax.random.normal(key_win, (LAYERS, D_MODEL, D_FF), jnp.float32) * D_MODEL ** -0.5).astype(jnp.bfloat16)
    w_out = (jax.random.normal(key_wout, (LAYERS, D_FF, D_MODEL), jnp.float32) * (2.0 / (D_FF * LAYERS)) ** 0.5).astype(jnp.bfloat16)
    return {"x_in": x_in, "dy_out": dy_out, "lengths": lengths, "w_in": w_in, "w_out": w_out}


def microbatch_grads(x_rows, dy_rows, len_rows, w_in, w_out):
    tokens = BATCH_ROWS * SEQ_LEN
    keep = jnp.arange(SEQ_LEN)[None, :] < len_rows[:, None]
    grad = jnp.where(keep[:, :, None], dy_rows, jnp.zeros((), jnp.bfloat16)).reshape(tokens, D_MODEL)
    hidden = x_rows.reshape(tokens, D_MODEL)

    def fwd_layer(hidden_in, weights):
        w_first, w_second = weights
        pre_act = jnp.dot(hidden_in, w_first, preferred_element_type=jnp.float32).astype(jnp.bfloat16)
        act_out = gelu_value(pre_act.astype(jnp.float32)).astype(jnp.bfloat16)
        next_hidden = (hidden_in.astype(jnp.float32) + jnp.dot(act_out, w_second, preferred_element_type=jnp.float32)).astype(jnp.bfloat16)
        return next_hidden, (hidden_in, pre_act, act_out)

    saved = lax.scan(fwd_layer, hidden, (w_in, w_out))[1]

    def bwd_layer(grad_in, layer_data):
        w_first, w_second, hidden_in, pre_act, act_out = layer_data
        g_second = jnp.dot(act_out.T, grad_in, preferred_element_type=jnp.float32)
        d_act = jnp.dot(grad_in, w_second.T, preferred_element_type=jnp.float32)
        d_preact = (d_act * gelu_slope(pre_act.astype(jnp.float32))).astype(jnp.bfloat16)
        g_first = jnp.dot(hidden_in.T, d_preact, preferred_element_type=jnp.float32)
        grad_next = (grad_in.astype(jnp.float32) + jnp.dot(d_preact, w_first.T, preferred_element_type=jnp.float32)).astype(jnp.bfloat16)
        return grad_next, (g_first, g_second)

    grad_x, grads = lax.scan(bwd_layer, grad, (w_in, w_out) + saved, reverse=True)
    return grads[0], grads[1], grad_x.reshape(BATCH_ROWS, SEQ_LEN, D_MODEL)


def reference(x_in, dy_out, lengths, w_in, w_out):
    count = DATA_DEVICES * MICRO_STEPS
    x_mb = x_in.reshape(count, BATCH_ROWS, SEQ_LEN, D_MODEL)
    dy_mb = dy_out.reshape(count, BATCH_ROWS, SEQ_LEN, D_MODEL)

    def step(carry, inputs):
        acc_in, acc_out = carry
        g_in, g_out, dx_mb = microbatch_grads(inputs[0], inputs[1], inputs[2], w_in, w_out)
        return (acc_in + g_in, acc_out + g_out), dx_mb

    init = (jnp.zeros((LAYERS, D_MODEL, D_FF), jnp.float32), jnp.zeros((LAYERS, D_FF, D_MODEL), jnp.float32))
    sums, dx_all = lax.scan(step, init, (x_mb, dy_mb, lengths))
    return sums[0].astype(jnp.bfloat16), sums[1].astype(jnp.bfloat16), dx_all.reshape(x_in.shape)
```

```python
import functools
import math
import jax
import jax.numpy as jnp
from jax import lax
from jax.experimental import pallas as pl
from jax.experimental.pallas import tpu as pltpu
from jax.sharding import PartitionSpec as P

GELU_SCALE = math.sqrt(2.0 / math.pi)
GELU_CUBIC = 0.044715
MESH = pl.DeviceIdType.MESH
NT = (((1,), (1,)), ((), ()))
TN = (((0,), (0,)), ((), ()))
f32 = jnp.float32
bf16 = jnp.bfloat16
ANY = pl.BlockSpec(memory_space=pl.ANY)

CHUNK = 256
STAGES = 5
EVENT_AT = (0, 1, 3, 5, 6, 7, 8, 9, 11, 13, 15)
LAG = 4


def gelu_both(u):
    sq = u * u
    half = 0.5 + 0.5 * jnp.tanh(u * (GELU_SCALE + (GELU_SCALE * GELU_CUBIC) * sq))
    slope = half + (u * (2.0 * GELU_SCALE + (6.0 * GELU_SCALE * GELU_CUBIC) * sq)) * (half * (1.0 - half))
    return u * half, slope


def part_table(d_model):
    rows = 1024 if d_model == 1280 else d_model // 2
    cols = 768 if d_model == 1280 else d_model // 2
    return (
        (0, 0, rows, 0, CHUNK, "cxyzw"),
        (0, rows, d_model - rows, 0, CHUNK, "czxyw"),
        (1, 0, CHUNK, 0, cols, "cyxzw"),
        (1, 0, CHUNK, cols, d_model - cols, "czyxw"),
    )


def grads_kernel(dims, len_ref, x_hbm, dy_hbm, w1_hbm, w2_hbm, o1_hbm, o2_hbm, du_hbm, *scratch):
    tokens, d_model, d_ff, seq = dims
    blocks = tokens // seq
    chunks = d_ff // CHUNK
    parts = part_table(d_model)
    (x_v, g_v, w1_v, w2_v, u0, u1, d0, d1, a_v, du_v, p1, p2) = scratch[:12]
    recv = [scratch[12 + 5 * k : 17 + 5 * k] for k in range(4)]
    (x_sem, g_sem, w_sem, du_sem, own_sem, rs_send, rs_recv, ag_send, ag_recv) = scratch[32:]

    me = lax.axis_index("data")
    weight = {"c": 1, "x": 2, "y": 4, "z": 8, "w": 16}
    bit = {k: lax.rem(lax.div(me, v), 2) for k, v in weight.items()}
    peer = {k: me + v * (1 - 2 * bit[k]) for k, v in weight.items()}

    barrier = pltpu.get_barrier_semaphore()
    for k in weight:
        pl.semaphore_signal(barrier, inc=1, device_id=(peer[k],), device_id_type=MESH)
    pl.semaphore_wait(barrier, STAGES)

    region, given = [], []
    for (_, r0, nr, c0, nc, order) in parts:
        mine, away = [(r0, nr, c0, nc)], []
        for s, name in enumerate(order):
            row, rows, col, cols = mine[-1]
            if s < STAGES - 1:
                half = rows // 2
                mine.append((row + bit[name] * half, half, col, cols))
                away.append((row + (1 - bit[name]) * half, half, col, cols))
            else:
                half = cols // 2
                mine.append((row, rows, col + bit[name] * half, half))
                away.append((row, rows, col + (1 - bit[name]) * half, half))
        region.append(mine)
        given.append(away)

    def cut(r):
        row, rows, col, cols = r
        row = row if isinstance(row, int) else pl.multiple_of(row, 16)
        col = col if isinstance(col, int) else pl.multiple_of(col, 128)
        return pl.ds(row, rows), pl.ds(col, cols)

    def partial(k, i, r):
        rows, cols = cut(r)
        return (p1, p2)[parts[k][0]].at[lax.rem(i, 3), rows, cols]

    def whole(k, i, r):
        row, rows, col, cols = r
        if parts[k][0] == 0:
            return o1_hbm.at[cut((row, rows, i * CHUNK + col, cols))]
        return o2_hbm.at[cut((i * CHUNK + row, rows, col, cols))]

    def reduce_copy(k, s, i):
        slot = lax.rem(i, 2)
        return pltpu.make_async_remote_copy(
            src_ref=partial(k, i, given[k][s]), dst_ref=recv[k][s].at[slot],
            send_sem=rs_send.at[slot, s, k], recv_sem=rs_recv.at[slot, s, k],
            device_id=(peer[parts[k][5][s]],), device_id_type=MESH)

    def gather_copy(k, s, i):
        slot = lax.rem(i, 2)
        r = region[k][s + 1]
        return pltpu.make_async_remote_copy(
            src_ref=partial(k, i, r) if s == STAGES - 1 else whole(k, i, r), dst_ref=whole(k, i, r),
            send_sem=ag_send.at[slot, s, k], recv_sem=ag_recv.at[slot, s, k],
            device_id=(peer[parts[k][5][s]],), device_id_type=MESH)

    def own_copy(k, i):
        r = region[k][STAGES]
        return pltpu.make_async_copy(partial(k, i, r), whole(k, i, r), own_sem.at[k])

    def event(e, i):
        for k in range(4):
            if 1 <= e <= STAGES:
                reduce_copy(k, e - 1, i).wait()
                rows, cols = cut(region[k][e])
                ref, slot = (p1, p2)[parts[k][0]], lax.rem(i, 3)
                ref[slot, rows, cols] = ref[slot, rows, cols] + recv[k][e - 1][lax.rem(i, 2)]
            if e < STAGES:
                reduce_copy(k, e, i).start()
            if e == STAGES:
                own_copy(k, i).start()
            if e > STAGES:
                gather_copy(k, 2 * STAGES - e, i).wait()
                if e == STAGES + 1:
                    own_copy(k, i).wait()
            if STAGES <= e < 2 * STAGES:
                gather_copy(k, 2 * STAGES - 1 - e, i).start()

    def events(i, point):
        for e in reversed(range(2 * STAGES + 1)):
            if EVENT_AT[e] % 4 == point:
                j = i - EVENT_AT[e] // 4 - (1 if point == 0 else 1)

                @pl.when((j >= 0) & (j < chunks))
                def _():
                    event(e, j)

    def weights(i):
        slot = lax.rem(i, 2)
        at = pl.ds(pl.multiple_of(i * CHUNK, CHUNK), CHUNK)
        return (pltpu.make_async_copy(w1_hbm.at[:, at], w1_v.at[slot], w_sem.at[slot, 0]),
                pltpu.make_async_copy(w2_hbm.at[at, :], w2_v.at[slot], w_sem.at[slot, 1]))

    def rows_of(b):
        return pl.ds(pl.multiple_of(b * seq, seq), seq)

    def loads(b):
        return (pltpu.make_async_copy(x_hbm.at[rows_of(b), :], x_v.at[rows_of(b), :], x_sem.at[b]),
                pltpu.make_async_copy(dy_hbm.at[rows_of(b), :], g_v.at[rows_of(b), :], g_sem.at[b]))

    def arrive(b):
        for copy in loads(b):
            copy.wait()
        keep = lax.broadcasted_iota(jnp.int32, (seq, d_model), 0) < len_ref[b]
        g_v[rows_of(b), :] = jnp.where(keep, g_v[rows_of(b), :], jnp.zeros((), bf16))

    def dots(b, slot, u, d):
        u[...] = jnp.dot(x_v[rows_of(b), :], w1_v[slot], preferred_element_type=f32).astype(bf16)
        d[...] = lax.dot_general(g_v[rows_of(b), :], w2_v[slot], NT, preferred_element_type=f32)

    def pointwise(b, u, d):
        a, slope = gelu_both(u[...].astype(f32))
        a_v[rows_of(b), :] = a.astype(bf16)
        du_v[rows_of(b), :] = (d[...] * slope).astype(bf16)

    def du_out(i):
        return pltpu.make_async_copy(du_v, du_hbm.at[:, pl.ds(pl.multiple_of(i * CHUNK, CHUNK), CHUNK)], du_sem)

    for copy in weights(0):
        copy.start()
    for b in range(blocks):
        for copy in loads(b):
            copy.start()
    for copy in weights(0):
        copy.wait()
    arrive(0)
    dots(0, 0, u0, d0)

    @pl.loop(0, chunks + LAG)
    def _(i):
        busy = i < chunks
        slot = lax.rem(i, 2)

        @pl.when(i + 1 < chunks)
        def _():
            for copy in weights(i + 1):
                copy.start()

        @pl.when((i > 0) & (i <= chunks))
        def _():
            du_out(i - 1).wait()

        @pl.loop(0, 2)
        def _(half):
            @pl.when(busy)
            def _():
                @pl.loop(0, blocks // 4)
                def _(pair):
                    b = half * (blocks // 2) + pair * 2
                    last = b + 2 >= blocks

                    @pl.when(i == 0)
                    def _():
                        arrive(b + 1)

                        @pl.when(jnp.logical_not(last))
                        def _():
                            arrive(b + 2)

                    @pl.when(last & (i + 1 < chunks))
                    def _():
                        for copy in weights(i + 1):
                            copy.wait()

                    pointwise(b, u0, d0)
                    dots(b + 1, slot, u1, d1)
                    pointwise(b + 1, u1, d1)
                    dots(lax.rem(b + 2, blocks), lax.rem(slot + last.astype(jnp.int32), 2), u0, d0)

            @pl.when(half == 0)
            def _():
                events(i, 1)

            @pl.when((half == 1) & busy)
            def _():
                du_out(i).start()

        events(i, 2)
        third = lax.rem(i, 3)

        @pl.when(busy)
        def _():
            p2[third] = lax.dot_general(a_v[...], g_v[...], TN, preferred_element_type=f32).astype(bf16)

        events(i, 3)

        @pl.when(busy)
        def _():
            p1[third] = lax.dot_general(x_v[...], du_v[...], TN, preferred_element_type=f32).astype(bf16)

        events(i + 1, 0)


def grads_call(dims, lens, x, dy, w1, w2):
    tokens, d_model, d_ff, seq = dims
    scratch = [
        pltpu.VMEM((tokens, d_model), bf16), pltpu.VMEM((tokens, d_model), bf16),
        pltpu.VMEM((2, d_model, CHUNK), bf16), pltpu.VMEM((2, CHUNK, d_model), bf16),
        pltpu.VMEM((seq, CHUNK), bf16), pltpu.VMEM((seq, CHUNK), bf16),
        pltpu.VMEM((seq, CHUNK), f32), pltpu.VMEM((seq, CHUNK), f32),
        pltpu.VMEM((tokens, CHUNK), bf16), pltpu.VMEM((tokens, CHUNK), bf16),
        pltpu.VMEM((3, d_model, CHUNK), bf16), pltpu.VMEM((3, CHUNK, d_model), bf16),
    ]
    for (_, _, rows, _, cols, _) in part_table(d_model):
        for s in range(STAGES):
            last = s == STAGES - 1
            scratch.append(pltpu.VMEM((2, rows >> (4 if last else s + 1), cols // 2 if last else cols), bf16))
    dma = pltpu.SemaphoreType.DMA
    scratch += [dma((tokens // seq,)), dma((tokens // seq,)), dma((2, 2)), dma, dma((4,))]
    scratch += [dma((2, STAGES, 4))] * 4
    flops = 8 * tokens * d_model * d_ff
    return pl.pallas_call(
        functools.partial(grads_kernel, dims),
        out_shape=[jax.ShapeDtypeStruct((d_model, d_ff), bf16), jax.ShapeDtypeStruct((d_ff, d_model), bf16),
                   jax.ShapeDtypeStruct((tokens, d_ff), bf16)],
        in_specs=[pl.BlockSpec(memory_space=pltpu.SMEM)] + [ANY] * 4,
        out_specs=[ANY] * 3,
        scratch_shapes=scratch,
        compiler_params=pltpu.CompilerParams(collective_id=0, has_side_effects=True, vmem_limit_bytes=62 * 2**20),
        cost_estimate=pl.CostEstimate(flops=flops, bytes_accessed=2 * tokens * d_ff, transcendentals=tokens * d_ff),
        name="grads",
    )(lens, x, dy, w1, w2)


def finish_kernel(dims, len_ref, o1_hbm, o2_hbm, du_hbm, dy_hbm, w1_hbm, g1_hbm, g2_hbm, dx_hbm,
                  w1_v, du_v, g_v, dx_v, c1_v, c2_v, w_sem, in_sem, out_sem, c_in, c_out):
    tokens, d_model, d_ff, seq, block = dims
    steps = tokens // block
    per_seq = seq // block
    n1, n2 = d_model // steps, d_ff // steps

    def rows(b, n):
        return pl.ds(pl.multiple_of(b * n, n), n)

    def valid(b):
        return len_ref[lax.div(b, per_seq)] > lax.rem(b, per_seq) * block

    def ins(b):
        slot = lax.rem(b, 2)
        return (pltpu.make_async_copy(du_hbm.at[rows(b, block), :], du_v.at[slot], in_sem.at[slot, 0]),
                pltpu.make_async_copy(dy_hbm.at[rows(b, block), :], g_v.at[slot], in_sem.at[slot, 1]))

    def out(b):
        slot = lax.rem(b, 2)
        return pltpu.make_async_copy(dx_v.at[slot], dx_hbm.at[rows(b, block), :], out_sem.at[slot])

    def carry_in(b):
        slot = lax.rem(b, 2)
        return (pltpu.make_async_copy(o1_hbm.at[rows(b, n1), :], c1_v.at[slot], c_in.at[slot, 0]),
                pltpu.make_async_copy(o2_hbm.at[rows(b, n2), :], c2_v.at[slot], c_in.at[slot, 1]))

    def carry_out(b):
        slot = lax.rem(b, 2)
        return (pltpu.make_async_copy(c1_v.at[slot], g1_hbm.at[rows(b, n1), :], c_out.at[slot, 0]),
                pltpu.make_async_copy(c2_v.at[slot], g2_hbm.at[rows(b, n2), :], c_out.at[slot, 1]))

    def fetch(b):
        @pl.when(valid(b))
        def _():
            for copy in ins(b):
                copy.start()

    fetch(0)
    load_w = pltpu.make_async_copy(w1_hbm, w1_v, w_sem)
    load_w.start()
    for copy in carry_in(0):
        copy.start()
    load_w.wait()

    @pl.loop(0, steps)
    def _(b):
        slot = lax.rem(b, 2)

        @pl.when(b + 1 < steps)
        def _():
            fetch(b + 1)

        @pl.when(b > 0)
        def _():
            for copy in carry_out(b - 1):
                copy.wait()

        @pl.when(b + 1 < steps)
        def _():
            for copy in carry_in(b + 1):
                copy.start()

        for copy in carry_in(b):
            copy.wait()
        for copy in carry_out(b):
            copy.start()

        @pl.when(b > 1)
        def _():
            out(b - 2).wait()

        @pl.when(valid(b))
        def _():
            for copy in ins(b):
                copy.wait()
            first = lax.rem(b, per_seq) * block
            keep = first + lax.broadcasted_iota(jnp.int32, (block, d_model), 0) < len_ref[lax.div(b, per_seq)]
            g = jnp.where(keep, g_v[slot], jnp.zeros((), bf16)).astype(f32)
            dx_v[slot] = (g + lax.dot_general(du_v[slot], w1_v[...], NT, preferred_element_type=f32)).astype(bf16)

        @pl.when(jnp.logical_not(valid(b)))
        def _():
            dx_v[slot] = jnp.zeros((block, d_model), bf16)

        out(b).start()

    for copy in carry_out(steps - 1):
        copy.wait()
    out(steps - 2).wait()
    out(steps - 1).wait()


def finish_call(dims, lens, o1, o2, du, dy, w1):
    tokens, d_model, d_ff, seq, block = dims
    steps = tokens // block
    dma = pltpu.SemaphoreType.DMA
    return pl.pallas_call(
        functools.partial(finish_kernel, dims),
        out_shape=[jax.ShapeDtypeStruct((d_model, d_ff), bf16), jax.ShapeDtypeStruct((d_ff, d_model), bf16),
                   jax.ShapeDtypeStruct((tokens, d_model), bf16)],
        in_specs=[pl.BlockSpec(memory_space=pltpu.SMEM)] + [ANY] * 5,
        out_specs=[ANY] * 3,
        scratch_shapes=[
            pltpu.VMEM((d_model, d_ff), bf16), pltpu.VMEM((2, block, d_ff), bf16), pltpu.VMEM((2, block, d_model), bf16),
            pltpu.VMEM((2, block, d_model), bf16), pltpu.VMEM((2, d_model // steps, d_ff), bf16),
            pltpu.VMEM((2, d_ff // steps, d_model), bf16), dma, dma((2, 2)), dma((2,)), dma((2, 2)), dma((2, 2))],
        compiler_params=pltpu.CompilerParams(vmem_limit_bytes=62 * 2**20),
        cost_estimate=pl.CostEstimate(flops=2 * tokens * d_model * d_ff, bytes_accessed=2 * tokens * d_ff, transcendentals=0),
        name="finish",
    )(lens, o1, o2, du, dy, w1)


def solution(mesh):
    def local_step(x_loc, dy_loc, len_loc, w_in, w_out):
        layers, d_model, d_ff = w_in.shape
        rows, seq, _ = x_loc.shape
        tokens = rows * seq
        lens = len_loc.reshape(rows)
        x, dy = x_loc.reshape(tokens, d_model), dy_loc.reshape(tokens, d_model)
        w1, w2 = w_in.reshape(d_model, d_ff), w_out.reshape(d_ff, d_model)
        o1, o2, du = grads_call((tokens, d_model, d_ff, seq), lens, x, dy, w1, w2)
        g1, g2, dx = finish_call((tokens, d_model, d_ff, seq, seq // 2), lens, o1, o2, du, dy, w1)
        return g1.reshape(layers, d_model, d_ff), g2.reshape(layers, d_ff, d_model), dx.reshape(rows, seq, d_model)

    return jax.shard_map(local_step, mesh=mesh, in_specs=(P("data"), P("data"), P("data"), P(), P()), out_specs=(P(), P(), P("data")), check_vma=False)
```

```python
import functools
import math
import jax
import jax.numpy as jnp
from jax import lax
from jax.experimental import pallas as pl
from jax.experimental.pallas import tpu as pltpu
from jax.sharding import PartitionSpec as P

GELU_SCALE = math.sqrt(2.0 / math.pi)
GELU_CUBIC = 0.044715
MESH = pl.DeviceIdType.MESH
NT = (((1,), (1,)), ((), ()))
TN = (((0,), (0,)), ((), ()))
f32 = jnp.float32
bf16 = jnp.bfloat16
ANY = pl.BlockSpec(memory_space=pl.ANY)
SMEM = pl.BlockSpec(memory_space=pltpu.SMEM)

CHUNK = 256
GRANULE = 16
BLOCKS = 8
STAGES = 5
WEIGHT = {"c": 1, "x": 2, "y": 4, "z": 8, "w": 16}
EVENT_AT = (0, 1, 3, 5, 7, 9, 11, 13, 15, 17, 18)
HELD = 4


def gelu_both(u):
    sq = u * u
    half = 0.5 + 0.5 * jnp.tanh(u * (GELU_SCALE + (GELU_SCALE * GELU_CUBIC) * sq))
    slope = half + (u * (2.0 * GELU_SCALE + (6.0 * GELU_SCALE * GELU_CUBIC) * sq)) * (half * (1.0 - half))
    return u * half, slope


def part_table(d_model):
    rows = 1024 if d_model == 1280 else d_model // 2
    cols = 768 if d_model == 1280 else d_model // 2
    return (
        (0, 0, rows, 0, CHUNK, "cxyzw"),
        (0, rows, d_model - rows, 0, CHUNK, "czxyw"),
        (1, 0, CHUNK, 0, cols, "cyxzw"),
        (1, 0, CHUNK, cols, d_model - cols, "czyxw"),
    )


def place():
    me = lax.axis_index("data")
    bit = {k: lax.rem(lax.div(me, v), 2) for k, v in WEIGHT.items()}
    return me, bit, {k: me + v * (1 - 2 * bit[k]) for k, v in WEIGHT.items()}


def granules(len_ref, s):
    return lax.div(len_ref[lax.div(s, 2), lax.rem(s, 2)] + (GRANULE - 1), GRANULE)


def length(len_ref, s):
    return len_ref[lax.div(s, 2), lax.rem(s, 2)]


def most_kernel(seqs, seq, sizes, len_ref, out_ref, table_ref, mine, plane, best, depth, send, recv):
    me, bit, _ = place()

    def other(d, names):
        return me + sum(WEIGHT[k] * (1 - 2 * bit[k]) for n, k in enumerate(names) if d >> n & 1)

    counts = [granules(len_ref, s) for s in range(seqs)]
    starts = [sum(counts[:s], jnp.int32(0)) for s in range(seqs + 1)]
    mine[...] = jnp.full(mine.shape, (starts[seqs] * GRANULE).astype(f32))
    barrier = pltpu.get_barrier_semaphore()
    near = [other(d, "cxy") for d in range(1, 8)]
    far = [other(d, "zw") for d in range(1, 4)]
    for device in near + far:
        pl.semaphore_signal(barrier, inc=1, device_id=(device,), device_id_type=MESH)
    pl.semaphore_wait(barrier, len(near) + len(far))

    def exchange(source, slots, devices, first):
        copies = [pltpu.make_async_remote_copy(source, slots.at[n], send.at[first + n], recv.at[first + n], device_id=(device,), device_id_type=MESH)
                  for n, device in enumerate(devices)]
        for copy in copies:
            copy.start()
        for copy in copies:
            copy.wait()
        return functools.reduce(jnp.maximum, [slots[n] for n in range(len(devices))], source[...])

    k = lax.broadcasted_iota(jnp.int32, (2, 128), 0) * 128 + lax.broadcasted_iota(jnp.int32, (2, 128), 1)
    source, left = k, length(len_ref, 0) - k * GRANULE
    for s in range(1, seqs):
        past = k >= starts[s]
        source = jnp.where(past, k - starts[s] + s * (seq // GRANULE), source)
        left = jnp.where(past, length(len_ref, s) - (k - starts[s]) * GRANULE, left)
    inside = k < starts[seqs]
    table_ref[0:2, :] = jnp.where(inside, source, 0)
    table_ref[2:4, :] = jnp.where(inside, left, 0)
    best[...] = exchange(mine, plane, near, 0)
    largest = exchange(best, depth, far, len(near))
    out_ref[...] = sum((largest > size).astype(jnp.int32) for size in sizes[:-1])


def most_call(lens, seq, sizes):
    tile = (8, 128)
    dma = pltpu.SemaphoreType.DMA
    return pl.pallas_call(
        functools.partial(most_kernel, lens.size, seq, sizes),
        out_shape=[jax.ShapeDtypeStruct(tile, jnp.int32), jax.ShapeDtypeStruct((4, 128), jnp.int32)],
        in_specs=[SMEM],
        out_specs=[pl.BlockSpec(memory_space=pltpu.VMEM)] * 2,
        scratch_shapes=[pltpu.VMEM(tile, f32), pltpu.VMEM((7, *tile), f32), pltpu.VMEM(tile, f32), pltpu.VMEM((3, *tile), f32), dma((10,)), dma((10,))],
        compiler_params=pltpu.CompilerParams(collective_id=0, has_side_effects=True),
        name="most",
    )(lens)


def grads_kernel(dims, table_ref, x_hbm, dy_hbm, w1_hbm, w2_hbm, o1_hbm, o2_hbm, du_hbm, dx_hbm, *scratch):
    tokens, d_model, d_ff, seq, packed, dx_block = dims
    seqs = tokens // seq
    chunks = d_ff // CHUNK
    block = packed // BLOCKS
    dx_blocks = packed // dx_block
    parts = part_table(d_model)
    (x_v, g_v, w1_v, w2_v, u0, u1, d0, d1, a_v, du_v, p1, p2, dub_v, dx_v) = scratch[:14]
    recv = [scratch[14 + 5 * k : 19 + 5 * k] for k in range(4)]
    (x_sem, g_sem, w_sem, du_sem, own_sem, dub_sem, dx_sem, rs_send, rs_recv, ag_send, ag_recv) = scratch[34:]

    _, bit, peer = place()
    for s in range(seqs):
        at = pl.ds(s * seq, seq)
        pltpu.make_async_copy(x_hbm.at[at, :], x_v.at[at, :], x_sem.at[s]).start()

    barrier = pltpu.get_barrier_semaphore()
    for k in WEIGHT:
        pl.semaphore_signal(barrier, inc=1, device_id=(peer[k],), device_id_type=MESH)
    pl.semaphore_wait(barrier, STAGES)

    region, given = [], []
    for (_, r0, nr, c0, nc, order) in parts:
        mine, away = [(r0, nr, c0, nc)], []
        for s, name in enumerate(order):
            row, rows, col, cols = mine[-1]
            if s < STAGES - 1:
                half = rows // 2
                mine.append((row + bit[name] * half, half, col, cols))
                away.append((row + (1 - bit[name]) * half, half, col, cols))
            else:
                half = cols // 2
                mine.append((row, rows, col + bit[name] * half, half))
                away.append((row, rows, col + (1 - bit[name]) * half, half))
        region.append(mine)
        given.append(away)

    def cut(r):
        row, rows, col, cols = r
        row = row if isinstance(row, int) else pl.multiple_of(row, 16)
        col = col if isinstance(col, int) else pl.multiple_of(col, 128)
        return pl.ds(row, rows), pl.ds(col, cols)

    def partial(k, i, r):
        rows, cols = cut(r)
        return (p1, p2)[parts[k][0]].at[lax.rem(i, HELD), rows, cols]

    def whole(k, i, r):
        row, rows, col, cols = r
        if parts[k][0] == 0:
            return o1_hbm.at[cut((row, rows, i * CHUNK + col, cols))]
        return o2_hbm.at[cut((i * CHUNK + row, rows, col, cols))]

    def reduce_copy(k, s, i):
        slot = lax.rem(i, 2)
        return pltpu.make_async_remote_copy(
            src_ref=partial(k, i, given[k][s]), dst_ref=recv[k][s].at[slot],
            send_sem=rs_send.at[slot, s, k], recv_sem=rs_recv.at[slot, s, k],
            device_id=(peer[parts[k][5][s]],), device_id_type=MESH)

    def gather_copy(k, s, i):
        slot = lax.rem(i, 2)
        r = region[k][s + 1]
        return pltpu.make_async_remote_copy(
            src_ref=partial(k, i, r) if s == STAGES - 1 else whole(k, i, r), dst_ref=whole(k, i, r),
            send_sem=ag_send.at[slot, s, k], recv_sem=ag_recv.at[slot, s, k],
            device_id=(peer[parts[k][5][s]],), device_id_type=MESH)

    def own_copy(k, i):
        r = region[k][STAGES]
        return pltpu.make_async_copy(partial(k, i, r), whole(k, i, r), own_sem.at[k])

    def event(e, i):
        for k in range(4):
            if 1 <= e <= STAGES:
                reduce_copy(k, e - 1, i).wait()
                rows, cols = cut(region[k][e])
                ref, slot = (p1, p2)[parts[k][0]], lax.rem(i, HELD)
                ref[slot, rows, cols] = ref[slot, rows, cols] + recv[k][e - 1][lax.rem(i, 2)]
            if e < STAGES:
                reduce_copy(k, e, i).start()
            if e == STAGES:
                own_copy(k, i).start()
            if e > STAGES:
                gather_copy(k, 2 * STAGES - e, i).wait()
                if e == STAGES + 1:
                    own_copy(k, i).wait()
            if STAGES <= e < 2 * STAGES:
                gather_copy(k, 2 * STAGES - 1 - e, i).start()

    def weights(i):
        slot = lax.rem(i, 2)
        at = pl.ds(pl.multiple_of(i * CHUNK, CHUNK), CHUNK)
        return (pltpu.make_async_copy(w1_hbm.at[:, at], w1_v.at[:, at], w_sem.at[slot, 0]),
                pltpu.make_async_copy(w2_hbm.at[at, :], w2_v.at[slot], w_sem.at[slot, 1]))

    def rows_of(b):
        return pl.ds(pl.multiple_of(b * block, 16), block)

    def dots(b, i, u, d):
        w1 = w1_v[:, pl.ds(pl.multiple_of(i * CHUNK, CHUNK), CHUNK)]
        u[...] = jnp.dot(x_v[rows_of(b), :], w1, preferred_element_type=f32).astype(bf16)
        d[...] = lax.dot_general(g_v[rows_of(b), :], w2_v[lax.rem(i, 2)], NT, preferred_element_type=f32)

    def pointwise(b, u, d):
        a, slope = gelu_both(u[...].astype(f32))
        a_v[rows_of(b), :] = a.astype(bf16)
        du_v[rows_of(b), :] = (d[...] * slope).astype(bf16)

    def du_out(i):
        return pltpu.make_async_copy(du_v, du_hbm.at[:, pl.ds(pl.multiple_of(i * CHUNK, CHUNK), CHUNK)], du_sem)

    def dx_rows(q):
        return pl.ds(pl.multiple_of(q * dx_block, 16), dx_block)

    def du_in(q):
        slot = lax.rem(q, 2)
        return pltpu.make_async_copy(du_hbm.at[dx_rows(q), :], dub_v.at[slot], dub_sem.at[slot])

    def dx_out(q):
        slot = lax.rem(q, 2)
        return pltpu.make_async_copy(dx_v.at[slot], dx_hbm.at[dx_rows(q), :], dx_sem.at[slot])

    for s in range(seqs):
        at = pl.ds(s * seq, seq)
        pltpu.make_async_copy(dy_hbm.at[at, :], g_v.at[at, :], g_sem.at[s]).start()
    for copy in weights(0):
        copy.start()
    with jax.named_scope("wait_x"):
        for s in range(seqs):
            at = pl.ds(s * seq, seq)
            pltpu.make_async_copy(x_hbm.at[at, :], x_v.at[at, :], x_sem.at[s]).wait()

    @pl.loop(0, packed // GRANULE)
    def _(k):
        x_v[pl.ds(pl.multiple_of(k * GRANULE, GRANULE), GRANULE), :] = x_v[pl.ds(table_ref[lax.div(k, 128), lax.rem(k, 128)] * GRANULE, GRANULE), :]

    with jax.named_scope("wait_g"):
        for s in range(seqs):
            at = pl.ds(s * seq, seq)
            pltpu.make_async_copy(dy_hbm.at[at, :], g_v.at[at, :], g_sem.at[s]).wait()

    @pl.loop(0, packed // GRANULE)
    def _(k):
        keep = lax.broadcasted_iota(jnp.int32, (GRANULE, d_model), 0) < table_ref[2 + lax.div(k, 128), lax.rem(k, 128)]
        rows = g_v[pl.ds(table_ref[lax.div(k, 128), lax.rem(k, 128)] * GRANULE, GRANULE), :]
        g_v[pl.ds(pl.multiple_of(k * GRANULE, GRANULE), GRANULE), :] = jnp.where(keep, rows, jnp.zeros((), bf16))

    with jax.named_scope("wait_w"):
        for copy in weights(0):
            copy.wait()
    dots(0, 0, u0, d0)

    @pl.loop(0, 4 * chunks + max(EVENT_AT[-1], dx_blocks))
    def _(tick):
        i, part = lax.div(tick, 4), lax.rem(tick, 4)
        busy = tick < 4 * chunks

        @pl.when(busy & (part == 0))
        def _():
            @pl.when(i + 1 < chunks)
            def _():
                for copy in weights(i + 1):
                    copy.start()

            @pl.when(i > 0)
            def _():
                du_out(i - 1).wait()

        @pl.when(busy & (part < 2))
        def _():
            @pl.when((part == 1) & (i + 1 < chunks))
            def _():
                for copy in weights(i + 1):
                    copy.wait()

            b = part * (BLOCKS // 2)
            after = jnp.minimum(i + part, chunks - 1)
            with jax.named_scope("tokens"):
                pointwise(b, u0, d0)
                dots(b + 1, i, u1, d1)
                pointwise(b + 1, u1, d1)
                dots(b + 2, i, u0, d0)
                pointwise(b + 2, u0, d0)
                dots(b + 3, i, u1, d1)
                pointwise(b + 3, u1, d1)
                dots(lax.rem(b + 4, BLOCKS), after, u0, d0)

            @pl.when(part == 1)
            def _():
                du_out(i).start()

        @pl.when(busy & (part == 2))
        def _():
            with jax.named_scope("dw2"):
                p2[lax.rem(i, HELD)] = lax.dot_general(a_v[...], g_v[:packed, :], TN, preferred_element_type=f32).astype(bf16)

        @pl.when(busy & (part == 3))
        def _():
            @pl.when(i == chunks - 1)
            def _():
                du_out(i).wait()
                du_in(0).start()

            with jax.named_scope("dw1"):
                p1[lax.rem(i, HELD)] = lax.dot_general(x_v[:packed, :], du_v[...], TN, preferred_element_type=f32).astype(bf16)

        q = tick - 4 * chunks

        @pl.when((q >= 0) & (q < dx_blocks))
        def _():
            slot = lax.rem(q, 2)

            @pl.when(q + 1 < dx_blocks)
            def _():
                du_in(q + 1).start()

            @pl.when(q > 1)
            def _():
                dx_out(q - 2).wait()

            with jax.named_scope("dx"):
                du_in(q).wait()
                dx_v[slot] = (g_v[dx_rows(q), :].astype(f32) + lax.dot_general(dub_v[slot], w1_v[...], NT, preferred_element_type=f32)).astype(bf16)
            dx_out(q).start()

        for e in reversed(range(2 * STAGES + 1)):
            since = tick + 1 - EVENT_AT[e]
            j = lax.div(since, 4) - 1

            @pl.when((since >= 4) & (lax.rem(since, 4) == 0) & (j < chunks))
            def _():
                with jax.named_scope(f"event{e}"):
                    event(e, j)

    dx_out(dx_blocks - 2).wait()
    dx_out(dx_blocks - 1).wait()


def grads_call(dims, ident, table, x, dy, w1, w2):
    tokens, d_model, d_ff, seq, packed, dx_block = dims
    scratch = [
        pltpu.VMEM((tokens, d_model), bf16), pltpu.VMEM((tokens, d_model), bf16),
        pltpu.VMEM((d_model, d_ff), bf16), pltpu.VMEM((2, CHUNK, d_model), bf16),
        pltpu.VMEM((packed // BLOCKS, CHUNK), bf16), pltpu.VMEM((packed // BLOCKS, CHUNK), bf16),
        pltpu.VMEM((packed // BLOCKS, CHUNK), f32), pltpu.VMEM((packed // BLOCKS, CHUNK), f32),
        pltpu.VMEM((packed, CHUNK), bf16), pltpu.VMEM((packed, CHUNK), bf16),
        pltpu.VMEM((HELD, d_model, CHUNK), bf16), pltpu.VMEM((HELD, CHUNK, d_model), bf16),
        pltpu.VMEM((2, dx_block, d_ff), bf16), pltpu.VMEM((2, dx_block, d_model), bf16),
    ]
    for (_, _, rows, _, cols, _) in part_table(d_model):
        for s in range(STAGES):
            last = s == STAGES - 1
            scratch.append(pltpu.VMEM((2, rows >> (4 if last else s + 1), cols // 2 if last else cols), bf16))
    dma = pltpu.SemaphoreType.DMA
    scratch += [dma((tokens // seq,)), dma((tokens // seq,)), dma((2, 2)), dma, dma((4,)), dma((2,)), dma((2,))]
    scratch += [dma((2, STAGES, 4))] * 4
    return pl.pallas_call(
        functools.partial(grads_kernel, dims),
        out_shape=[jax.ShapeDtypeStruct((d_model, d_ff), bf16), jax.ShapeDtypeStruct((d_ff, d_model), bf16),
                   jax.ShapeDtypeStruct((packed, d_ff), bf16), jax.ShapeDtypeStruct((packed + seq, d_model), bf16)],
        in_specs=[SMEM] + [ANY] * 4,
        out_specs=[ANY] * 4,
        scratch_shapes=scratch,
        compiler_params=pltpu.CompilerParams(collective_id=ident, has_side_effects=True, vmem_limit_bytes=62 * 2**20),
        cost_estimate=pl.CostEstimate(flops=10 * packed * d_model * d_ff, bytes_accessed=4 * packed * d_ff, transcendentals=packed * d_ff),
        name=f"grads{packed}",
    )(table, x, dy, w1, w2)


def finish_kernel(dims, len_ref, o1_hbm, o2_hbm, dxp_hbm, g1_hbm, g2_hbm, dx_hbm, c1_v, c2_v, dx_v, starts, c_in, c_out, dx_in, dx_out):
    tokens, d_model, d_ff, seq = dims
    seqs = tokens // seq
    steps, slots = 2 * seqs, 4
    n1, n2 = d_model // steps, d_ff // steps

    def rows(b, n):
        return pl.ds(pl.multiple_of(b * n, 16), n)

    def carry_in(b):
        slot = lax.rem(b, slots)
        return (pltpu.make_async_copy(o1_hbm.at[rows(b, n1), :], c1_v.at[slot], c_in.at[slot, 0]),
                pltpu.make_async_copy(o2_hbm.at[rows(b, n2), :], c2_v.at[slot], c_in.at[slot, 1]))

    def carry_out(b):
        slot = lax.rem(b, slots)
        return (pltpu.make_async_copy(c1_v.at[slot], g1_hbm.at[rows(b, n1), :], c_out.at[slot, 0]),
                pltpu.make_async_copy(c2_v.at[slot], g2_hbm.at[rows(b, n2), :], c_out.at[slot, 1]))

    starts[0] = jnp.int32(0)
    for s in range(1, seqs):
        starts[s] = starts[s - 1] + granules(len_ref, s - 1)

    def unpack_in(s):
        slot = lax.rem(s, slots)
        at = pl.ds(pl.multiple_of(starts[s] * GRANULE, GRANULE), seq)
        return pltpu.make_async_copy(dxp_hbm.at[at, :], dx_v.at[slot], dx_in.at[slot])

    def unpack_out(s):
        slot = lax.rem(s, slots)
        return pltpu.make_async_copy(dx_v.at[slot], dx_hbm.at[rows(s, seq), :], dx_out.at[slot])

    for b in (0, 1):
        for copy in carry_in(b):
            copy.start()
        unpack_in(b).start()

    @pl.loop(0, steps)
    def _(b):
        with jax.named_scope("carry_in_wait"):
            for copy in carry_in(b):
                copy.wait()
        for copy in carry_out(b):
            copy.start()

        @pl.when(b >= 2)
        def _():
            for copy in carry_out(b - 2):
                copy.wait()

        @pl.when(b + 2 < steps)
        def _():
            for copy in carry_in(b + 2):
                copy.start()

        s = lax.div(b, 2)

        @pl.when(lax.rem(b, 2) == 1)
        def _():
            unpack_in(s).wait()
            slot = lax.rem(s, slots)
            keep = lax.broadcasted_iota(jnp.int32, (seq, d_model), 0) < length(len_ref, s)
            dx_v[slot] = jnp.where(keep, dx_v[slot], jnp.zeros((), bf16))
            unpack_out(s).start()

            @pl.when(s >= 2)
            def _():
                unpack_out(s - 2).wait()

            @pl.when(s + 2 < seqs)
            def _():
                unpack_in(s + 2).start()

    for b in (steps - 2, steps - 1):
        for copy in carry_out(b):
            copy.wait()
    for s in (seqs - 2, seqs - 1):
        unpack_out(s).wait()


def finish_call(dims, lens, o1, o2, dxp):
    tokens, d_model, d_ff, seq = dims
    steps = 2 * (tokens // seq)
    dma = pltpu.SemaphoreType.DMA
    return pl.pallas_call(
        functools.partial(finish_kernel, dims),
        out_shape=[jax.ShapeDtypeStruct((d_model, d_ff), bf16), jax.ShapeDtypeStruct((d_ff, d_model), bf16),
                   jax.ShapeDtypeStruct((tokens, d_model), bf16)],
        in_specs=[SMEM] + [ANY] * 3,
        out_specs=[ANY] * 3,
        scratch_shapes=[
            pltpu.VMEM((4, d_model // steps, d_ff), bf16), pltpu.VMEM((4, d_ff // steps, d_model), bf16), pltpu.VMEM((4, seq, d_model), bf16),
            pltpu.SMEM((tokens // seq,), jnp.int32), dma((4, 2)), dma((4, 2)), dma((4,)), dma((4,))],
        compiler_params=pltpu.CompilerParams(vmem_limit_bytes=40 * 2**20),
        cost_estimate=pl.CostEstimate(flops=tokens * d_model, bytes_accessed=8 * d_model * d_ff, transcendentals=0),
        name="finish",
    )(lens, o1, o2, dxp)


def solution(mesh):
    def local_step(x_loc, dy_loc, lens, w_in, w_out):
        layers, d_model, d_ff = w_in.shape
        rows, seq, _ = x_loc.shape
        tokens = rows * seq
        x, dy = x_loc.reshape(tokens, d_model), dy_loc.reshape(tokens, d_model)
        w1, w2 = w_in.reshape(d_model, d_ff), w_out.reshape(d_ff, d_model)
        sizes = tuple(tokens * n // 16 for n in (12, 13, 16))

        def branch(n):
            def run(lens, table, x, dy, w1, w2):
                packed = sizes[n]
                o1, o2, _, dxp = grads_call((tokens, d_model, d_ff, seq, packed, tokens // 16), n + 1, table, x, dy, w1, w2)
                return finish_call((tokens, d_model, d_ff, seq), lens, o1, o2, dxp)

            return run

        size, table = most_call(lens, seq, sizes)
        g1, g2, dx = lax.switch(size[0, 0], [branch(n) for n in range(len(sizes))], lens, table, x, dy, w1, w2)
        return g1.reshape(layers, d_model, d_ff), g2.reshape(layers, d_ff, d_model), dx.reshape(rows, seq, d_model)

    return jax.shard_map(local_step, mesh=mesh, in_specs=(P("data"), P("data"), P("data"), P(), P()), out_specs=(P(), P(), P("data")), check_vma=False)
```

```python
import functools
import math
import jax
import jax.numpy as jnp
from jax import lax
from jax.experimental import pallas as pl
from jax.experimental.pallas import tpu as pltpu
from jax.sharding import PartitionSpec as P

GELU_SCALE = math.sqrt(2.0 / math.pi)
GELU_CUBIC = 0.044715
MESH = pl.DeviceIdType.MESH
NT = (((1,), (1,)), ((), ()))
TN = (((0,), (0,)), ((), ()))
f32 = jnp.float32
bf16 = jnp.bfloat16
ANY = pl.BlockSpec(memory_space=pl.ANY)
SMEM = pl.BlockSpec(memory_space=pltpu.SMEM)

CHUNK = 256
GRANULE = 16
BLOCKS = 8
STAGES = 5
WEIGHT = {"c": 1, "x": 2, "y": 4, "z": 8, "w": 16}
EVENTS = 2 * STAGES + 1
HELD = 4


def gelu_both(u):
    sq = u * u
    half = 0.5 + 0.5 * jnp.tanh(u * (GELU_SCALE + (GELU_SCALE * GELU_CUBIC) * sq))
    slope = half + (u * (2.0 * GELU_SCALE + (6.0 * GELU_SCALE * GELU_CUBIC) * sq)) * (half * (1.0 - half))
    return u * half, slope


def part_table(d_model):
    rows = 1024 if d_model == 1280 else d_model // 2
    cols = 768 if d_model == 1280 else d_model // 2
    return (
        (0, 0, rows, 0, CHUNK, "cxyzw"),
        (0, rows, d_model - rows, 0, CHUNK, "czxyw"),
        (1, 0, CHUNK, 0, cols, "cyxzw"),
        (1, 0, CHUNK, cols, d_model - cols, "czyxw"),
    )


def place():
    me = lax.axis_index("data")
    bit = {k: lax.rem(lax.div(me, v), 2) for k, v in WEIGHT.items()}
    return me, bit, {k: me + v * (1 - 2 * bit[k]) for k, v in WEIGHT.items()}


def granules(len_ref, s):
    return lax.div(length(len_ref, s) + (GRANULE - 1), GRANULE)


def length(len_ref, s):
    return len_ref[lax.rem(s, 2), lax.div(s, 2)]


def most_kernel(seqs, seq, sizes, len_ref, out_ref, table_ref, mine, plane, best, depth, send, recv):
    me, bit, _ = place()

    def other(d, names):
        return me + sum(WEIGHT[k] * (1 - 2 * bit[k]) for n, k in enumerate(names) if d >> n & 1)

    counts = [granules(len_ref, s) for s in range(seqs)]
    starts = [sum(counts[:s], jnp.int32(0)) for s in range(seqs + 1)]
    mine[...] = jnp.full(mine.shape, (starts[seqs] * GRANULE).astype(f32))
    barrier = pltpu.get_barrier_semaphore()
    near = [other(d, "cxy") for d in range(1, 8)]
    far = [other(d, "zw") for d in range(1, 4)]
    for device in near + far:
        pl.semaphore_signal(barrier, inc=1, device_id=(device,), device_id_type=MESH)
    pl.semaphore_wait(barrier, len(near) + len(far))

    def exchange(source, slots, devices, first):
        copies = [pltpu.make_async_remote_copy(source, slots.at[n], send.at[first + n], recv.at[first + n], device_id=(device,), device_id_type=MESH)
                  for n, device in enumerate(devices)]
        for copy in copies:
            copy.start()
        for copy in copies:
            copy.wait()
        return functools.reduce(jnp.maximum, [slots[n] for n in range(len(devices))], source[...])

    k = lax.broadcasted_iota(jnp.int32, (2, 128), 0) * 128 + lax.broadcasted_iota(jnp.int32, (2, 128), 1)
    source, left = k, length(len_ref, 0) - k * GRANULE
    for s in range(1, seqs):
        past = k >= starts[s]
        source = jnp.where(past, k - starts[s] + s * (seq // GRANULE), source)
        left = jnp.where(past, length(len_ref, s) - (k - starts[s]) * GRANULE, left)
    inside = k < starts[seqs]
    table_ref[0:2, :] = jnp.where(inside, source, 0)
    table_ref[2:4, :] = jnp.where(inside, left, 0)
    best[...] = exchange(mine, plane, near, 0)
    largest = exchange(best, depth, far, len(near))
    out_ref[...] = sum((largest > size).astype(jnp.int32) for size in sizes[:-1])


def most_call(lens, seq, sizes):
    tile = (8, 128)
    dma = pltpu.SemaphoreType.DMA
    return pl.pallas_call(
        functools.partial(most_kernel, lens.size, seq, sizes),
        out_shape=[jax.ShapeDtypeStruct(tile, jnp.int32), jax.ShapeDtypeStruct((4, 128), jnp.int32)],
        in_specs=[SMEM],
        out_specs=[pl.BlockSpec(memory_space=pltpu.VMEM)] * 2,
        scratch_shapes=[pltpu.VMEM(tile, f32), pltpu.VMEM((7, *tile), f32), pltpu.VMEM(tile, f32), pltpu.VMEM((3, *tile), f32), dma((10,)), dma((10,))],
        compiler_params=pltpu.CompilerParams(collective_id=0, has_side_effects=True),
        name="most",
    )(lens)


def grads_kernel(dims, table_ref, x_hbm, dy_hbm, w1_hbm, w2_hbm, o1_hbm, o2_hbm, du_hbm, dx_hbm, *scratch):
    tokens, d_model, d_ff, seq, packed, dx_block = dims
    seqs = tokens // seq
    chunks = d_ff // CHUNK
    block = packed // BLOCKS
    dx_blocks = packed // dx_block
    parts = part_table(d_model)
    (x_v, g_v, w1_v, w2_v, u0, u1, d0, d1, a_v, du_v, p1, p2, dub_v, dx_v) = scratch[:14]
    recv = [scratch[14 + 5 * k : 19 + 5 * k] for k in range(4)]
    (x_sem, g_sem, w_sem, du_sem, own_sem, dub_sem, dx_sem, rs_send, rs_recv, ag_send, ag_recv) = scratch[34:]

    _, bit, peer = place()
    for s in range(seqs):
        at = pl.ds(s * seq, seq)
        pltpu.make_async_copy(x_hbm.at[at, :], x_v.at[at, :], x_sem.at[s]).start()

    barrier = pltpu.get_barrier_semaphore()
    for k in WEIGHT:
        pl.semaphore_signal(barrier, inc=1, device_id=(peer[k],), device_id_type=MESH)
    pl.semaphore_wait(barrier, STAGES)

    region, given = [], []
    for (_, r0, nr, c0, nc, order) in parts:
        mine, away = [(r0, nr, c0, nc)], []
        for s, name in enumerate(order):
            row, rows, col, cols = mine[-1]
            if s < STAGES - 1:
                half = rows // 2
                mine.append((row + bit[name] * half, half, col, cols))
                away.append((row + (1 - bit[name]) * half, half, col, cols))
            else:
                half = cols // 2
                mine.append((row, rows, col + bit[name] * half, half))
                away.append((row, rows, col + (1 - bit[name]) * half, half))
        region.append(mine)
        given.append(away)

    def cut(r):
        row, rows, col, cols = r
        row = row if isinstance(row, int) else pl.multiple_of(row, 16)
        col = col if isinstance(col, int) else pl.multiple_of(col, 128)
        return pl.ds(row, rows), pl.ds(col, cols)

    def partial(k, i, r):
        rows, cols = cut(r)
        return (p1, p2)[parts[k][0]].at[lax.rem(i, HELD), rows, cols]

    def whole(k, i, r):
        row, rows, col, cols = r
        if parts[k][0] == 0:
            return o1_hbm.at[cut((row, rows, i * CHUNK + col, cols))]
        return o2_hbm.at[cut((i * CHUNK + row, rows, col, cols))]

    def reduce_copy(k, s, i):
        slot = lax.rem(i, 2)
        return pltpu.make_async_remote_copy(
            src_ref=partial(k, i, given[k][s]), dst_ref=recv[k][s].at[slot],
            send_sem=rs_send.at[slot, s, k], recv_sem=rs_recv.at[slot, s, k],
            device_id=(peer[parts[k][5][s]],), device_id_type=MESH)

    def gather_copy(k, s, i):
        slot = lax.rem(i, 2)
        r = region[k][s + 1]
        return pltpu.make_async_remote_copy(
            src_ref=partial(k, i, r) if s == STAGES - 1 else whole(k, i, r), dst_ref=whole(k, i, r),
            send_sem=ag_send.at[slot, s, k], recv_sem=ag_recv.at[slot, s, k],
            device_id=(peer[parts[k][5][s]],), device_id_type=MESH)

    def own_copy(k, i):
        r = region[k][STAGES]
        return pltpu.make_async_copy(partial(k, i, r), whole(k, i, r), own_sem.at[k])

    def event(e, i):
        for k in range(4):
            if 1 <= e <= STAGES:
                reduce_copy(k, e - 1, i).wait()
                rows, cols = cut(region[k][e])
                ref, slot = (p1, p2)[parts[k][0]], lax.rem(i, HELD)
                ref[slot, rows, cols] = ref[slot, rows, cols] + recv[k][e - 1][lax.rem(i, 2)]
            if e < STAGES:
                reduce_copy(k, e, i).start()
            if e == STAGES:
                own_copy(k, i).start()
            if e > STAGES:
                gather_copy(k, 2 * STAGES - e, i).wait()
                if e == STAGES + 1:
                    own_copy(k, i).wait()
            if STAGES <= e < 2 * STAGES:
                gather_copy(k, 2 * STAGES - 1 - e, i).start()

    def weights(i):
        slot = lax.rem(i, 2)
        at = pl.ds(pl.multiple_of(i * CHUNK, CHUNK), CHUNK)
        return (pltpu.make_async_copy(w1_hbm.at[:, at], w1_v.at[:, at], w_sem.at[slot, 0]),
                pltpu.make_async_copy(w2_hbm.at[at, :], w2_v.at[slot], w_sem.at[slot, 1]))

    def rows_of(b):
        return pl.ds(pl.multiple_of(b * block, 16), block)

    def dots(b, i, u, d):
        w1 = w1_v[:, pl.ds(pl.multiple_of(i * CHUNK, CHUNK), CHUNK)]
        u[...] = jnp.dot(x_v[rows_of(b), :], w1, preferred_element_type=f32).astype(bf16)
        d[...] = lax.dot_general(g_v[rows_of(b), :], w2_v[lax.rem(i, 2)], NT, preferred_element_type=f32)

    def pointwise(b, u, d):
        a, slope = gelu_both(u[...].astype(f32))
        a_v[rows_of(b), :] = a.astype(bf16)
        du_v[rows_of(b), :] = (d[...] * slope).astype(bf16)

    def du_out(i):
        return pltpu.make_async_copy(du_v, du_hbm.at[:, pl.ds(pl.multiple_of(i * CHUNK, CHUNK), CHUNK)], du_sem)

    def dx_rows(q):
        return pl.ds(pl.multiple_of(q * dx_block, 16), dx_block)

    def du_in(q):
        slot = lax.rem(q, 2)
        return pltpu.make_async_copy(du_hbm.at[dx_rows(q), :], dub_v.at[slot], dub_sem.at[slot])

    def dx_out(q):
        slot = lax.rem(q, 2)
        return pltpu.make_async_copy(dx_v.at[slot], dx_hbm.at[dx_rows(q), :], dx_sem.at[slot])

    for s in range(seqs):
        at = pl.ds(s * seq, seq)
        pltpu.make_async_copy(dy_hbm.at[at, :], g_v.at[at, :], g_sem.at[s]).start()
    for copy in weights(0):
        copy.start()
    with jax.named_scope("wait_x"):
        for s in range(seqs):
            at = pl.ds(s * seq, seq)
            pltpu.make_async_copy(x_hbm.at[at, :], x_v.at[at, :], x_sem.at[s]).wait()

    group = 4 if packed % (4 * GRANULE) == 0 else 2

    def granule_rows(k):
        return pl.ds(pl.multiple_of(k * GRANULE, GRANULE), GRANULE)

    def source_rows(k):
        return pl.ds(table_ref[lax.div(k, 128), lax.rem(k, 128)] * GRANULE, GRANULE)

    @pl.loop(0, packed // GRANULE // group)
    def _(n):
        rows = [x_v[source_rows(n * group + k), :] for k in range(group)]
        for k in range(group):
            x_v[granule_rows(n * group + k), :] = rows[k]

    with jax.named_scope("wait_g"):
        for s in range(seqs):
            at = pl.ds(s * seq, seq)
            pltpu.make_async_copy(dy_hbm.at[at, :], g_v.at[at, :], g_sem.at[s]).wait()

    @pl.loop(0, packed // GRANULE // group)
    def _(n):
        rows = [g_v[source_rows(n * group + k), :] for k in range(group)]
        for k in range(group):
            at = n * group + k
            keep = lax.broadcasted_iota(jnp.int32, (GRANULE, d_model), 0) < table_ref[2 + lax.div(at, 128), lax.rem(at, 128)]
            g_v[granule_rows(at), :] = jnp.where(keep, rows[k], jnp.zeros((), bf16))

    with jax.named_scope("wait_w"):
        for copy in weights(0):
            copy.wait()
    dots(0, 0, u0, d0)

    def events(i, point):
        for e in reversed(range(EVENTS)):
            if e % 2 != point % 2:
                j = i - lax.div(e + 1, 2)

                @pl.when((j >= 0) & (j < chunks))
                def _():
                    with jax.named_scope(f"event{e}"):
                        event(e, j)

    @pl.loop(0, chunks)
    def _(i):
        @pl.when(i + 1 < chunks)
        def _():
            for copy in weights(i + 1):
                copy.start()

        @pl.when(i > 0)
        def _():
            du_out(i - 1).wait()

        @pl.loop(0, 2)
        def _(half):
            @pl.when((half == 1) & (i + 1 < chunks))
            def _():
                for copy in weights(i + 1):
                    copy.wait()

            b = half * (BLOCKS // 2)
            after = jnp.minimum(i + half, chunks - 1)
            with jax.named_scope("tokens"):
                pointwise(b, u0, d0)
                dots(b + 1, i, u1, d1)
                pointwise(b + 1, u1, d1)
                dots(b + 2, i, u0, d0)
                pointwise(b + 2, u0, d0)
                dots(b + 3, i, u1, d1)
                pointwise(b + 3, u1, d1)
                dots(lax.rem(b + 4, BLOCKS), after, u0, d0)

        du_out(i).start()
        events(i, 0)
        slot = lax.rem(i, HELD)
        with jax.named_scope("dw"):
            p2[slot] = lax.dot_general(a_v[...], g_v[:packed, :], TN, preferred_element_type=f32).astype(bf16)
            p1[slot] = lax.dot_general(x_v[:packed, :], du_v[...], TN, preferred_element_type=f32).astype(bf16)
        events(i, 1)

    du_out(chunks - 1).wait()
    du_in(0).start()

    @pl.loop(0, max(2 * STAGES, dx_blocks))
    def _(q):
        @pl.when(q < dx_blocks)
        def _():
            slot = lax.rem(q, 2)

            @pl.when(q + 1 < dx_blocks)
            def _():
                du_in(q + 1).start()

            @pl.when(q > 1)
            def _():
                dx_out(q - 2).wait()

            with jax.named_scope("dx"):
                du_in(q).wait()
                dx_v[slot] = (g_v[dx_rows(q), :].astype(f32) + lax.dot_general(dub_v[slot], w1_v[...], NT, preferred_element_type=f32)).astype(bf16)
            dx_out(q).start()

        i = chunks + lax.div(q, 2)

        @pl.when(lax.rem(q, 2) == 0)
        def _():
            events(i, 0)

        @pl.when(lax.rem(q, 2) == 1)
        def _():
            events(i, 1)

    dx_out(dx_blocks - 2).wait()
    dx_out(dx_blocks - 1).wait()


def grads_call(dims, ident, table, x, dy, w1, w2):
    tokens, d_model, d_ff, seq, packed, dx_block = dims
    scratch = [
        pltpu.VMEM((tokens, d_model), bf16), pltpu.VMEM((tokens, d_model), bf16),
        pltpu.VMEM((d_model, d_ff), bf16), pltpu.VMEM((2, CHUNK, d_model), bf16),
        pltpu.VMEM((packed // BLOCKS, CHUNK), bf16), pltpu.VMEM((packed // BLOCKS, CHUNK), bf16),
        pltpu.VMEM((packed // BLOCKS, CHUNK), f32), pltpu.VMEM((packed // BLOCKS, CHUNK), f32),
        pltpu.VMEM((packed, CHUNK), bf16), pltpu.VMEM((packed, CHUNK), bf16),
        pltpu.VMEM((HELD, d_model, CHUNK), bf16), pltpu.VMEM((HELD, CHUNK, d_model), bf16),
        pltpu.VMEM((2, dx_block, d_ff), bf16), pltpu.VMEM((2, dx_block, d_model), bf16),
    ]
    for (_, _, rows, _, cols, _) in part_table(d_model):
        for s in range(STAGES):
            last = s == STAGES - 1
            scratch.append(pltpu.VMEM((2, rows >> (4 if last else s + 1), cols // 2 if last else cols), bf16))
    dma = pltpu.SemaphoreType.DMA
    scratch += [dma((tokens // seq,)), dma((tokens // seq,)), dma((2, 2)), dma, dma((4,)), dma((2,)), dma((2,))]
    scratch += [dma((2, STAGES, 4))] * 4
    return pl.pallas_call(
        functools.partial(grads_kernel, dims),
        out_shape=[jax.ShapeDtypeStruct((d_model, d_ff), bf16), jax.ShapeDtypeStruct((d_ff, d_model), bf16),
                   jax.ShapeDtypeStruct((packed, d_ff), bf16), jax.ShapeDtypeStruct((packed + seq, d_model), bf16)],
        in_specs=[SMEM] + [ANY] * 4,
        out_specs=[ANY] * 4,
        scratch_shapes=scratch,
        compiler_params=pltpu.CompilerParams(collective_id=ident, has_side_effects=True, vmem_limit_bytes=62 * 2**20),
        cost_estimate=pl.CostEstimate(flops=10 * packed * d_model * d_ff, bytes_accessed=4 * packed * d_ff, transcendentals=packed * d_ff),
        name=f"grads{packed}",
    )(table, x, dy, w1, w2)


def finish_kernel(dims, len_ref, o1_hbm, o2_hbm, dxp_hbm, g1_hbm, g2_hbm, dx_hbm, c1_v, c2_v, dx_v, starts, c_in, c_out, dx_in, dx_out):
    tokens, d_model, d_ff, seq = dims
    seqs = tokens // seq
    steps, slots = 2 * seqs, 4
    n1, n2 = d_model // steps, d_ff // steps

    def rows(b, n):
        return pl.ds(pl.multiple_of(b * n, 16), n)

    def carry_in(b):
        slot = lax.rem(b, slots)
        return (pltpu.make_async_copy(o1_hbm.at[rows(b, n1), :], c1_v.at[slot], c_in.at[slot, 0]),
                pltpu.make_async_copy(o2_hbm.at[rows(b, n2), :], c2_v.at[slot], c_in.at[slot, 1]))

    def carry_out(b):
        slot = lax.rem(b, slots)
        return (pltpu.make_async_copy(c1_v.at[slot], g1_hbm.at[rows(b, n1), :], c_out.at[slot, 0]),
                pltpu.make_async_copy(c2_v.at[slot], g2_hbm.at[rows(b, n2), :], c_out.at[slot, 1]))

    starts[0] = jnp.int32(0)
    for s in range(1, seqs):
        starts[s] = starts[s - 1] + granules(len_ref, s - 1)

    def unpack_in(s):
        slot = lax.rem(s, slots)
        at = pl.ds(pl.multiple_of(starts[s] * GRANULE, GRANULE), seq)
        return pltpu.make_async_copy(dxp_hbm.at[at, :], dx_v.at[slot], dx_in.at[slot])

    def unpack_out(s):
        slot = lax.rem(s, slots)
        return pltpu.make_async_copy(dx_v.at[slot], dx_hbm.at[rows(s, seq), :], dx_out.at[slot])

    for b in (0, 1):
        for copy in carry_in(b):
            copy.start()
        unpack_in(b).start()

    @pl.loop(0, steps)
    def _(b):
        with jax.named_scope("carry_in_wait"):
            for copy in carry_in(b):
                copy.wait()
        for copy in carry_out(b):
            copy.start()

        @pl.when(b >= 2)
        def _():
            for copy in carry_out(b - 2):
                copy.wait()

        @pl.when(b + 2 < steps)
        def _():
            for copy in carry_in(b + 2):
                copy.start()

        s = lax.div(b, 2)

        @pl.when(lax.rem(b, 2) == 1)
        def _():
            unpack_in(s).wait()
            slot = lax.rem(s, slots)
            keep = lax.broadcasted_iota(jnp.int32, (seq, d_model), 0) < length(len_ref, s)
            dx_v[slot] = jnp.where(keep, dx_v[slot], jnp.zeros((), bf16))
            unpack_out(s).start()

            @pl.when(s >= 2)
            def _():
                unpack_out(s - 2).wait()

            @pl.when(s + 2 < seqs)
            def _():
                unpack_in(s + 2).start()

    for b in (steps - 2, steps - 1):
        for copy in carry_out(b):
            copy.wait()
    for s in (seqs - 2, seqs - 1):
        unpack_out(s).wait()


def finish_call(dims, lens, o1, o2, dxp):
    tokens, d_model, d_ff, seq = dims
    steps = 2 * (tokens // seq)
    dma = pltpu.SemaphoreType.DMA
    return pl.pallas_call(
        functools.partial(finish_kernel, dims),
        out_shape=[jax.ShapeDtypeStruct((d_model, d_ff), bf16), jax.ShapeDtypeStruct((d_ff, d_model), bf16),
                   jax.ShapeDtypeStruct((tokens, d_model), bf16)],
        in_specs=[SMEM] + [ANY] * 3,
        out_specs=[ANY] * 3,
        scratch_shapes=[
            pltpu.VMEM((4, d_model // steps, d_ff), bf16), pltpu.VMEM((4, d_ff // steps, d_model), bf16), pltpu.VMEM((4, seq, d_model), bf16),
            pltpu.SMEM((tokens // seq,), jnp.int32), dma((4, 2)), dma((4, 2)), dma((4,)), dma((4,))],
        compiler_params=pltpu.CompilerParams(vmem_limit_bytes=63 * 2**20),
        cost_estimate=pl.CostEstimate(flops=tokens * d_model, bytes_accessed=8 * d_model * d_ff, transcendentals=0),
        name="finish",
    )(lens, o1, o2, dxp)


def solution(mesh):
    def local_step(x_loc, dy_loc, len_loc, w_in, w_out):
        layers, d_model, d_ff = w_in.shape
        rows, seq, _ = x_loc.shape
        tokens = rows * seq
        lens = len_loc.T
        x, dy = x_loc.reshape(tokens, d_model), dy_loc.reshape(tokens, d_model)
        w1, w2 = w_in.reshape(d_model, d_ff), w_out.reshape(d_ff, d_model)
        sizes = tuple(tokens * n // 16 for n in (12, 13, 16))

        def branch(n):
            def run(lens, table, x, dy, w1, w2):
                packed = sizes[n]
                o1, o2, _, dxp = grads_call((tokens, d_model, d_ff, seq, packed, tokens // 16), n + 1, table, x, dy, w1, w2)
                return finish_call((tokens, d_model, d_ff, seq), lens, o1, o2, dxp)

            return run

        size, table = most_call(lens, seq, sizes)
        g1, g2, dx = lax.switch(size[0, 0], [branch(n) for n in range(len(sizes))], lens, table, x, dy, w1, w2)
        return g1.reshape(layers, d_model, d_ff), g2.reshape(layers, d_ff, d_model), dx.reshape(rows, seq, d_model)

    return jax.shard_map(local_step, mesh=mesh, in_specs=(P("data"), P("data"), P("data"), P(), P()), out_specs=(P(), P(), P("data")), check_vma=False)
```

```python
import functools
import math
import jax
import jax.numpy as jnp
from jax import lax
from jax.experimental import pallas as pl
from jax.experimental.pallas import tpu as pltpu
from jax.sharding import PartitionSpec as P

GELU_SCALE = math.sqrt(2.0 / math.pi)
GELU_CUBIC = 0.044715
MESH = pl.DeviceIdType.MESH
NT = (((1,), (1,)), ((), ()))
TN = (((0,), (0,)), ((), ()))
f32 = jnp.float32
bf16 = jnp.bfloat16
ANY = pl.BlockSpec(memory_space=pl.ANY)
SMEM = pl.BlockSpec(memory_space=pltpu.SMEM)

CHUNK = 256
GRANULE = 16
BLOCKS = 8
STAGES = 5
DEVICES = 2**STAGES
WEIGHT = {"c": 1, "x": 2, "y": 4, "z": 8, "w": 16}
EVENTS = 2 * STAGES + 1
HELD = 4


def gelu_both(u):
    sq = u * u
    half = 0.5 + 0.5 * jnp.tanh(u * (GELU_SCALE + (GELU_SCALE * GELU_CUBIC) * sq))
    value = u * half
    return value, half + (value * (1.0 - half)) * (2.0 * GELU_SCALE + (6.0 * GELU_SCALE * GELU_CUBIC) * sq)


def part_table(d_model):
    rows = 1024 if d_model == 1280 else d_model // 2
    cols = 768 if d_model == 1280 else d_model // 2
    return (
        (0, 0, rows, 0, CHUNK, "cxyzw"),
        (0, rows, d_model - rows, 0, CHUNK, "czxyw"),
        (1, 0, CHUNK, 0, cols, "cyxzw"),
        (1, 0, CHUNK, cols, d_model - cols, "czyxw"),
    )


def place():
    me = lax.axis_index("data")
    bit = {k: lax.rem(lax.div(me, v), 2) for k, v in WEIGHT.items()}
    return me, bit, {k: me + v * (1 - 2 * bit[k]) for k, v in WEIGHT.items()}


def granules(len_ref, s):
    return lax.div(length(len_ref, s) + (GRANULE - 1), GRANULE)


def length(len_ref, s):
    return len_ref[lax.rem(s, 2), lax.div(s, 2)]


def most_kernel(seqs, seq, sizes, len_ref, out_ref, table_ref, mine, theirs, send, recv):
    me, bit, _ = place()

    def other(d, names):
        return me + sum(WEIGHT[k] * (1 - 2 * bit[k]) for n, k in enumerate(names) if d >> n & 1)

    counts = [granules(len_ref, s) for s in range(seqs)]
    starts = [sum(counts[:s], jnp.int32(0)) for s in range(seqs + 1)]
    mine[...] = jnp.full(mine.shape, (starts[seqs] * GRANULE).astype(f32))
    barrier = pltpu.get_barrier_semaphore()
    others = [other(d, "cxyzw") for d in range(1, DEVICES)]
    for device in others:
        pl.semaphore_signal(barrier, inc=1, device_id=(device,), device_id_type=MESH)
    pl.semaphore_wait(barrier, DEVICES - 1)

    copies = [pltpu.make_async_remote_copy(mine, theirs.at[n], send.at[n], recv.at[n], device_id=(device,), device_id_type=MESH)
              for n, device in enumerate(others)]
    for copy in copies:
        copy.start()
    k = lax.broadcasted_iota(jnp.int32, (2, 128), 0) * 128 + lax.broadcasted_iota(jnp.int32, (2, 128), 1)
    source, left = k, length(len_ref, 0) - k * GRANULE
    for s in range(1, seqs):
        past = k >= starts[s]
        source = jnp.where(past, k - starts[s] + s * (seq // GRANULE), source)
        left = jnp.where(past, length(len_ref, s) - (k - starts[s]) * GRANULE, left)
    inside = k < starts[seqs]
    table_ref[0:2, :] = jnp.where(inside, source, 0)
    table_ref[2:4, :] = jnp.where(inside, left, 0)
    for copy in copies:
        copy.wait()
    largest = functools.reduce(jnp.maximum, [theirs[n] for n in range(DEVICES - 1)], mine[...])
    out_ref[...] = sum((largest > size).astype(jnp.int32) for size in sizes[:-1])


def most_call(lens, seq, sizes):
    tile = (8, 128)
    dma = pltpu.SemaphoreType.DMA
    return pl.pallas_call(
        functools.partial(most_kernel, lens.size, seq, sizes),
        out_shape=[jax.ShapeDtypeStruct(tile, jnp.int32), jax.ShapeDtypeStruct((4, 128), jnp.int32)],
        in_specs=[SMEM],
        out_specs=[pl.BlockSpec(memory_space=pltpu.VMEM)] * 2,
        scratch_shapes=[pltpu.VMEM(tile, f32), pltpu.VMEM((DEVICES - 1, *tile), f32), dma((DEVICES - 1,)), dma((DEVICES - 1,))],
        compiler_params=pltpu.CompilerParams(collective_id=0, has_side_effects=True),
        name="most",
    )(lens)


def grads_kernel(dims, table_ref, x_hbm, dy_hbm, w1_hbm, w2_hbm, o1_hbm, o2_hbm, du_hbm, dx_hbm, *scratch):
    tokens, d_model, d_ff, seq, packed, dx_block = dims
    seqs = tokens // seq
    chunks = d_ff // CHUNK
    block = packed // BLOCKS
    dx_blocks = packed // dx_block
    span = BLOCKS // 2 if packed < tokens else 2
    parts = part_table(d_model)
    (x_v, g_v, w1_v, w2_v, u0, u1, d0, d1, a_v, du_v, p1, p2, dub_v, dx_v) = scratch[:14]
    recv = [scratch[14 + 5 * k : 19 + 5 * k] for k in range(4)]
    (x_sem, g_sem, w_sem, du_sem, own_sem, dub_sem, dx_sem, rs_send, rs_recv, ag_send, ag_recv) = scratch[34:]

    _, bit, peer = place()
    for s in range(seqs):
        at = pl.ds(s * seq, seq)
        pltpu.make_async_copy(x_hbm.at[at, :], x_v.at[at, :], x_sem.at[s]).start()

    barrier = pltpu.get_barrier_semaphore()
    for k in WEIGHT:
        pl.semaphore_signal(barrier, inc=1, device_id=(peer[k],), device_id_type=MESH)
    pl.semaphore_wait(barrier, STAGES)

    region, given = [], []
    for (_, r0, nr, c0, nc, order) in parts:
        mine, away = [(r0, nr, c0, nc)], []
        for s, name in enumerate(order):
            row, rows, col, cols = mine[-1]
            if s < STAGES - 1:
                half = rows // 2
                mine.append((row + bit[name] * half, half, col, cols))
                away.append((row + (1 - bit[name]) * half, half, col, cols))
            else:
                half = cols // 2
                mine.append((row, rows, col + bit[name] * half, half))
                away.append((row, rows, col + (1 - bit[name]) * half, half))
        region.append(mine)
        given.append(away)

    def cut(r):
        row, rows, col, cols = r
        row = row if isinstance(row, int) else pl.multiple_of(row, 16)
        col = col if isinstance(col, int) else pl.multiple_of(col, 128)
        return pl.ds(row, rows), pl.ds(col, cols)

    def partial(k, i, r):
        rows, cols = cut(r)
        return (p1, p2)[parts[k][0]].at[lax.rem(i, HELD), rows, cols]

    def whole(k, i, r):
        row, rows, col, cols = r
        if parts[k][0] == 0:
            return o1_hbm.at[cut((row, rows, i * CHUNK + col, cols))]
        return o2_hbm.at[cut((i * CHUNK + row, rows, col, cols))]

    def reduce_copy(k, s, i):
        slot = lax.rem(i, 2)
        return pltpu.make_async_remote_copy(
            src_ref=partial(k, i, given[k][s]), dst_ref=recv[k][s].at[slot],
            send_sem=rs_send.at[slot, s, k], recv_sem=rs_recv.at[slot, s, k],
            device_id=(peer[parts[k][5][s]],), device_id_type=MESH)

    def gather_copy(k, s, i):
        slot = lax.rem(i, 2)
        r = region[k][s + 1]
        return pltpu.make_async_remote_copy(
            src_ref=partial(k, i, r) if s == STAGES - 1 else whole(k, i, r), dst_ref=whole(k, i, r),
            send_sem=ag_send.at[slot, s, k], recv_sem=ag_recv.at[slot, s, k],
            device_id=(peer[parts[k][5][s]],), device_id_type=MESH)

    def own_copy(k, i):
        r = region[k][STAGES]
        return pltpu.make_async_copy(partial(k, i, r), whole(k, i, r), own_sem.at[k])

    def event(e, i):
        for k in range(4):
            if 1 <= e <= STAGES:
                reduce_copy(k, e - 1, i).wait()
                rows, cols = cut(region[k][e])
                ref, slot = (p1, p2)[parts[k][0]], lax.rem(i, HELD)
                ref[slot, rows, cols] = ref[slot, rows, cols] + recv[k][e - 1][lax.rem(i, 2)]
            if e < STAGES:
                reduce_copy(k, e, i).start()
            if e == STAGES:
                own_copy(k, i).start()
            if e > STAGES:
                gather_copy(k, 2 * STAGES - e, i).wait()
                if e == STAGES + 1:
                    own_copy(k, i).wait()
            if STAGES <= e < 2 * STAGES:
                gather_copy(k, 2 * STAGES - 1 - e, i).start()

    def weights(i):
        slot = lax.rem(i, 2)
        at = pl.ds(pl.multiple_of(i * CHUNK, CHUNK), CHUNK)
        return (pltpu.make_async_copy(w1_hbm.at[:, at], w1_v.at[:, at], w_sem.at[slot, 0]),
                pltpu.make_async_copy(w2_hbm.at[at, :], w2_v.at[slot], w_sem.at[slot, 1]))

    def rows_of(b):
        return pl.ds(pl.multiple_of(b * block, 16), block)

    def dots(b, i, u, d):
        w1 = w1_v[:, pl.ds(pl.multiple_of(i * CHUNK, CHUNK), CHUNK)]
        u[...] = jnp.dot(x_v[rows_of(b), :], w1, preferred_element_type=f32).astype(bf16)
        d[...] = lax.dot_general(g_v[rows_of(b), :], w2_v[lax.rem(i, 2)], NT, preferred_element_type=f32)

    def pointwise(b, u, d):
        a, slope = gelu_both(u[...].astype(f32))
        a_v[rows_of(b), :] = a.astype(bf16)
        du_v[rows_of(b), :] = (d[...] * slope).astype(bf16)

    def du_out(i):
        return pltpu.make_async_copy(du_v, du_hbm.at[:, pl.ds(pl.multiple_of(i * CHUNK, CHUNK), CHUNK)], du_sem)

    def dx_rows(q):
        return pl.ds(pl.multiple_of(q * dx_block, 16), dx_block)

    def du_in(q):
        slot = lax.rem(q, 2)
        return pltpu.make_async_copy(du_hbm.at[dx_rows(q), :], dub_v.at[slot], dub_sem.at[slot])

    def dx_out(q):
        slot = lax.rem(q, 2)
        return pltpu.make_async_copy(dx_v.at[slot], dx_hbm.at[dx_rows(q), :], dx_sem.at[slot])

    for s in range(seqs):
        at = pl.ds(s * seq, seq)
        pltpu.make_async_copy(dy_hbm.at[at, :], g_v.at[at, :], g_sem.at[s]).start()
    for copy in weights(0):
        copy.start()
    with jax.named_scope("wait_x"):
        for s in range(seqs):
            at = pl.ds(s * seq, seq)
            pltpu.make_async_copy(x_hbm.at[at, :], x_v.at[at, :], x_sem.at[s]).wait()

    group = 4 if packed % (4 * GRANULE) == 0 else 2

    def granule_rows(k):
        return pl.ds(pl.multiple_of(k * GRANULE, GRANULE), GRANULE)

    def source_rows(k):
        return pl.ds(table_ref[lax.div(k, 128), lax.rem(k, 128)] * GRANULE, GRANULE)

    @pl.loop(0, packed // GRANULE // group)
    def _(n):
        rows = [x_v[source_rows(n * group + k), :] for k in range(group)]
        for k in range(group):
            x_v[granule_rows(n * group + k), :] = rows[k]

    with jax.named_scope("wait_g"):
        for s in range(seqs):
            at = pl.ds(s * seq, seq)
            pltpu.make_async_copy(dy_hbm.at[at, :], g_v.at[at, :], g_sem.at[s]).wait()

    @pl.loop(0, packed // GRANULE // group)
    def _(n):
        rows = [g_v[source_rows(n * group + k), :] for k in range(group)]
        for k in range(group):
            at = n * group + k
            keep = lax.broadcasted_iota(jnp.int32, (GRANULE, d_model), 0) < table_ref[2 + lax.div(at, 128), lax.rem(at, 128)]
            g_v[granule_rows(at), :] = jnp.where(keep, rows[k], jnp.zeros((), bf16))

    with jax.named_scope("wait_w"):
        for copy in weights(0):
            copy.wait()
    dots(0, 0, u0, d0)

    def events(i, which):
        for e in which:
            j = i - lax.div(e + 1, 2)

            @pl.when((j >= 0) & (j < chunks))
            def _():
                with jax.named_scope(f"event{e}"):
                    event(e, j)

    @pl.loop(0, chunks)
    def _(i):
        @pl.when(i + 1 < chunks)
        def _():
            for copy in weights(i + 1):
                copy.start()

        @pl.when(i > 0)
        def _():
            du_out(i - 1).wait()

        @pl.loop(0, BLOCKS // span)
        def _(n):
            last = n == BLOCKS // span - 1

            @pl.when(last & (i + 1 < chunks))
            def _():
                for copy in weights(i + 1):
                    copy.wait()

            b = n * span
            after = jnp.minimum(i + last.astype(jnp.int32), chunks - 1)
            sets = ((u0, d0), (u1, d1))
            with jax.named_scope("tokens"):
                for k in range(span):
                    pointwise(b + k, *sets[k % 2])
                    if k < span - 1:
                        dots(b + k + 1, i, *sets[(k + 1) % 2])
                    else:
                        dots(lax.rem(b + span, BLOCKS), after, *sets[0])

            @pl.when(n == BLOCKS // span // 2 - 1)
            def _():
                events(i, (1,))

        du_out(i).start()
        events(i, (9, 7, 5, 3))
        slot = lax.rem(i, HELD)
        with jax.named_scope("dw"):
            p2[slot] = lax.dot_general(a_v[...], g_v[:packed, :], TN, preferred_element_type=f32).astype(bf16)
            p1[slot] = lax.dot_general(x_v[:packed, :], du_v[...], TN, preferred_element_type=f32).astype(bf16)

        @pl.when(i == chunks - 1)
        def _():
            du_out(i).wait()
            du_in(0).start()

        events(i, (0, 10, 8, 6, 4, 2))

    @pl.loop(0, max(2 * STAGES, dx_blocks))
    def _(q):
        @pl.when(q < dx_blocks)
        def _():
            slot = lax.rem(q, 2)

            @pl.when(q + 1 < dx_blocks)
            def _():
                du_in(q + 1).start()

            @pl.when(q > 1)
            def _():
                dx_out(q - 2).wait()

            with jax.named_scope("dx"):
                du_in(q).wait()
                dx_v[slot] = (g_v[dx_rows(q), :].astype(f32) + lax.dot_general(dub_v[slot], w1_v[...], NT, preferred_element_type=f32)).astype(bf16)
            dx_out(q).start()

        i = chunks + lax.div(q, 2)

        @pl.when(lax.rem(q, 2) == 0)
        def _():
            events(i, (1, 9, 7, 5, 3))

        @pl.when(lax.rem(q, 2) == 1)
        def _():
            events(i, (10, 8, 6, 4, 2))

    dx_out(dx_blocks - 2).wait()
    dx_out(dx_blocks - 1).wait()


def grads_call(dims, ident, table, x, dy, w1, w2):
    tokens, d_model, d_ff, seq, packed, dx_block = dims
    scratch = [
        pltpu.VMEM((tokens, d_model), bf16), pltpu.VMEM((tokens, d_model), bf16),
        pltpu.VMEM((d_model, d_ff), bf16), pltpu.VMEM((2, CHUNK, d_model), bf16),
        pltpu.VMEM((packed // BLOCKS, CHUNK), bf16), pltpu.VMEM((packed // BLOCKS, CHUNK), bf16),
        pltpu.VMEM((packed // BLOCKS, CHUNK), f32), pltpu.VMEM((packed // BLOCKS, CHUNK), f32),
        pltpu.VMEM((packed, CHUNK), bf16), pltpu.VMEM((packed, CHUNK), bf16),
        pltpu.VMEM((HELD, d_model, CHUNK), bf16), pltpu.VMEM((HELD, CHUNK, d_model), bf16),
        pltpu.VMEM((2, dx_block, d_ff), bf16), pltpu.VMEM((2, dx_block, d_model), bf16),
    ]
    for (_, _, rows, _, cols, _) in part_table(d_model):
        for s in range(STAGES):
            last = s == STAGES - 1
            scratch.append(pltpu.VMEM((2, rows >> (4 if last else s + 1), cols // 2 if last else cols), bf16))
    dma = pltpu.SemaphoreType.DMA
    scratch += [dma((tokens // seq,)), dma((tokens // seq,)), dma((2, 2)), dma, dma((4,)), dma((2,)), dma((2,))]
    scratch += [dma((2, STAGES, 4))] * 4
    return pl.pallas_call(
        functools.partial(grads_kernel, dims),
        out_shape=[jax.ShapeDtypeStruct((d_model, d_ff), bf16), jax.ShapeDtypeStruct((d_ff, d_model), bf16),
                   jax.ShapeDtypeStruct((packed, d_ff), bf16), jax.ShapeDtypeStruct((packed + seq, d_model), bf16)],
        in_specs=[SMEM] + [ANY] * 4,
        out_specs=[ANY] * 4,
        scratch_shapes=scratch,
        compiler_params=pltpu.CompilerParams(collective_id=ident, has_side_effects=True, vmem_limit_bytes=62 * 2**20),
        cost_estimate=pl.CostEstimate(flops=10 * packed * d_model * d_ff, bytes_accessed=4 * packed * d_ff, transcendentals=packed * d_ff),
        name=f"grads{packed}",
    )(table, x, dy, w1, w2)


def finish_kernel(dims, len_ref, o1_hbm, o2_hbm, dxp_hbm, g1_hbm, g2_hbm, dx_hbm, c1_v, c2_v, dx_v, starts, c_in, c_out, dx_in, dx_out):
    tokens, d_model, d_ff, seq = dims
    seqs = tokens // seq
    steps, slots, ahead = 2 * seqs, 6, 3
    n1, n2 = d_model // steps, d_ff // steps

    def rows(b, n):
        return pl.ds(pl.multiple_of(b * n, 16), n)

    def carry_in(b):
        slot = lax.rem(b, slots)
        return (pltpu.make_async_copy(o1_hbm.at[rows(b, n1), :], c1_v.at[slot], c_in.at[slot, 0]),
                pltpu.make_async_copy(o2_hbm.at[rows(b, n2), :], c2_v.at[slot], c_in.at[slot, 1]))

    def carry_out(b):
        slot = lax.rem(b, slots)
        return (pltpu.make_async_copy(c1_v.at[slot], g1_hbm.at[rows(b, n1), :], c_out.at[slot, 0]),
                pltpu.make_async_copy(c2_v.at[slot], g2_hbm.at[rows(b, n2), :], c_out.at[slot, 1]))

    starts[0] = jnp.int32(0)
    for s in range(1, seqs):
        starts[s] = starts[s - 1] + granules(len_ref, s - 1)

    def unpack_in(s, act):
        slot, half = lax.rem(s, slots), seq // 2
        for n in range(2):
            at = pl.ds(pl.multiple_of(starts[s] * GRANULE, GRANULE) + n * half, half)

            @pl.when(length(len_ref, s) > n * half)
            def _():
                act(pltpu.make_async_copy(dxp_hbm.at[at, :], dx_v.at[slot, pl.ds(n * half, half), :], dx_in.at[slot, n]))

    def unpack_out(s):
        slot = lax.rem(s, slots)
        return pltpu.make_async_copy(dx_v.at[slot], dx_hbm.at[rows(s, seq), :], dx_out.at[slot])

    for b in range(ahead):
        for copy in carry_in(b):
            copy.start()
    for s in range(2):
        unpack_in(s, lambda copy: copy.start())

    @pl.loop(0, steps)
    def _(b):
        with jax.named_scope("carry_in_wait"):
            for copy in carry_in(b):
                copy.wait()
        for copy in carry_out(b):
            copy.start()

        @pl.when(b >= ahead)
        def _():
            for copy in carry_out(b - ahead):
                copy.wait()

        @pl.when(b + ahead < steps)
        def _():
            for copy in carry_in(b + ahead):
                copy.start()

        s = lax.div(b, 2)

        @pl.when(lax.rem(b, 2) == 1)
        def _():
            unpack_in(s, lambda copy: copy.wait())
            slot = lax.rem(s, slots)
            keep = lax.broadcasted_iota(jnp.int32, (seq, d_model), 0) < length(len_ref, s)
            dx_v[slot] = jnp.where(keep, dx_v[slot], jnp.zeros((), bf16))
            unpack_out(s).start()

            @pl.when(s >= 2)
            def _():
                unpack_out(s - 2).wait()

            @pl.when(s + 2 < seqs)
            def _():
                unpack_in(s + 2, lambda copy: copy.start())

    for b in range(steps - ahead, steps):
        for copy in carry_out(b):
            copy.wait()
    for s in (seqs - 2, seqs - 1):
        unpack_out(s).wait()


def finish_call(dims, lens, o1, o2, dxp):
    tokens, d_model, d_ff, seq = dims
    steps = 2 * (tokens // seq)
    dma = pltpu.SemaphoreType.DMA
    return pl.pallas_call(
        functools.partial(finish_kernel, dims),
        out_shape=[jax.ShapeDtypeStruct((d_model, d_ff), bf16), jax.ShapeDtypeStruct((d_ff, d_model), bf16),
                   jax.ShapeDtypeStruct((tokens, d_model), bf16)],
        in_specs=[SMEM] + [ANY] * 3,
        out_specs=[ANY] * 3,
        scratch_shapes=[
            pltpu.VMEM((6, d_model // steps, d_ff), bf16), pltpu.VMEM((6, d_ff // steps, d_model), bf16), pltpu.VMEM((6, seq, d_model), bf16),
            pltpu.SMEM((tokens // seq,), jnp.int32), dma((6, 2)), dma((6, 2)), dma((6, 2)), dma((6,))],
        compiler_params=pltpu.CompilerParams(vmem_limit_bytes=63 * 2**20),
        cost_estimate=pl.CostEstimate(flops=tokens * d_model, bytes_accessed=8 * d_model * d_ff, transcendentals=0),
        name="finish",
    )(lens, o1, o2, dxp)


def solution(mesh):
    def local_step(x_loc, dy_loc, len_loc, w_in, w_out):
        layers, d_model, d_ff = w_in.shape
        rows, seq, _ = x_loc.shape
        tokens = rows * seq
        lens = len_loc.T
        x, dy = x_loc.reshape(tokens, d_model), dy_loc.reshape(tokens, d_model)
        w1, w2 = w_in.reshape(d_model, d_ff), w_out.reshape(d_ff, d_model)
        sizes = tuple(tokens * n // 16 for n in (12, 13, 16))

        def branch(n):
            def run(lens, table, x, dy, w1, w2):
                packed = sizes[n]
                o1, o2, _, dxp = grads_call((tokens, d_model, d_ff, seq, packed, tokens // 16), n + 1, table, x, dy, w1, w2)
                return finish_call((tokens, d_model, d_ff, seq), lens, o1, o2, dxp)

            return run

        size, table = most_call(lens, seq, sizes)
        g1, g2, dx = lax.switch(size[0, 0], [branch(n) for n in range(len(sizes))], lens, table, x, dy, w1, w2)
        return g1.reshape(layers, d_model, d_ff), g2.reshape(layers, d_ff, d_model), dx.reshape(rows, seq, d_model)

    return jax.shard_map(local_step, mesh=mesh, in_specs=(P("data"), P("data"), P("data"), P(), P()), out_specs=(P(), P(), P("data")), check_vma=False)
```

```python
import functools
import math
import jax
import jax.numpy as jnp
from jax import lax
from jax.experimental import pallas as pl
from jax.experimental.pallas import tpu as pltpu
from jax.sharding import PartitionSpec as P

GELU_SCALE = math.sqrt(2.0 / math.pi)
GELU_CUBIC = 0.044715
MESH = pl.DeviceIdType.MESH
NT = (((1,), (1,)), ((), ()))
TN = (((0,), (0,)), ((), ()))
f32 = jnp.float32
bf16 = jnp.bfloat16
ANY = pl.BlockSpec(memory_space=pl.ANY)
SMEM = pl.BlockSpec(memory_space=pltpu.SMEM)

CHUNK = 256
GRANULE = 16
BLOCKS = 8
STAGES = 5
WEIGHT = {"c": 1, "x": 2, "y": 4, "z": 8, "w": 16}
EARLY = ((1, 1), (8, 5))
MIDDLE = ((3, 2), (5, 3), (7, 4), (10, 6))
LATE = ((0, 0), (2, 1), (4, 2), (6, 3), (9, 5))
CARRY, GROUP = 16, 4
TAIL = 2 * STAGES
HELD = 4


def gelu_both(u):
    sq = u * u
    half = 0.5 + 0.5 * jnp.tanh(u * (GELU_SCALE + (GELU_SCALE * GELU_CUBIC) * sq))
    value = u * half
    return value, half + (value * (1.0 - half)) * (2.0 * GELU_SCALE + (6.0 * GELU_SCALE * GELU_CUBIC) * sq)


def part_table(d_model):
    rows = 1024 if d_model == 1280 else d_model // 2
    cols = 768 if d_model == 1280 else d_model // 2
    return (
        (0, 0, rows, 0, CHUNK, "cxyzw"),
        (0, rows, d_model - rows, 0, CHUNK, "czxyw"),
        (1, 0, CHUNK, 0, cols, "cyxzw"),
        (1, 0, CHUNK, cols, d_model - cols, "czyxw"),
    )


def place():
    me = lax.axis_index("data")
    bit = {k: lax.rem(lax.div(me, v), 2) for k, v in WEIGHT.items()}
    return me, bit, {k: me + v * (1 - 2 * bit[k]) for k, v in WEIGHT.items()}


def granules(len_ref, s):
    return lax.div(length(len_ref, s) + (GRANULE - 1), GRANULE)


def length(len_ref, s):
    return len_ref[lax.rem(s, 2), lax.div(s, 2)]


def most_kernel(seqs, seq, sizes, len_ref, out_ref, table_ref, mine, plane, best, depth, send, recv):
    me, bit, _ = place()

    def other(d, names):
        return me + sum(WEIGHT[k] * (1 - 2 * bit[k]) for n, k in enumerate(names) if d >> n & 1)

    counts = [granules(len_ref, s) for s in range(seqs)]
    starts = [sum(counts[:s], jnp.int32(0)) for s in range(seqs + 1)]
    mine[...] = jnp.full(mine.shape, (starts[seqs] * GRANULE).astype(f32))
    barrier = pltpu.get_barrier_semaphore()
    near = [other(d, "cxy") for d in range(1, 8)]
    far = [other(d, "zw") for d in range(1, 4)]
    for device in near + far:
        pl.semaphore_signal(barrier, inc=1, device_id=(device,), device_id_type=MESH)
    pl.semaphore_wait(barrier, len(near) + len(far))

    def exchange(source, slots, devices, first):
        copies = [pltpu.make_async_remote_copy(source, slots.at[n], send.at[first + n], recv.at[first + n], device_id=(device,), device_id_type=MESH)
                  for n, device in enumerate(devices)]
        for copy in copies:
            copy.start()
        return copies

    def largest_of(copies, source, slots):
        for copy in copies:
            copy.wait()
        return functools.reduce(jnp.maximum, [slots[n] for n in range(len(copies))], source[...])

    first = exchange(mine, plane, near, 0)
    k = lax.broadcasted_iota(jnp.int32, (2, 128), 0) * 128 + lax.broadcasted_iota(jnp.int32, (2, 128), 1)
    source, left = k, length(len_ref, 0) - k * GRANULE
    for s in range(1, seqs):
        past = k >= starts[s]
        source = jnp.where(past, k - starts[s] + s * (seq // GRANULE), source)
        left = jnp.where(past, length(len_ref, s) - (k - starts[s]) * GRANULE, left)
    inside = k < starts[seqs]
    table_ref[0:2, :] = jnp.where(inside, source, 0)
    table_ref[2:4, :] = jnp.where(inside, left, 0)
    best[...] = largest_of(first, mine, plane)
    largest = largest_of(exchange(best, depth, far, len(near)), best, depth)
    out_ref[...] = sum((largest > size).astype(jnp.int32) for size in sizes[:-1])


def most_call(lens, seq, sizes):
    tile = (8, 128)
    dma = pltpu.SemaphoreType.DMA
    return pl.pallas_call(
        functools.partial(most_kernel, lens.size, seq, sizes),
        out_shape=[jax.ShapeDtypeStruct(tile, jnp.int32), jax.ShapeDtypeStruct((4, 128), jnp.int32)],
        in_specs=[SMEM],
        out_specs=[pl.BlockSpec(memory_space=pltpu.VMEM)] * 2,
        scratch_shapes=[pltpu.VMEM(tile, f32), pltpu.VMEM((7, *tile), f32), pltpu.VMEM(tile, f32), pltpu.VMEM((3, *tile), f32), dma((10,)), dma((10,))],
        compiler_params=pltpu.CompilerParams(collective_id=0, has_side_effects=True),
        name="most",
    )(lens)


def grads_kernel(dims, table_ref, x_hbm, dy_hbm, w1_hbm, w2_hbm, o1_hbm, o2_hbm, du_hbm, dx_hbm, *scratch):
    tokens, d_model, d_ff, seq, packed, dx_block, near = dims
    seqs = tokens // seq
    chunks = d_ff // CHUNK
    block = packed // BLOCKS
    span = BLOCKS // 2 if packed < tokens else 2
    cuts = 1 if packed < tokens else 2
    parts = part_table(d_model)
    (x_v, g_v, w1_v, w2_v, u0, u1, d0, d1, a_v, du_v, p1, p2, dub_v, dx_v) = scratch[:14]
    recv = [scratch[14 + 5 * k : 19 + 5 * k] for k in range(4)]
    (x_sem, g_sem, w_sem, du_sem, own_sem, dub_sem, dx_sem, g_out_sem, rs_send, rs_recv, ag_send, ag_recv) = scratch[34:]

    _, bit, peer = place()
    for s in range(seqs):
        at = pl.ds(s * seq, seq)
        pltpu.make_async_copy(x_hbm.at[at, :], x_v.at[at, :], x_sem.at[s]).start()

    barrier = pltpu.get_barrier_semaphore()
    for k in WEIGHT:
        pl.semaphore_signal(barrier, inc=1, device_id=(peer[k],), device_id_type=MESH)
    pl.semaphore_wait(barrier, STAGES)

    region, given = [], []
    for (_, r0, nr, c0, nc, order) in parts:
        mine, away = [(r0, nr, c0, nc)], []
        for s, name in enumerate(order):
            row, rows, col, cols = mine[-1]
            if s < STAGES - 1:
                half = rows // 2
                mine.append((row + bit[name] * half, half, col, cols))
                away.append((row + (1 - bit[name]) * half, half, col, cols))
            else:
                half = cols // 2
                mine.append((row, rows, col + bit[name] * half, half))
                away.append((row, rows, col + (1 - bit[name]) * half, half))
        region.append(mine)
        given.append(away)

    def cut(r):
        row, rows, col, cols = r
        row = row if isinstance(row, int) else pl.multiple_of(row, 16)
        col = col if isinstance(col, int) else pl.multiple_of(col, 128)
        return pl.ds(row, rows), pl.ds(col, cols)

    def partial(k, i, r):
        rows, cols = cut(r)
        return (p1, p2)[parts[k][0]].at[lax.rem(i, HELD), rows, cols]

    def whole(k, i, r):
        row, rows, col, cols = r
        if parts[k][0] == 0:
            return o1_hbm.at[cut((row, rows, i * CHUNK + col, cols))]
        return o2_hbm.at[cut((i * CHUNK + row, rows, col, cols))]

    def reduce_copy(k, s, i):
        slot = lax.rem(i, 2)
        return pltpu.make_async_remote_copy(
            src_ref=partial(k, i, given[k][s]), dst_ref=recv[k][s].at[slot],
            send_sem=rs_send.at[slot, s, k], recv_sem=rs_recv.at[slot, s, k],
            device_id=(peer[parts[k][5][s]],), device_id_type=MESH)

    def gather_copy(k, s, i):
        slot = lax.rem(i, 2)
        r = region[k][s + 1]
        return pltpu.make_async_remote_copy(
            src_ref=partial(k, i, r) if s == STAGES - 1 else whole(k, i, r), dst_ref=whole(k, i, r),
            send_sem=ag_send.at[slot, s, k], recv_sem=ag_recv.at[slot, s, k],
            device_id=(peer[parts[k][5][s]],), device_id_type=MESH)

    def own_copy(k, i):
        r = region[k][STAGES]
        return pltpu.make_async_copy(partial(k, i, r), whole(k, i, r), own_sem.at[k])

    def event(e, i):
        for k in range(4):
            if 1 <= e <= STAGES:
                reduce_copy(k, e - 1, i).wait()
                rows, cols = cut(region[k][e])
                ref, slot = (p1, p2)[parts[k][0]], lax.rem(i, HELD)
                ref[slot, rows, cols] = ref[slot, rows, cols] + recv[k][e - 1][lax.rem(i, 2)]
            if e < STAGES:
                reduce_copy(k, e, i).start()
            if e == STAGES:
                own_copy(k, i).start()
            if e > STAGES:
                gather_copy(k, 2 * STAGES - e, i).wait()
                if e == STAGES + 1:
                    own_copy(k, i).wait()
            if STAGES <= e < 2 * STAGES:
                gather_copy(k, 2 * STAGES - 1 - e, i).start()

    def weights(i):
        slot = lax.rem(i, 2)
        at = pl.ds(pl.multiple_of(i * CHUNK, CHUNK), CHUNK)
        return (pltpu.make_async_copy(w1_hbm.at[:, at], w1_v.at[:, at], w_sem.at[slot, 0]),
                pltpu.make_async_copy(w2_hbm.at[at, :], w2_v.at[slot], w_sem.at[slot, 1]))

    def rows_of(b):
        return pl.ds(pl.multiple_of(b * block, 16), block)

    def dots(b, i, u, d):
        w1 = w1_v[:, pl.ds(pl.multiple_of(i * CHUNK, CHUNK), CHUNK)]
        u[...] = jnp.dot(x_v[rows_of(b), :], w1, preferred_element_type=f32).astype(bf16)
        d[...] = lax.dot_general(g_v[rows_of(b), :], w2_v[lax.rem(i, 2)], NT, preferred_element_type=f32)

    def pointwise(b, u, d):
        a, slope = gelu_both(u[...].astype(f32))
        a_v[rows_of(b), :] = a.astype(bf16)
        du_v[rows_of(b), :] = (d[...] * slope).astype(bf16)

    def du_out(i):
        return pltpu.make_async_copy(du_v, du_hbm.at[pl.ds(0, packed), pl.ds(pl.multiple_of(i * CHUNK, CHUNK), CHUNK)], du_sem)

    def dx_rows(q):
        return pl.ds(pl.multiple_of(q * dx_block, 16), dx_block)

    def du_in(q):
        slot = lax.rem(q, 2)
        return pltpu.make_async_copy(du_hbm.at[dx_rows(q), :], dub_v.at[slot], dub_sem.at[slot])

    def dx_out(q):
        slot = lax.rem(q, 2)
        return pltpu.make_async_copy(dx_v.at[slot], dx_hbm.at[dx_rows(q), :], dx_sem.at[slot])

    for s in range(seqs):
        at = pl.ds(s * seq, seq)
        pltpu.make_async_copy(dy_hbm.at[at, :], g_v.at[at, :], g_sem.at[s]).start()
    for copy in weights(0):
        copy.start()
    with jax.named_scope("wait_x"):
        for s in range(seqs):
            at = pl.ds(s * seq, seq)
            pltpu.make_async_copy(x_hbm.at[at, :], x_v.at[at, :], x_sem.at[s]).wait()

    group = 4 if packed % (4 * GRANULE) == 0 else 2

    def granule_rows(k):
        return pl.ds(pl.multiple_of(k * GRANULE, GRANULE), GRANULE)

    def source_rows(k):
        return pl.ds(table_ref[lax.div(k, 128), lax.rem(k, 128)] * GRANULE, GRANULE)

    @pl.loop(0, packed // GRANULE // group)
    def _(n):
        rows = [x_v[source_rows(n * group + k), :] for k in range(group)]
        for k in range(group):
            x_v[granule_rows(n * group + k), :] = rows[k]

    with jax.named_scope("wait_g"):
        for s in range(seqs):
            at = pl.ds(s * seq, seq)
            pltpu.make_async_copy(dy_hbm.at[at, :], g_v.at[at, :], g_sem.at[s]).wait()

    @pl.loop(0, packed // GRANULE // group)
    def _(n):
        rows = [g_v[source_rows(n * group + k), :] for k in range(group)]
        for k in range(group):
            at = n * group + k
            keep = lax.broadcasted_iota(jnp.int32, (GRANULE, d_model), 0) < table_ref[2 + lax.div(at, 128), lax.rem(at, 128)]
            g_v[granule_rows(at), :] = jnp.where(keep, rows[k], jnp.zeros((), bf16))

    far = pl.ds(near * dx_block, packed - near * dx_block)
    g_out = pltpu.make_async_copy(g_v.at[far, :], dx_hbm.at[far, :], g_out_sem)
    g_out.start()
    with jax.named_scope("wait_w"):
        for copy in weights(0):
            copy.wait()

    @pl.loop(0, 2)
    def _(n):
        at = pl.ds(pl.multiple_of(n * (block // 2), 16), block // 2)
        u0[at, :] = jnp.dot(x_v[at, :], w1_v[:, 0:CHUNK], preferred_element_type=f32).astype(bf16)
        d0[at, :] = lax.dot_general(g_v[at, :], w2_v[0], NT, preferred_element_type=f32)


    def events(i, which):
        for e, lag in which:
            j = i - lag

            @pl.when((j >= 0) & (j < chunks))
            def _():
                with jax.named_scope(f"event{e}"):
                    event(e, j)

    @pl.loop(0, chunks)
    def _(i):
        @pl.when(i + 1 < chunks)
        def _():
            for copy in weights(i + 1):
                copy.start()

        @pl.when(i > 0)
        def _():
            du_out(i - 1).wait()

        @pl.loop(0, BLOCKS // span)
        def _(n):
            last = n == BLOCKS // span - 1

            @pl.when(last & (i + 1 < chunks))
            def _():
                for copy in weights(i + 1):
                    copy.wait()

            b = n * span
            after = jnp.minimum(i + last.astype(jnp.int32), chunks - 1)
            sets = ((u0, d0), (u1, d1))
            with jax.named_scope("tokens"):
                for k in range(span):
                    pointwise(b + k, *sets[k % 2])
                    if k < span - 1:
                        dots(b + k + 1, i, *sets[(k + 1) % 2])
                    else:
                        dots(lax.rem(b + span, BLOCKS), after, *sets[0])

            @pl.when(n == BLOCKS // span // 2 - 1)
            def _():
                events(i, EARLY)

        du_out(i).start()
        events(i, MIDDLE)
        slot = lax.rem(i, HELD)
        with jax.named_scope("dw"):
            @pl.loop(0, cuts)
            def _(n):
                n2, n1 = CHUNK // cuts, d_model // cuts
                at2, at1 = pl.ds(pl.multiple_of(n * n2, n2), n2), pl.ds(pl.multiple_of(n * n1, n1), n1)
                p2[slot, at2, :] = lax.dot_general(a_v[:, at2], g_v[:packed, :], TN, preferred_element_type=f32).astype(bf16)
                p1[slot, at1, :] = lax.dot_general(x_v[:packed, at1], du_v[...], TN, preferred_element_type=f32).astype(bf16)

        @pl.when(i == chunks - 1)
        def _():
            du_out(i).wait()
            du_in(0).start()

        events(i, LATE)

    @pl.loop(0, TAIL)
    def _(q):
        @pl.when(q < near)
        def _():
            slot = lax.rem(q, 2)

            @pl.when(q + 1 < near)
            def _():
                du_in(q + 1).start()

            @pl.when(q > 1)
            def _():
                dx_out(q - 2).wait()

            with jax.named_scope("dx"):
                du_in(q).wait()
                dx_v[slot] = (g_v[dx_rows(q), :].astype(f32) + lax.dot_general(dub_v[slot], w1_v[...], NT, preferred_element_type=f32)).astype(bf16)
            dx_out(q).start()

        seen = {lag: max(e for e, behind in EARLY + MIDDLE + LATE if behind <= lag) for lag in range(6)}
        for e in reversed(range(1, TAIL + 1)):
            steps = {e - 1 - last: lag for lag, last in seen.items() if last < e}
            lag = sum(jnp.where(q == step, behind, 0) for step, behind in steps.items())
            j = chunks - 1 - lag

            @pl.when(functools.reduce(jnp.logical_or, [q == step for step in steps]) & (j >= 0))
            def _():
                with jax.named_scope(f"event{e}"):
                    event(e, j)

    dx_out(near - 2).wait()
    dx_out(near - 1).wait()
    g_out.wait()


def grads_call(dims, ident, table, x, dy, w1, w2):
    tokens, d_model, d_ff, seq, packed, dx_block, near = dims
    scratch = [
        pltpu.VMEM((tokens, d_model), bf16), pltpu.VMEM((tokens, d_model), bf16),
        pltpu.VMEM((d_model, d_ff), bf16), pltpu.VMEM((2, CHUNK, d_model), bf16),
        pltpu.VMEM((packed // BLOCKS, CHUNK), bf16), pltpu.VMEM((packed // BLOCKS, CHUNK), bf16),
        pltpu.VMEM((packed // BLOCKS, CHUNK), f32), pltpu.VMEM((packed // BLOCKS, CHUNK), f32),
        pltpu.VMEM((packed, CHUNK), bf16), pltpu.VMEM((packed, CHUNK), bf16),
        pltpu.VMEM((HELD, d_model, CHUNK), bf16), pltpu.VMEM((HELD, CHUNK, d_model), bf16),
        pltpu.VMEM((2, dx_block, d_ff), bf16), pltpu.VMEM((2, dx_block, d_model), bf16),
    ]
    for (_, _, rows, _, cols, _) in part_table(d_model):
        for s in range(STAGES):
            last = s == STAGES - 1
            scratch.append(pltpu.VMEM((2, rows >> (4 if last else s + 1), cols // 2 if last else cols), bf16))
    dma = pltpu.SemaphoreType.DMA
    scratch += [dma((tokens // seq,)), dma((tokens // seq,)), dma((2, 2)), dma, dma((4,)), dma((2,)), dma((2,)), dma]
    scratch += [dma((2, STAGES, 4))] * 4
    return pl.pallas_call(
        functools.partial(grads_kernel, dims),
        out_shape=[jax.ShapeDtypeStruct((d_model, d_ff), bf16), jax.ShapeDtypeStruct((d_ff, d_model), bf16),
                   jax.ShapeDtypeStruct((tokens, d_ff), bf16), jax.ShapeDtypeStruct((tokens, d_model), bf16)],
        in_specs=[SMEM] + [ANY] * 4,
        out_specs=[ANY] * 4,
        scratch_shapes=scratch,
        compiler_params=pltpu.CompilerParams(collective_id=ident, has_side_effects=True, vmem_limit_bytes=62 * 2**20),
        cost_estimate=pl.CostEstimate(flops=10 * packed * d_model * d_ff, bytes_accessed=4 * packed * d_ff, transcendentals=packed * d_ff),
        name=f"grads{packed}",
    )(table, x, dy, w1, w2)


def finish_kernel(dims, len_ref, o1_hbm, o2_hbm, du_hbm, dxp_hbm, w1_hbm, g1_hbm, g2_hbm, dx_hbm,
                  w1_v, dx_v, du_v, out_v, c1_v, c2_v, starts, w_sem, dx_sem, du_sem, out_sem, c_in, c_out):
    tokens, d_model, d_ff, seq, block, near = dims
    seqs = tokens // seq
    n1, n2 = d_model // CARRY, d_ff // CARRY
    blocks = tokens // block - near
    rounds = max(blocks, CARRY // GROUP + 1)

    def rows(b, n):
        return pl.ds(pl.multiple_of(b * n, 16), n)

    def carry_in(b):
        slot = lax.rem(b, 2 * GROUP)
        return (pltpu.make_async_copy(o1_hbm.at[rows(b, n1), :], c1_v.at[slot], c_in.at[slot, 0]),
                pltpu.make_async_copy(o2_hbm.at[rows(b, n2), :], c2_v.at[slot], c_in.at[slot, 1]))

    def carry_out(b):
        slot = lax.rem(b, 2 * GROUP)
        return (pltpu.make_async_copy(c1_v.at[slot], g1_hbm.at[rows(b, n1), :], c_out.at[slot, 0]),
                pltpu.make_async_copy(c2_v.at[slot], g2_hbm.at[rows(b, n2), :], c_out.at[slot, 1]))

    starts[0] = jnp.int32(0)
    for s in range(seqs):
        starts[s + 1] = starts[s] + granules(len_ref, s)
    total = starts[seqs] * GRANULE

    def valid(n):
        return (n < blocks) & ((near + n) * block < total)

    def du_in(n):
        slot = lax.rem(n, 2)
        return pltpu.make_async_copy(du_hbm.at[rows(near + n, block), :], du_v.at[slot], du_sem.at[slot])

    def unpacked(s, slot):
        return pltpu.make_async_copy(out_v.at[slot], dx_hbm.at[rows(s, seq), :], out_sem.at[slot])

    load_w = pltpu.make_async_copy(w1_hbm, w1_v, w_sem)
    load_dx = pltpu.make_async_copy(dxp_hbm, dx_v.at[pl.ds(0, tokens), :], dx_sem)
    load_w.start()

    @pl.when(valid(0))
    def _():
        du_in(0).start()

    load_dx.start()
    for b in range(GROUP):
        for copy in carry_in(b):
            copy.start()
    load_dx.wait()

    @pl.loop(0, rounds)
    def _(n):
        with jax.named_scope("carry"):
            @pl.loop(0, GROUP)
            def _(k):
                b = n * GROUP + k

                @pl.when(b < CARRY)
                def _():
                    for copy in carry_in(b):
                        copy.wait()
                    for copy in carry_out(b):
                        copy.start()

                @pl.when((b >= GROUP) & (b < CARRY + GROUP))
                def _():
                    for copy in carry_out(b - GROUP):
                        copy.wait()

                @pl.when(b + GROUP < CARRY)
                def _():
                    for copy in carry_in(b + GROUP):
                        copy.start()

        @pl.when(valid(n + 1))
        def _():
            du_in(n + 1).start()

        @pl.when(n == 0)
        def _():
            load_w.wait()

        @pl.when(valid(n))
        def _():
            with jax.named_scope("dx"):
                du_in(n).wait()
                at = rows(near + n, block)
                dx_v[at, :] = (dx_v[at, :].astype(f32) + lax.dot_general(du_v[lax.rem(n, 2)], w1_v[...], NT, preferred_element_type=f32)).astype(bf16)

        done = jnp.where(n == rounds - 1, tokens, (near + n + 1) * block)
        before = jnp.where(n == 0, 0, (near + n) * block)

        @pl.loop(0, seqs)
        def _(s):
            end = starts[s + 1] * GRANULE

            @pl.when((end > before) & (end <= done))
            def _():
                slot = lax.rem(s, 4)

                @pl.when(s >= 4)
                def _():
                    unpacked(s - 4, slot).wait()

                keep = lax.broadcasted_iota(jnp.int32, (seq, d_model), 0) < length(len_ref, s)
                rows_in = dx_v[pl.ds(pl.multiple_of(starts[s] * GRANULE, GRANULE), seq), :]
                out_v[slot] = jnp.where(keep, rows_in, jnp.zeros((), bf16))
                unpacked(s, slot).start()

    for s in range(seqs - 4, seqs):
        unpacked(s, s % 4).wait()


def finish_call(dims, lens, o1, o2, du, dxp, w1):
    tokens, d_model, d_ff, seq, block, _ = dims
    dma = pltpu.SemaphoreType.DMA
    slots = 2 * GROUP
    return pl.pallas_call(
        functools.partial(finish_kernel, dims),
        out_shape=[jax.ShapeDtypeStruct((d_model, d_ff), bf16), jax.ShapeDtypeStruct((d_ff, d_model), bf16),
                   jax.ShapeDtypeStruct((tokens, d_model), bf16)],
        in_specs=[SMEM] + [ANY] * 5,
        out_specs=[ANY] * 3,
        scratch_shapes=[
            pltpu.VMEM((d_model, d_ff), bf16), pltpu.VMEM((tokens + seq, d_model), bf16), pltpu.VMEM((2, block, d_ff), bf16),
            pltpu.VMEM((4, seq, d_model), bf16), pltpu.VMEM((slots, d_model // CARRY, d_ff), bf16), pltpu.VMEM((slots, d_ff // CARRY, d_model), bf16),
            pltpu.SMEM((tokens // seq + 1,), jnp.int32), dma, dma, dma((2,)), dma((4,)), dma((slots, 2)), dma((slots, 2))],
        compiler_params=pltpu.CompilerParams(vmem_limit_bytes=63 * 2**20),
        cost_estimate=pl.CostEstimate(flops=tokens * d_model, bytes_accessed=8 * d_model * d_ff, transcendentals=0),
        name="finish",
    )(lens, o1, o2, du, dxp, w1)


def solution(mesh):
    def local_step(x_loc, dy_loc, len_loc, w_in, w_out):
        layers, d_model, d_ff = w_in.shape
        rows, seq, _ = x_loc.shape
        tokens = rows * seq
        lens = len_loc.T
        x, dy = x_loc.reshape(tokens, d_model), dy_loc.reshape(tokens, d_model)
        w1, w2 = w_in.reshape(d_model, d_ff), w_out.reshape(d_ff, d_model)
        sizes = tuple(tokens * n // 16 for n in (12, 13, 16))

        block = tokens // 16
        near = sizes[0] // block // 2

        def branch(n):
            def run(table, x, dy, w1, w2):
                return grads_call((tokens, d_model, d_ff, seq, sizes[n], block, near), n + 1, table, x, dy, w1, w2)

            return run

        size, table = most_call(lens, seq, sizes)
        o1, o2, du, dxp = lax.switch(size[0, 0], [branch(n) for n in range(len(sizes))], table, x, dy, w1, w2)
        g1, g2, dx = finish_call((tokens, d_model, d_ff, seq, block, near), lens, o1, o2, du, dxp, w1)
        return g1.reshape(layers, d_model, d_ff), g2.reshape(layers, d_ff, d_model), dx.reshape(rows, seq, d_model)

    return jax.shard_map(local_step, mesh=mesh, in_specs=(P("data"), P("data"), P("data"), P(), P()), out_specs=(P(), P(), P("data")), check_vma=False)
```

```python
import functools
import math
import jax
import jax.numpy as jnp
from jax import lax
from jax.experimental import pallas as pl
from jax.experimental.pallas import tpu as pltpu
from jax.sharding import PartitionSpec as P

GELU_SCALE = math.sqrt(2.0 / math.pi)
GELU_CUBIC = 0.044715
MESH = pl.DeviceIdType.MESH
NT = (((1,), (1,)), ((), ()))
TN = (((0,), (0,)), ((), ()))
f32 = jnp.float32
bf16 = jnp.bfloat16
ANY = pl.BlockSpec(memory_space=pl.ANY)
SMEM = pl.BlockSpec(memory_space=pltpu.SMEM)

CHUNK = 256
GRANULE = 16
BLOCKS = 8
STAGES = 5
WEIGHT = {"c": 1, "x": 2, "y": 4, "z": 8, "w": 16}
EARLY = ((1, 1), (8, 5))
MIDDLE = ((3, 2), (5, 3), (7, 4), (10, 6))
LATE = ((0, 0), (2, 1), (4, 2), (6, 3), (9, 5))
TAIL = 2 * STAGES
HELD = 4


def gelu_both(u):
    sq = u * u
    half = 0.5 + 0.5 * jnp.tanh(u * (GELU_SCALE + (GELU_SCALE * GELU_CUBIC) * sq))
    value = u * half
    return value, half + (value * (1.0 - half)) * (2.0 * GELU_SCALE + (6.0 * GELU_SCALE * GELU_CUBIC) * sq)


def part_table(d_model):
    rows = 1024 if d_model == 1280 else d_model // 2
    cols = 768 if d_model == 1280 else d_model // 2
    return (
        (0, 0, rows, 0, CHUNK, "cxyzw"),
        (0, rows, d_model - rows, 0, CHUNK, "czxyw"),
        (1, 0, CHUNK, 0, cols, "cyxzw"),
        (1, 0, CHUNK, cols, d_model - cols, "czyxw"),
    )


def place():
    me = lax.axis_index("data")
    bit = {k: lax.rem(lax.div(me, v), 2) for k, v in WEIGHT.items()}
    return me, bit, {k: me + v * (1 - 2 * bit[k]) for k, v in WEIGHT.items()}


def granules(len_ref, s):
    return lax.div(length(len_ref, s) + (GRANULE - 1), GRANULE)


def length(len_ref, s):
    return len_ref[lax.rem(s, 2), lax.div(s, 2)]


def most_kernel(seqs, seq, sizes, len_ref, out_ref, table_ref, mine, plane, best, depth, send, recv):
    me, bit, _ = place()

    def other(d, names):
        return me + sum(WEIGHT[k] * (1 - 2 * bit[k]) for n, k in enumerate(names) if d >> n & 1)

    counts = [granules(len_ref, s) for s in range(seqs)]
    starts = [sum(counts[:s], jnp.int32(0)) for s in range(seqs + 1)]
    mine[...] = jnp.full(mine.shape, (starts[seqs] * GRANULE).astype(f32))
    barrier = pltpu.get_barrier_semaphore()
    near = [other(d, "cxy") for d in range(1, 8)]
    far = [other(d, "zw") for d in range(1, 4)]
    for device in near + far:
        pl.semaphore_signal(barrier, inc=1, device_id=(device,), device_id_type=MESH)
    pl.semaphore_wait(barrier, len(near) + len(far))

    def exchange(source, slots, devices, first):
        copies = [pltpu.make_async_remote_copy(source, slots.at[n], send.at[first + n], recv.at[first + n], device_id=(device,), device_id_type=MESH)
                  for n, device in enumerate(devices)]
        for copy in copies:
            copy.start()
        return copies

    def largest_of(copies, source, slots):
        for copy in copies:
            copy.wait()
        return functools.reduce(jnp.maximum, [slots[n] for n in range(len(copies))], source[...])

    first = exchange(mine, plane, near, 0)
    k = lax.broadcasted_iota(jnp.int32, (2, 128), 0) * 128 + lax.broadcasted_iota(jnp.int32, (2, 128), 1)
    source, left = k, length(len_ref, 0) - k * GRANULE
    for s in range(1, seqs):
        past = k >= starts[s]
        source = jnp.where(past, k - starts[s] + s * (seq // GRANULE), source)
        left = jnp.where(past, length(len_ref, s) - (k - starts[s]) * GRANULE, left)
    inside = k < starts[seqs]
    table_ref[0:2, :] = jnp.where(inside, source, 0)
    table_ref[2:4, :] = jnp.where(inside, left, 0)
    best[...] = largest_of(first, mine, plane)
    largest = largest_of(exchange(best, depth, far, len(near)), best, depth)
    out_ref[0, 0] = jnp.max(sum((largest > size).astype(jnp.int32) for size in sizes[:-1]))


def most_call(lens, seq, sizes):
    tile = (8, 128)
    dma = pltpu.SemaphoreType.DMA
    return pl.pallas_call(
        functools.partial(most_kernel, lens.size, seq, sizes),
        out_shape=[jax.ShapeDtypeStruct((1, 1), jnp.int32), jax.ShapeDtypeStruct((4, 128), jnp.int32)],
        in_specs=[SMEM],
        out_specs=[SMEM, pl.BlockSpec(memory_space=pltpu.VMEM)],
        scratch_shapes=[pltpu.VMEM(tile, f32), pltpu.VMEM((7, *tile), f32), pltpu.VMEM(tile, f32), pltpu.VMEM((3, *tile), f32), dma((10,)), dma((10,))],
        compiler_params=pltpu.CompilerParams(collective_id=0, has_side_effects=True),
        name="most",
    )(lens)


def grads_kernel(dims, table_ref, x_hbm, dy_hbm, w1_hbm, w2_hbm, o1_hbm, o2_hbm, du_hbm, dx_hbm, *scratch):
    tokens, d_model, d_ff, seq, packed, dx_block = dims
    seqs = tokens // seq
    chunks = d_ff // CHUNK
    block = packed // BLOCKS
    dx_blocks = packed // dx_block
    span = BLOCKS // 2 if packed < tokens else 2
    cuts = 1 if packed < tokens else 2
    parts = part_table(d_model)
    (x_v, g_v, w1_v, w2_v, u0, u1, d0, d1, a_v, du_v, p1, p2, dub_v, dx_v) = scratch[:14]
    recv = [scratch[14 + 5 * k : 19 + 5 * k] for k in range(4)]
    (x_sem, g_sem, w_sem, du_sem, own_sem, dub_sem, dx_sem, rs_send, rs_recv, ag_send, ag_recv) = scratch[34:]

    _, bit, peer = place()
    for s in range(seqs):
        at = pl.ds(s * seq, seq)
        pltpu.make_async_copy(x_hbm.at[at, :], x_v.at[at, :], x_sem.at[s]).start()

    barrier = pltpu.get_barrier_semaphore()
    for k in WEIGHT:
        pl.semaphore_signal(barrier, inc=1, device_id=(peer[k],), device_id_type=MESH)
    pl.semaphore_wait(barrier, STAGES)

    region, given = [], []
    for (_, r0, nr, c0, nc, order) in parts:
        mine, away = [(r0, nr, c0, nc)], []
        for s, name in enumerate(order):
            row, rows, col, cols = mine[-1]
            if s < STAGES - 1:
                half = rows // 2
                mine.append((row + bit[name] * half, half, col, cols))
                away.append((row + (1 - bit[name]) * half, half, col, cols))
            else:
                half = cols // 2
                mine.append((row, rows, col + bit[name] * half, half))
                away.append((row, rows, col + (1 - bit[name]) * half, half))
        region.append(mine)
        given.append(away)

    def cut(r):
        row, rows, col, cols = r
        row = row if isinstance(row, int) else pl.multiple_of(row, 16)
        col = col if isinstance(col, int) else pl.multiple_of(col, 128)
        return pl.ds(row, rows), pl.ds(col, cols)

    def partial(k, i, r):
        rows, cols = cut(r)
        return (p1, p2)[parts[k][0]].at[lax.rem(i, HELD), rows, cols]

    def whole(k, i, r):
        row, rows, col, cols = r
        if parts[k][0] == 0:
            return o1_hbm.at[cut((row, rows, i * CHUNK + col, cols))]
        return o2_hbm.at[cut((i * CHUNK + row, rows, col, cols))]

    def reduce_copy(k, s, i):
        slot = lax.rem(i, 2)
        return pltpu.make_async_remote_copy(
            src_ref=partial(k, i, given[k][s]), dst_ref=recv[k][s].at[slot],
            send_sem=rs_send.at[slot, s, k], recv_sem=rs_recv.at[slot, s, k],
            device_id=(peer[parts[k][5][s]],), device_id_type=MESH)

    def gather_copy(k, s, i):
        slot = lax.rem(i, 2)
        r = region[k][s + 1]
        return pltpu.make_async_remote_copy(
            src_ref=partial(k, i, r) if s == STAGES - 1 else whole(k, i, r), dst_ref=whole(k, i, r),
            send_sem=ag_send.at[slot, s, k], recv_sem=ag_recv.at[slot, s, k],
            device_id=(peer[parts[k][5][s]],), device_id_type=MESH)

    def own_copy(k, i):
        r = region[k][STAGES]
        return pltpu.make_async_copy(partial(k, i, r), whole(k, i, r), own_sem.at[k])

    def event(e, i):
        for k in range(4):
            if 1 <= e <= STAGES:
                reduce_copy(k, e - 1, i).wait()
                rows, cols = cut(region[k][e])
                ref, slot = (p1, p2)[parts[k][0]], lax.rem(i, HELD)
                ref[slot, rows, cols] = ref[slot, rows, cols] + recv[k][e - 1][lax.rem(i, 2)]
            if e < STAGES:
                reduce_copy(k, e, i).start()
            if e == STAGES:
                own_copy(k, i).start()
            if e > STAGES:
                gather_copy(k, 2 * STAGES - e, i).wait()
                if e == STAGES + 1:
                    own_copy(k, i).wait()
            if STAGES <= e < 2 * STAGES:
                gather_copy(k, 2 * STAGES - 1 - e, i).start()

    def weights(i):
        slot = lax.rem(i, 2)
        at = pl.ds(pl.multiple_of(i * CHUNK, CHUNK), CHUNK)
        return (pltpu.make_async_copy(w1_hbm.at[:, at], w1_v.at[:, at], w_sem.at[slot, 0]),
                pltpu.make_async_copy(w2_hbm.at[at, :], w2_v.at[slot], w_sem.at[slot, 1]))

    def rows_of(b):
        return pl.ds(pl.multiple_of(b * block, 16), block)

    def dots(b, i, u, d):
        w1 = w1_v[:, pl.ds(pl.multiple_of(i * CHUNK, CHUNK), CHUNK)]
        u[...] = jnp.dot(x_v[rows_of(b), :], w1, preferred_element_type=f32).astype(bf16)
        d[...] = lax.dot_general(g_v[rows_of(b), :], w2_v[lax.rem(i, 2)], NT, preferred_element_type=f32)

    def pointwise(b, u, d):
        a, slope = gelu_both(u[...].astype(f32))
        a_v[rows_of(b), :] = a.astype(bf16)
        du_v[rows_of(b), :] = (d[...] * slope).astype(bf16)

    def du_out(i):
        return pltpu.make_async_copy(du_v, du_hbm.at[pl.ds(0, packed), pl.ds(pl.multiple_of(i * CHUNK, CHUNK), CHUNK)], du_sem)

    def dx_rows(q):
        return pl.ds(pl.multiple_of(q * dx_block, 16), dx_block)

    def du_in(q):
        slot = lax.rem(q, 2)
        return pltpu.make_async_copy(du_hbm.at[dx_rows(q), :], dub_v.at[slot], dub_sem.at[slot])

    def dx_out(q):
        slot = lax.rem(q, 2)
        return pltpu.make_async_copy(dx_v.at[slot], dx_hbm.at[dx_rows(q), :], dx_sem.at[slot])

    for s in range(seqs):
        at = pl.ds(s * seq, seq)
        pltpu.make_async_copy(dy_hbm.at[at, :], g_v.at[at, :], g_sem.at[s]).start()
    for copy in weights(0):
        copy.start()
    with jax.named_scope("wait_x"):
        for s in range(seqs):
            at = pl.ds(s * seq, seq)
            pltpu.make_async_copy(x_hbm.at[at, :], x_v.at[at, :], x_sem.at[s]).wait()

    group = 4 if packed % (4 * GRANULE) == 0 else 2

    def granule_rows(k):
        return pl.ds(pl.multiple_of(k * GRANULE, GRANULE), GRANULE)

    def source_rows(k):
        return pl.ds(table_ref[lax.div(k, 128), lax.rem(k, 128)] * GRANULE, GRANULE)

    @pl.loop(0, packed // GRANULE // group)
    def _(n):
        rows = [x_v[source_rows(n * group + k), :] for k in range(group)]
        for k in range(group):
            x_v[granule_rows(n * group + k), :] = rows[k]

    with jax.named_scope("wait_g"):
        for s in range(seqs):
            at = pl.ds(s * seq, seq)
            pltpu.make_async_copy(dy_hbm.at[at, :], g_v.at[at, :], g_sem.at[s]).wait()

    @pl.loop(0, packed // GRANULE // group)
    def _(n):
        rows = [g_v[source_rows(n * group + k), :] for k in range(group)]
        for k in range(group):
            at = n * group + k
            keep = lax.broadcasted_iota(jnp.int32, (GRANULE, d_model), 0) < table_ref[2 + lax.div(at, 128), lax.rem(at, 128)]
            g_v[granule_rows(at), :] = jnp.where(keep, rows[k], jnp.zeros((), bf16))

    with jax.named_scope("wait_w"):
        for copy in weights(0):
            copy.wait()

    @pl.loop(0, 2)
    def _(n):
        at = pl.ds(pl.multiple_of(n * (block // 2), 16), block // 2)
        u0[at, :] = jnp.dot(x_v[at, :], w1_v[:, 0:CHUNK], preferred_element_type=f32).astype(bf16)
        d0[at, :] = lax.dot_general(g_v[at, :], w2_v[0], NT, preferred_element_type=f32)


    def events(i, which):
        for e, lag in which:
            j = i - lag

            @pl.when((j >= 0) & (j < chunks))
            def _():
                with jax.named_scope(f"event{e}"):
                    event(e, j)

    @pl.loop(0, chunks)
    def _(i):
        @pl.when(i + 1 < chunks)
        def _():
            for copy in weights(i + 1):
                copy.start()

        @pl.when(i > 0)
        def _():
            du_out(i - 1).wait()

        @pl.loop(0, BLOCKS // span)
        def _(n):
            last = n == BLOCKS // span - 1

            @pl.when(last & (i + 1 < chunks))
            def _():
                for copy in weights(i + 1):
                    copy.wait()

            b = n * span
            after = jnp.minimum(i + last.astype(jnp.int32), chunks - 1)
            sets = ((u0, d0), (u1, d1))
            with jax.named_scope("tokens"):
                for k in range(span):
                    pointwise(b + k, *sets[k % 2])
                    if k < span - 1:
                        dots(b + k + 1, i, *sets[(k + 1) % 2])
                    else:
                        dots(lax.rem(b + span, BLOCKS), after, *sets[0])

            @pl.when(n == BLOCKS // span // 2 - 1)
            def _():
                events(i, EARLY)

        du_out(i).start()
        events(i, MIDDLE)
        slot = lax.rem(i, HELD)
        with jax.named_scope("dw"):
            @pl.loop(0, cuts)
            def _(n):
                n2, n1 = CHUNK // cuts, d_model // cuts
                at2, at1 = pl.ds(pl.multiple_of(n * n2, n2), n2), pl.ds(pl.multiple_of(n * n1, n1), n1)
                p2[slot, at2, :] = lax.dot_general(a_v[:, at2], g_v[:packed, :], TN, preferred_element_type=f32).astype(bf16)
                p1[slot, at1, :] = lax.dot_general(x_v[:packed, at1], du_v[...], TN, preferred_element_type=f32).astype(bf16)

        @pl.when(i == chunks - 1)
        def _():
            du_out(i).wait()
            du_in(0).start()

        events(i, LATE)

    @pl.loop(0, max(TAIL, dx_blocks))
    def _(q):
        @pl.when(q < dx_blocks)
        def _():
            slot = lax.rem(q, 2)

            @pl.when(q + 1 < dx_blocks)
            def _():
                du_in(q + 1).start()

            @pl.when(q > 1)
            def _():
                dx_out(q - 2).wait()

            with jax.named_scope("dx"):
                du_in(q).wait()
                dx_v[slot] = (g_v[dx_rows(q), :].astype(f32) + lax.dot_general(dub_v[slot], w1_v[...], NT, preferred_element_type=f32)).astype(bf16)
            dx_out(q).start()

        seen = {lag: max(e for e, behind in EARLY + MIDDLE + LATE if behind <= lag) for lag in range(6)}
        for e in reversed(range(1, TAIL + 1)):
            steps = {e - 1 - last: lag for lag, last in seen.items() if last < e}
            lag = sum(jnp.where(q == step, behind, 0) for step, behind in steps.items())
            j = chunks - 1 - lag

            @pl.when(functools.reduce(jnp.logical_or, [q == step for step in steps]) & (j >= 0))
            def _():
                with jax.named_scope(f"event{e}"):
                    event(e, j)

    dx_out(dx_blocks - 2).wait()
    dx_out(dx_blocks - 1).wait()


def grads_call(dims, ident, table, x, dy, w1, w2):
    tokens, d_model, d_ff, seq, packed, dx_block = dims
    scratch = [
        pltpu.VMEM((tokens, d_model), bf16), pltpu.VMEM((tokens, d_model), bf16),
        pltpu.VMEM((d_model, d_ff), bf16), pltpu.VMEM((2, CHUNK, d_model), bf16),
        pltpu.VMEM((packed // BLOCKS, CHUNK), bf16), pltpu.VMEM((packed // BLOCKS, CHUNK), bf16),
        pltpu.VMEM((packed // BLOCKS, CHUNK), f32), pltpu.VMEM((packed // BLOCKS, CHUNK), f32),
        pltpu.VMEM((packed, CHUNK), bf16), pltpu.VMEM((packed, CHUNK), bf16),
        pltpu.VMEM((HELD, d_model, CHUNK), bf16), pltpu.VMEM((HELD, CHUNK, d_model), bf16),
        pltpu.VMEM((2, dx_block, d_ff), bf16), pltpu.VMEM((2, dx_block, d_model), bf16),
    ]
    for (_, _, rows, _, cols, _) in part_table(d_model):
        for s in range(STAGES):
            last = s == STAGES - 1
            scratch.append(pltpu.VMEM((2, rows >> (4 if last else s + 1), cols // 2 if last else cols), bf16))
    dma = pltpu.SemaphoreType.DMA
    scratch += [dma((tokens // seq,)), dma((tokens // seq,)), dma((2, 2)), dma, dma((4,)), dma((2,)), dma((2,))]
    scratch += [dma((2, STAGES, 4))] * 4
    return pl.pallas_call(
        functools.partial(grads_kernel, dims),
        out_shape=[jax.ShapeDtypeStruct((d_model, d_ff), bf16), jax.ShapeDtypeStruct((d_ff, d_model), bf16),
                   jax.ShapeDtypeStruct((tokens, d_ff), bf16), jax.ShapeDtypeStruct((tokens + seq, d_model), bf16)],
        in_specs=[SMEM] + [ANY] * 4,
        out_specs=[ANY] * 4,
        scratch_shapes=scratch,
        compiler_params=pltpu.CompilerParams(collective_id=ident, has_side_effects=True, vmem_limit_bytes=62 * 2**20),
        cost_estimate=pl.CostEstimate(flops=10 * packed * d_model * d_ff, bytes_accessed=4 * packed * d_ff, transcendentals=packed * d_ff),
        name=f"grads{packed}",
    )(table, x, dy, w1, w2)


def finish_kernel(dims, len_ref, o1_hbm, o2_hbm, dxp_hbm, g1_hbm, g2_hbm, dx_hbm, c1_v, c2_v, dx_v, starts, c_in, c_out, dx_in, dx_out):
    tokens, d_model, d_ff, seq = dims
    seqs = tokens // seq
    steps, slots, ahead = 2 * seqs, 6, 3
    n1, n2 = d_model // steps, d_ff // steps

    def rows(b, n):
        return pl.ds(pl.multiple_of(b * n, 16), n)

    def carry_in(b):
        slot = lax.rem(b, slots)
        return (pltpu.make_async_copy(o1_hbm.at[rows(b, n1), :], c1_v.at[slot], c_in.at[slot, 0]),
                pltpu.make_async_copy(o2_hbm.at[rows(b, n2), :], c2_v.at[slot], c_in.at[slot, 1]))

    def carry_out(b):
        slot = lax.rem(b, slots)
        return (pltpu.make_async_copy(c1_v.at[slot], g1_hbm.at[rows(b, n1), :], c_out.at[slot, 0]),
                pltpu.make_async_copy(c2_v.at[slot], g2_hbm.at[rows(b, n2), :], c_out.at[slot, 1]))

    starts[0] = jnp.int32(0)
    for s in range(1, seqs):
        starts[s] = starts[s - 1] + granules(len_ref, s - 1)

    def unpack_in(s, act):
        slot, half = lax.rem(s, slots), seq // 2
        for n in range(2):
            at = pl.ds(pl.multiple_of(starts[s] * GRANULE, GRANULE) + n * half, half)

            @pl.when(length(len_ref, s) > n * half)
            def _():
                act(pltpu.make_async_copy(dxp_hbm.at[at, :], dx_v.at[slot, pl.ds(n * half, half), :], dx_in.at[slot, n]))

    def unpack_out(s):
        slot = lax.rem(s, slots)
        return pltpu.make_async_copy(dx_v.at[slot], dx_hbm.at[rows(s, seq), :], dx_out.at[slot])

    for b in range(ahead):
        for copy in carry_in(b):
            copy.start()
    for s in range(2):
        unpack_in(s, lambda copy: copy.start())

    @pl.loop(0, steps)
    def _(b):
        with jax.named_scope("carry_in_wait"):
            for copy in carry_in(b):
                copy.wait()
        for copy in carry_out(b):
            copy.start()

        @pl.when(b >= ahead)
        def _():
            for copy in carry_out(b - ahead):
                copy.wait()

        @pl.when(b + ahead < steps)
        def _():
            for copy in carry_in(b + ahead):
                copy.start()

        s = lax.div(b, 2)

        @pl.when(lax.rem(b, 2) == 1)
        def _():
            unpack_in(s, lambda copy: copy.wait())
            slot = lax.rem(s, slots)
            keep = lax.broadcasted_iota(jnp.int32, (seq, d_model), 0) < length(len_ref, s)
            dx_v[slot] = jnp.where(keep, dx_v[slot], jnp.zeros((), bf16))
            unpack_out(s).start()

            @pl.when(s >= 2)
            def _():
                unpack_out(s - 2).wait()

            @pl.when(s + 2 < seqs)
            def _():
                unpack_in(s + 2, lambda copy: copy.start())

    for b in range(steps - ahead, steps):
        for copy in carry_out(b):
            copy.wait()
    for s in (seqs - 2, seqs - 1):
        unpack_out(s).wait()


def finish_call(dims, lens, o1, o2, dxp):
    tokens, d_model, d_ff, seq = dims
    steps = 2 * (tokens // seq)
    dma = pltpu.SemaphoreType.DMA
    return pl.pallas_call(
        functools.partial(finish_kernel, dims),
        out_shape=[jax.ShapeDtypeStruct((d_model, d_ff), bf16), jax.ShapeDtypeStruct((d_ff, d_model), bf16),
                   jax.ShapeDtypeStruct((tokens, d_model), bf16)],
        in_specs=[SMEM] + [ANY] * 3,
        out_specs=[ANY] * 3,
        scratch_shapes=[
            pltpu.VMEM((6, d_model // steps, d_ff), bf16), pltpu.VMEM((6, d_ff // steps, d_model), bf16), pltpu.VMEM((6, seq, d_model), bf16),
            pltpu.SMEM((tokens // seq,), jnp.int32), dma((6, 2)), dma((6, 2)), dma((6, 2)), dma((6,))],
        compiler_params=pltpu.CompilerParams(vmem_limit_bytes=63 * 2**20),
        cost_estimate=pl.CostEstimate(flops=tokens * d_model, bytes_accessed=8 * d_model * d_ff, transcendentals=0),
        name="finish",
    )(lens, o1, o2, dxp)


def solution(mesh):
    def local_step(x_loc, dy_loc, len_loc, w_in, w_out):
        layers, d_model, d_ff = w_in.shape
        rows, seq, _ = x_loc.shape
        tokens = rows * seq
        lens = len_loc.T
        x, dy = x_loc.reshape(tokens, d_model), dy_loc.reshape(tokens, d_model)
        w1, w2 = w_in.reshape(d_model, d_ff), w_out.reshape(d_ff, d_model)
        sizes = tuple(tokens * n // 16 for n in (12, 13, 16))

        def branch(n):
            def run(table, x, dy, w1, w2):
                return grads_call((tokens, d_model, d_ff, seq, sizes[n], tokens // 16), n + 1, table, x, dy, w1, w2)

            return run

        size, table = most_call(lens, seq, sizes)
        o1, o2, _, dxp = lax.switch(size[0, 0], [branch(n) for n in range(len(sizes))], table, x, dy, w1, w2)
        g1, g2, dx = finish_call((tokens, d_model, d_ff, seq), lens, o1, o2, dxp)
        return g1.reshape(layers, d_model, d_ff), g2.reshape(layers, d_ff, d_model), dx.reshape(rows, seq, d_model)

    return jax.shard_map(local_step, mesh=mesh, in_specs=(P("data"), P("data"), P("data"), P(), P()), out_specs=(P(), P(), P("data")), check_vma=False)
```

```python
import functools
import math
import jax
import jax.numpy as jnp
from jax import lax
from jax.experimental import pallas as pl
from jax.experimental.pallas import tpu as pltpu
from jax.sharding import PartitionSpec as P

GELU_SCALE = math.sqrt(2.0 / math.pi)
GELU_CUBIC = 0.044715
MESH = pl.DeviceIdType.MESH
NT = (((1,), (1,)), ((), ()))
TN = (((0,), (0,)), ((), ()))
f32 = jnp.float32
bf16 = jnp.bfloat16
ANY = pl.BlockSpec(memory_space=pl.ANY)
SMEM = pl.BlockSpec(memory_space=pltpu.SMEM)

CHUNK = 256
GRANULE = 16
BLOCKS = 8
STAGES = 5
WEIGHT = {"c": 1, "x": 2, "y": 4, "z": 8, "w": 16}
EARLY = ((1, 1), (8, 5))
MIDDLE = ((3, 2), (5, 3), (7, 4), (10, 6))
LATE = ((0, 0), (2, 1), (4, 2), (6, 3), (9, 5))
TAIL = 2 * STAGES
TAIL_STEPS = {e: tuple((lag, step) for lag, seen in enumerate((
    {n: n - 1 for n in range(1, 11)}, {n: n - 2 for n in range(3, 11)}, {n: n - 4 for n in range(5, 11)},
    {n: n - 6 for n in range(7, 11)}, {8: 0, 9: 2, 10: 3}, {10: 0})) for n, step in seen.items() if n == e) for e in range(1, TAIL + 1)}
WEIGHT = {"c": 1, "x": 2, "y": 4, "z": 8, "w": 16}
EARLY = ((1, 1), (8, 5))
MIDDLE = ((3, 2), (5, 3), (7, 4), (10, 6))
LATE = ((0, 0), (2, 1), (4, 2), (6, 3), (9, 5))
TAIL = 2 * STAGES
HELD = 4


def gelu_both(u):
    sq = u * u
    half = 0.5 + 0.5 * jnp.tanh(u * (GELU_SCALE + (GELU_SCALE * GELU_CUBIC) * sq))
    value = u * half
    return value, half + (value * (1.0 - half)) * (2.0 * GELU_SCALE + (6.0 * GELU_SCALE * GELU_CUBIC) * sq)


def part_table(d_model):
    rows = 1024 if d_model == 1280 else d_model // 2
    cols = 768 if d_model == 1280 else d_model // 2
    return (
        (0, 0, rows, 0, CHUNK, "cxyzw"),
        (0, rows, d_model - rows, 0, CHUNK, "czxyw"),
        (1, 0, CHUNK, 0, cols, "cyxzw"),
        (1, 0, CHUNK, cols, d_model - cols, "czyxw"),
    )


def place():
    me = lax.axis_index("data")
    bit = {k: lax.rem(lax.div(me, v), 2) for k, v in WEIGHT.items()}
    return me, bit, {k: me + v * (1 - 2 * bit[k]) for k, v in WEIGHT.items()}


def granules(len_ref, s):
    return lax.div(length(len_ref, s) + (GRANULE - 1), GRANULE)


def length(len_ref, s):
    return len_ref[lax.rem(s, 2), lax.div(s, 2)]


def most_kernel(seqs, seq, sizes, len_ref, out_ref, table_ref, mine, plane, best, depth, send, recv):
    me, bit, _ = place()

    def other(d, names):
        return me + sum(WEIGHT[k] * (1 - 2 * bit[k]) for n, k in enumerate(names) if d >> n & 1)

    counts = [granules(len_ref, s) for s in range(seqs)]
    starts = [sum(counts[:s], jnp.int32(0)) for s in range(seqs + 1)]
    mine[...] = jnp.full(mine.shape, (starts[seqs] * GRANULE).astype(f32))
    barrier = pltpu.get_barrier_semaphore()
    near = [other(d, "cxy") for d in range(1, 8)]
    far = [other(d, "zw") for d in range(1, 4)]
    for device in near + far:
        pl.semaphore_signal(barrier, inc=1, device_id=(device,), device_id_type=MESH)
    pl.semaphore_wait(barrier, len(near) + len(far))

    def exchange(source, slots, devices, first):
        copies = [pltpu.make_async_remote_copy(source, slots.at[n], send.at[first + n], recv.at[first + n], device_id=(device,), device_id_type=MESH)
                  for n, device in enumerate(devices)]
        for copy in copies:
            copy.start()
        return copies

    def largest_of(copies, source, slots):
        for copy in copies:
            copy.wait()
        return functools.reduce(jnp.maximum, [slots[n] for n in range(len(copies))], source[...])

    first = exchange(mine, plane, near, 0)
    k = lax.broadcasted_iota(jnp.int32, (2, 128), 0) * 128 + lax.broadcasted_iota(jnp.int32, (2, 128), 1)
    source, left = k, length(len_ref, 0) - k * GRANULE
    for s in range(1, seqs):
        past = k >= starts[s]
        source = jnp.where(past, k - starts[s] + s * (seq // GRANULE), source)
        left = jnp.where(past, length(len_ref, s) - (k - starts[s]) * GRANULE, left)
    inside = k < starts[seqs]
    table_ref[0:2, :] = jnp.where(inside, source, 0)
    table_ref[2:4, :] = jnp.where(inside, left, 0)
    best[...] = largest_of(first, mine, plane)
    largest = largest_of(exchange(best, depth, far, len(near)), best, depth)
    out_ref[0, 0] = jnp.max(sum((largest > size).astype(jnp.int32) for size in sizes[:-1]))


def most_call(lens, seq, sizes):
    tile = (8, 128)
    dma = pltpu.SemaphoreType.DMA
    return pl.pallas_call(
        functools.partial(most_kernel, lens.size, seq, sizes),
        out_shape=[jax.ShapeDtypeStruct((1, 1), jnp.int32), jax.ShapeDtypeStruct((4, 128), jnp.int32)],
        in_specs=[SMEM],
        out_specs=[SMEM, pl.BlockSpec(memory_space=pltpu.VMEM)],
        scratch_shapes=[pltpu.VMEM(tile, f32), pltpu.VMEM((7, *tile), f32), pltpu.VMEM(tile, f32), pltpu.VMEM((3, *tile), f32), dma((10,)), dma((10,))],
        compiler_params=pltpu.CompilerParams(collective_id=0, has_side_effects=True),
        name="most",
    )(lens)


def grads_kernel(dims, table_ref, x_hbm, dy_hbm, w1_hbm, w2_hbm, o1_hbm, o2_hbm, du_hbm, dx_hbm, *scratch):
    tokens, d_model, d_ff, seq, packed, dx_block = dims
    seqs = tokens // seq
    chunks = d_ff // CHUNK
    block = packed // BLOCKS
    dx_blocks = packed // dx_block
    span = BLOCKS // 2 if packed < tokens else 2
    cuts = 1 if packed < tokens else 2
    parts = part_table(d_model)
    (x_v, g_v, w1_v, w2_v, u0, u1, d0, d1, a_v, du_v, p1, p2, dub_v, dx_v) = scratch[:14]
    recv = [scratch[14 + 5 * k : 19 + 5 * k] for k in range(4)]
    (x_sem, g_sem, w_sem, du_sem, own_sem, dub_sem, dx_sem, rs_send, rs_recv, ag_send, ag_recv) = scratch[34:]

    _, bit, peer = place()
    for s in range(seqs):
        at = pl.ds(s * seq, seq)
        pltpu.make_async_copy(x_hbm.at[at, :], x_v.at[at, :], x_sem.at[s]).start()

    barrier = pltpu.get_barrier_semaphore()
    for k in WEIGHT:
        pl.semaphore_signal(barrier, inc=1, device_id=(peer[k],), device_id_type=MESH)
    for s in range(seqs):
        at = pl.ds(s * seq, seq)
        pltpu.make_async_copy(dy_hbm.at[at, :], g_v.at[at, :], g_sem.at[s]).start()
    pl.semaphore_wait(barrier, STAGES)

    region, given = [], []
    for (_, r0, nr, c0, nc, order) in parts:
        mine, away = [(r0, nr, c0, nc)], []
        for s, name in enumerate(order):
            row, rows, col, cols = mine[-1]
            if s < STAGES - 1:
                half = rows // 2
                mine.append((row + bit[name] * half, half, col, cols))
                away.append((row + (1 - bit[name]) * half, half, col, cols))
            else:
                half = cols // 2
                mine.append((row, rows, col + bit[name] * half, half))
                away.append((row, rows, col + (1 - bit[name]) * half, half))
        region.append(mine)
        given.append(away)

    def cut(r):
        row, rows, col, cols = r
        row = row if isinstance(row, int) else pl.multiple_of(row, 16)
        col = col if isinstance(col, int) else pl.multiple_of(col, 128)
        return pl.ds(row, rows), pl.ds(col, cols)

    def partial(k, i, r):
        rows, cols = cut(r)
        return (p1, p2)[parts[k][0]].at[lax.rem(i, HELD), rows, cols]

    def whole(k, i, r):
        row, rows, col, cols = r
        if parts[k][0] == 0:
            return o1_hbm.at[cut((row, rows, i * CHUNK + col, cols))]
        return o2_hbm.at[cut((i * CHUNK + row, rows, col, cols))]

    def reduce_copy(k, s, i):
        slot = lax.rem(i, 2)
        return pltpu.make_async_remote_copy(
            src_ref=partial(k, i, given[k][s]), dst_ref=recv[k][s].at[slot],
            send_sem=rs_send.at[slot, s, k], recv_sem=rs_recv.at[slot, s, k],
            device_id=(peer[parts[k][5][s]],), device_id_type=MESH)

    def gather_copy(k, s, i):
        slot = lax.rem(i, 2)
        r = region[k][s + 1]
        return pltpu.make_async_remote_copy(
            src_ref=partial(k, i, r) if s == STAGES - 1 else whole(k, i, r), dst_ref=whole(k, i, r),
            send_sem=ag_send.at[slot, s, k], recv_sem=ag_recv.at[slot, s, k],
            device_id=(peer[parts[k][5][s]],), device_id_type=MESH)

    def own_copy(k, i):
        r = region[k][STAGES]
        return pltpu.make_async_copy(partial(k, i, r), whole(k, i, r), own_sem.at[k])

    def event(e, i):
        for k in range(4):
            if 1 <= e <= STAGES:
                reduce_copy(k, e - 1, i).wait()
                rows, cols = cut(region[k][e])
                ref, slot = (p1, p2)[parts[k][0]], lax.rem(i, HELD)
                ref[slot, rows, cols] = ref[slot, rows, cols] + recv[k][e - 1][lax.rem(i, 2)]
            if e < STAGES:
                reduce_copy(k, e, i).start()
            if e == STAGES:
                own_copy(k, i).start()
            if e > STAGES:
                gather_copy(k, 2 * STAGES - e, i).wait()
                if e == STAGES + 1:
                    own_copy(k, i).wait()
            if STAGES <= e < 2 * STAGES:
                gather_copy(k, 2 * STAGES - 1 - e, i).start()

    def weights(i):
        slot = lax.rem(i, 2)
        at = pl.ds(pl.multiple_of(i * CHUNK, CHUNK), CHUNK)
        return (pltpu.make_async_copy(w1_hbm.at[:, at], w1_v.at[:, at], w_sem.at[slot, 0]),
                pltpu.make_async_copy(w2_hbm.at[at, :], w2_v.at[slot], w_sem.at[slot, 1]))

    def rows_of(b):
        return pl.ds(pl.multiple_of(b * block, 16), block)

    def dots(b, i, u, d):
        w1 = w1_v[:, pl.ds(pl.multiple_of(i * CHUNK, CHUNK), CHUNK)]
        u[...] = jnp.dot(x_v[rows_of(b), :], w1, preferred_element_type=f32).astype(bf16)
        d[...] = lax.dot_general(g_v[rows_of(b), :], w2_v[lax.rem(i, 2)], NT, preferred_element_type=f32)

    def pointwise(b, u, d):
        a, slope = gelu_both(u[...].astype(f32))
        a_v[rows_of(b), :] = a.astype(bf16)
        du_v[rows_of(b), :] = (d[...] * slope).astype(bf16)

    def du_out(i):
        return pltpu.make_async_copy(du_v, du_hbm.at[pl.ds(0, packed), pl.ds(pl.multiple_of(i * CHUNK, CHUNK), CHUNK)], du_sem)

    def dx_rows(q):
        return pl.ds(pl.multiple_of(q * dx_block, 16), dx_block)

    def du_in(q):
        slot = lax.rem(q, 2)
        return pltpu.make_async_copy(du_hbm.at[dx_rows(q), :], dub_v.at[slot], dub_sem.at[slot])

    def du_first():
        ready = pl.ds(0, (chunks - 1) * CHUNK)
        return pltpu.make_async_copy(du_hbm.at[dx_rows(0), ready], dub_v.at[0, :, ready], dub_sem.at[0])

    def dx_out(q):
        slot = lax.rem(q, 2)
        return pltpu.make_async_copy(dx_v.at[slot], dx_hbm.at[dx_rows(q), :], dx_sem.at[slot])

    for copy in weights(0):
        copy.start()

    with jax.named_scope("wait_x"):
        for s in range(seqs):
            at = pl.ds(s * seq, seq)
            pltpu.make_async_copy(x_hbm.at[at, :], x_v.at[at, :], x_sem.at[s]).wait()

    group = 4 if packed % (4 * GRANULE) == 0 else 2

    def granule_rows(k):
        return pl.ds(pl.multiple_of(k * GRANULE, GRANULE), GRANULE)

    def source_rows(k):
        return pl.ds(table_ref[lax.div(k, 128), lax.rem(k, 128)] * GRANULE, GRANULE)

    @pl.loop(0, packed // GRANULE // group)
    def _(n):
        rows = [x_v[source_rows(n * group + k), :] for k in range(group)]
        for k in range(group):
            x_v[granule_rows(n * group + k), :] = rows[k]

    with jax.named_scope("wait_g"):
        for s in range(seqs):
            at = pl.ds(s * seq, seq)
            pltpu.make_async_copy(dy_hbm.at[at, :], g_v.at[at, :], g_sem.at[s]).wait()

    @pl.loop(0, packed // GRANULE // group)
    def _(n):
        rows = [g_v[source_rows(n * group + k), :] for k in range(group)]
        for k in range(group):
            at = n * group + k
            keep = lax.broadcasted_iota(jnp.int32, (GRANULE, d_model), 0) < table_ref[2 + lax.div(at, 128), lax.rem(at, 128)]
            g_v[granule_rows(at), :] = jnp.where(keep, rows[k], jnp.zeros((), bf16))

    with jax.named_scope("wait_w"):
        for copy in weights(0):
            copy.wait()

    @pl.loop(0, 2)
    def _(n):
        at = pl.ds(pl.multiple_of(n * (block // 2), 16), block // 2)
        u0[at, :] = jnp.dot(x_v[at, :], w1_v[:, 0:CHUNK], preferred_element_type=f32).astype(bf16)
        d0[at, :] = lax.dot_general(g_v[at, :], w2_v[0], NT, preferred_element_type=f32)


    def events(i, which):
        for e, lag in which:
            j = i - lag

            @pl.when((j >= 0) & (j < chunks))
            def _():
                with jax.named_scope(f"event{e}"):
                    event(e, j)

    @pl.loop(0, chunks)
    def _(i):
        @pl.when(i + 1 < chunks)
        def _():
            for copy in weights(i + 1):
                copy.start()

        @pl.when(i > 0)
        def _():
            du_out(i - 1).wait()

        @pl.loop(0, BLOCKS // span)
        def _(n):
            last = n == BLOCKS // span - 1

            @pl.when(last & (i + 1 < chunks))
            def _():
                for copy in weights(i + 1):
                    copy.wait()

            b = n * span
            after = jnp.minimum(i + last.astype(jnp.int32), chunks - 1)
            sets = ((u0, d0), (u1, d1))
            with jax.named_scope("tokens"):
                for k in range(span):
                    pointwise(b + k, *sets[k % 2])
                    if k < span - 1:
                        dots(b + k + 1, i, *sets[(k + 1) % 2])
                    else:
                        dots(lax.rem(b + span, BLOCKS), after, *sets[0])

            @pl.when(n == BLOCKS // span // 2 - 1)
            def _():
                events(i, EARLY)

        du_out(i).start()
        events(i, MIDDLE)

        @pl.when(i == chunks - 1)
        def _():
            du_first().start()

        slot = lax.rem(i, HELD)
        with jax.named_scope("dw"):
            @pl.loop(0, cuts)
            def _(n):
                n2, n1 = CHUNK // cuts, d_model // cuts
                at2, at1 = pl.ds(pl.multiple_of(n * n2, n2), n2), pl.ds(pl.multiple_of(n * n1, n1), n1)
                p2[slot, at2, :] = lax.dot_general(a_v[:, at2], g_v[:packed, :], TN, preferred_element_type=f32).astype(bf16)
                p1[slot, at1, :] = lax.dot_general(x_v[:packed, at1], du_v[...], TN, preferred_element_type=f32).astype(bf16)

        events(i, LATE)

    @pl.loop(0, max(TAIL, dx_blocks))
    def _(q):
        @pl.when(q < dx_blocks)
        def _():
            slot = lax.rem(q, 2)

            @pl.when(q == 0)
            def _():
                du_out(chunks - 1).wait()
                du_first().wait()
                dub_v[0, :, pl.ds((chunks - 1) * CHUNK, CHUNK)] = du_v[dx_rows(0), :]

            @pl.when(q + 1 < dx_blocks)
            def _():
                du_in(q + 1).start()

            @pl.when(q > 0)
            def _():
                du_in(q).wait()

            @pl.when(q > 1)
            def _():
                dx_out(q - 2).wait()

            with jax.named_scope("dx"):
                dx_v[slot] = (g_v[dx_rows(q), :].astype(f32) + lax.dot_general(dub_v[slot], w1_v[...], NT, preferred_element_type=f32)).astype(bf16)
            dx_out(q).start()

        for e in (1, *reversed(range(2, TAIL + 1))):
            lag = sum(jnp.where(q == step, behind, 0) for behind, step in TAIL_STEPS[e])
            j = chunks - 1 - lag

            @pl.when(functools.reduce(jnp.logical_or, [q == step for _, step in TAIL_STEPS[e]]) & (j >= 0))
            def _():
                with jax.named_scope(f"event{e}"):
                    event(e, j)

    dx_out(dx_blocks - 2).wait()
    dx_out(dx_blocks - 1).wait()


def grads_call(dims, ident, table, x, dy, w1, w2):
    tokens, d_model, d_ff, seq, packed, dx_block = dims
    scratch = [
        pltpu.VMEM((tokens, d_model), bf16), pltpu.VMEM((tokens, d_model), bf16),
        pltpu.VMEM((d_model, d_ff), bf16), pltpu.VMEM((2, CHUNK, d_model), bf16),
        pltpu.VMEM((packed // BLOCKS, CHUNK), bf16), pltpu.VMEM((packed // BLOCKS, CHUNK), bf16),
        pltpu.VMEM((packed // BLOCKS, CHUNK), f32), pltpu.VMEM((packed // BLOCKS, CHUNK), f32),
        pltpu.VMEM((packed, CHUNK), bf16), pltpu.VMEM((packed, CHUNK), bf16),
        pltpu.VMEM((HELD, d_model, CHUNK), bf16), pltpu.VMEM((HELD, CHUNK, d_model), bf16),
        pltpu.VMEM((2, dx_block, d_ff), bf16), pltpu.VMEM((2, dx_block, d_model), bf16),
    ]
    for (_, _, rows, _, cols, _) in part_table(d_model):
        for s in range(STAGES):
            last = s == STAGES - 1
            scratch.append(pltpu.VMEM((2, rows >> (4 if last else s + 1), cols // 2 if last else cols), bf16))
    dma = pltpu.SemaphoreType.DMA
    scratch += [dma((tokens // seq,)), dma((tokens // seq,)), dma((2, 2)), dma, dma((4,)), dma((2,)), dma((2,))]
    scratch += [dma((2, STAGES, 4))] * 4
    return pl.pallas_call(
        functools.partial(grads_kernel, dims),
        out_shape=[jax.ShapeDtypeStruct((d_model, d_ff), bf16), jax.ShapeDtypeStruct((d_ff, d_model), bf16),
                   jax.ShapeDtypeStruct((tokens, d_ff), bf16), jax.ShapeDtypeStruct((tokens + seq, d_model), bf16)],
        in_specs=[SMEM] + [ANY] * 4,
        out_specs=[ANY] * 4,
        scratch_shapes=scratch,
        compiler_params=pltpu.CompilerParams(collective_id=ident, has_side_effects=True, vmem_limit_bytes=62 * 2**20),
        cost_estimate=pl.CostEstimate(flops=10 * packed * d_model * d_ff, bytes_accessed=4 * packed * d_ff, transcendentals=packed * d_ff),
        name=f"grads{packed}",
    )(table, x, dy, w1, w2)


def finish_kernel(dims, len_ref, o1_hbm, o2_hbm, dxp_hbm, g1_hbm, g2_hbm, dx_hbm, c1_v, c2_v, dx_v, starts, c_in, c_out, dx_in, dx_out):
    tokens, d_model, d_ff, seq = dims
    seqs = tokens // seq
    steps, slots, ahead = 2 * seqs, 6, 3
    n1, n2 = d_model // steps, d_ff // steps

    def rows(b, n):
        return pl.ds(pl.multiple_of(b * n, 16), n)

    def carry_in(b):
        slot = lax.rem(b, slots)
        return (pltpu.make_async_copy(o1_hbm.at[rows(b, n1), :], c1_v.at[slot], c_in.at[slot, 0]),
                pltpu.make_async_copy(o2_hbm.at[rows(b, n2), :], c2_v.at[slot], c_in.at[slot, 1]))

    def carry_out(b):
        slot = lax.rem(b, slots)
        return (pltpu.make_async_copy(c1_v.at[slot], g1_hbm.at[rows(b, n1), :], c_out.at[slot, 0]),
                pltpu.make_async_copy(c2_v.at[slot], g2_hbm.at[rows(b, n2), :], c_out.at[slot, 1]))

    starts[0] = jnp.int32(0)
    for s in range(1, seqs):
        starts[s] = starts[s - 1] + granules(len_ref, s - 1)

    def unpack_in(s, act):
        slot, half = lax.rem(s, slots), seq // 2
        for n in range(2):
            at = pl.ds(pl.multiple_of(starts[s] * GRANULE, GRANULE) + n * half, half)

            @pl.when(length(len_ref, s) > n * half)
            def _():
                act(pltpu.make_async_copy(dxp_hbm.at[at, :], dx_v.at[slot, pl.ds(n * half, half), :], dx_in.at[slot, n]))

    def unpack_out(s):
        slot = lax.rem(s, slots)
        return pltpu.make_async_copy(dx_v.at[slot], dx_hbm.at[rows(s, seq), :], dx_out.at[slot])

    for b in range(ahead):
        for copy in carry_in(b):
            copy.start()
    for s in range(2):
        unpack_in(s, lambda copy: copy.start())

    @pl.loop(0, steps)
    def _(b):
        with jax.named_scope("carry_in_wait"):
            for copy in carry_in(b):
                copy.wait()
        for copy in carry_out(b):
            copy.start()

        @pl.when(b >= ahead)
        def _():
            for copy in carry_out(b - ahead):
                copy.wait()

        @pl.when(b + ahead < steps)
        def _():
            for copy in carry_in(b + ahead):
                copy.start()

        s = lax.div(b, 2)

        @pl.when(lax.rem(b, 2) == 1)
        def _():
            unpack_in(s, lambda copy: copy.wait())
            slot = lax.rem(s, slots)
            keep = lax.broadcasted_iota(jnp.int32, (seq, d_model), 0) < length(len_ref, s)
            dx_v[slot] = jnp.where(keep, dx_v[slot], jnp.zeros((), bf16))
            unpack_out(s).start()

            @pl.when(s >= 2)
            def _():
                unpack_out(s - 2).wait()

            @pl.when(s + 2 < seqs)
            def _():
                unpack_in(s + 2, lambda copy: copy.start())

    for b in range(steps - ahead, steps):
        for copy in carry_out(b):
            copy.wait()
    for s in (seqs - 2, seqs - 1):
        unpack_out(s).wait()


def finish_call(dims, lens, o1, o2, dxp):
    tokens, d_model, d_ff, seq = dims
    steps = 2 * (tokens // seq)
    dma = pltpu.SemaphoreType.DMA
    return pl.pallas_call(
        functools.partial(finish_kernel, dims),
        out_shape=[jax.ShapeDtypeStruct((d_model, d_ff), bf16), jax.ShapeDtypeStruct((d_ff, d_model), bf16),
                   jax.ShapeDtypeStruct((tokens, d_model), bf16)],
        in_specs=[SMEM] + [ANY] * 3,
        out_specs=[ANY] * 3,
        scratch_shapes=[
            pltpu.VMEM((6, d_model // steps, d_ff), bf16), pltpu.VMEM((6, d_ff // steps, d_model), bf16), pltpu.VMEM((6, seq, d_model), bf16),
            pltpu.SMEM((tokens // seq,), jnp.int32), dma((6, 2)), dma((6, 2)), dma((6, 2)), dma((6,))],
        compiler_params=pltpu.CompilerParams(vmem_limit_bytes=63 * 2**20),
        cost_estimate=pl.CostEstimate(flops=tokens * d_model, bytes_accessed=8 * d_model * d_ff, transcendentals=0),
        name="finish",
    )(lens, o1, o2, dxp)


def solution(mesh):
    def local_step(x_loc, dy_loc, len_loc, w_in, w_out):
        layers, d_model, d_ff = w_in.shape
        rows, seq, _ = x_loc.shape
        tokens = rows * seq
        lens = len_loc.T
        x, dy = x_loc.reshape(tokens, d_model), dy_loc.reshape(tokens, d_model)
        w1, w2 = w_in.reshape(d_model, d_ff), w_out.reshape(d_ff, d_model)
        sizes = tuple(tokens * n // 16 for n in (12, 13, 16))

        def branch(n):
            def run(table, x, dy, w1, w2):
                return grads_call((tokens, d_model, d_ff, seq, sizes[n], tokens // 16), n + 1, table, x, dy, w1, w2)

            return run

        size, table = most_call(lens, seq, sizes)
        o1, o2, _, dxp = lax.switch(size[0, 0], [branch(n) for n in range(len(sizes))], table, x, dy, w1, w2)
        g1, g2, dx = finish_call((tokens, d_model, d_ff, seq), lens, o1, o2, dxp)
        return g1.reshape(layers, d_model, d_ff), g2.reshape(layers, d_ff, d_model), dx.reshape(rows, seq, d_model)

    return jax.shard_map(local_step, mesh=mesh, in_specs=(P("data"), P("data"), P("data"), P(), P()), out_specs=(P(), P(), P("data")), check_vma=False)
```

```python
import functools
import math
import jax
import jax.numpy as jnp
from jax import lax
from jax.experimental import pallas as pl
from jax.experimental.pallas import tpu as pltpu
from jax.sharding import PartitionSpec as P

GELU_SCALE = math.sqrt(2.0 / math.pi)
GELU_CUBIC = 0.044715
MESH = pl.DeviceIdType.MESH
NT = (((1,), (1,)), ((), ()))
TN = (((0,), (0,)), ((), ()))
f32 = jnp.float32
bf16 = jnp.bfloat16
ANY = pl.BlockSpec(memory_space=pl.ANY)
SMEM = pl.BlockSpec(memory_space=pltpu.SMEM)

CHUNK = 256
GRANULE = 16
BLOCKS = 8
STAGES = 5
WEIGHT = {"c": 1, "x": 2, "y": 4, "z": 8, "w": 16}
EARLY = ((1, 1), (9, 6))
MIDDLE = ((3, 2), (5, 3), (8, 5), (7, 4), (10, 6))
LATE = ((0, 0), (2, 1), (4, 2), (6, 3))
TAIL = 2 * STAGES
TAIL_STEPS = {e: tuple((lag, step) for lag, seen in enumerate((
    {n: n - 1 for n in range(1, 11)}, {n: n - 2 for n in range(3, 11)}, {n: n - 4 for n in range(5, 11)},
    {n: n - 6 for n in range(7, 11)}, {8: 0, 9: 2, 10: 3}, {9: 0, 10: 1})) for n, step in seen.items() if n == e) for e in range(1, TAIL + 1)}
WEIGHT = {"c": 1, "x": 2, "y": 4, "z": 8, "w": 16}
EARLY = ((1, 1), (9, 6))
MIDDLE = ((3, 2), (5, 3), (8, 5), (7, 4), (10, 6))
LATE = ((0, 0), (2, 1), (4, 2), (6, 3))
TAIL = 2 * STAGES
HELD = 4


def gelu_both(u):
    sq = u * u
    half = 0.5 + 0.5 * jnp.tanh(u * (GELU_SCALE + (GELU_SCALE * GELU_CUBIC) * sq))
    value = u * half
    return value, half + (value * (1.0 - half)) * (2.0 * GELU_SCALE + (6.0 * GELU_SCALE * GELU_CUBIC) * sq)


def part_table(d_model):
    rows = 1024 if d_model == 1280 else d_model // 2
    cols = 768 if d_model == 1280 else d_model // 2
    return (
        (0, 0, rows, 0, CHUNK, "cxyzw"),
        (0, rows, d_model - rows, 0, CHUNK, "czxyw"),
        (1, 0, CHUNK, 0, cols, "cyxzw"),
        (1, 0, CHUNK, cols, d_model - cols, "czyxw"),
    )


def place():
    me = lax.axis_index("data")
    bit = {k: lax.rem(lax.div(me, v), 2) for k, v in WEIGHT.items()}
    return me, bit, {k: me + v * (1 - 2 * bit[k]) for k, v in WEIGHT.items()}


def granules(len_ref, s):
    return lax.div(length(len_ref, s) + (GRANULE - 1), GRANULE)


def length(len_ref, s):
    return len_ref[lax.rem(s, 2), lax.div(s, 2)]


def most_kernel(seqs, seq, sizes, len_ref, out_ref, table_ref, mine, plane, best, depth, send, recv):
    me, bit, _ = place()

    def other(d, names):
        return me + sum(WEIGHT[k] * (1 - 2 * bit[k]) for n, k in enumerate(names) if d >> n & 1)

    counts = [granules(len_ref, s) for s in range(seqs)]
    starts = [sum(counts[:s], jnp.int32(0)) for s in range(seqs + 1)]
    mine[...] = jnp.full(mine.shape, (starts[seqs] * GRANULE).astype(f32))
    barrier = pltpu.get_barrier_semaphore()
    near = [other(d, "cxy") for d in range(1, 8)]
    far = [other(d, "zw") for d in range(1, 4)]
    for device in near + far:
        pl.semaphore_signal(barrier, inc=1, device_id=(device,), device_id_type=MESH)
    pl.semaphore_wait(barrier, len(near) + len(far))

    def exchange(source, slots, devices, first):
        copies = [pltpu.make_async_remote_copy(source, slots.at[n], send.at[first + n], recv.at[first + n], device_id=(device,), device_id_type=MESH)
                  for n, device in enumerate(devices)]
        for copy in copies:
            copy.start()
        return copies

    def largest_of(copies, source, slots):
        for copy in copies:
            copy.wait()
        return functools.reduce(jnp.maximum, [slots[n] for n in range(len(copies))], source[...])

    first = exchange(mine, plane, near, 0)
    k = lax.broadcasted_iota(jnp.int32, (2, 128), 0) * 128 + lax.broadcasted_iota(jnp.int32, (2, 128), 1)
    source, left = k, length(len_ref, 0) - k * GRANULE
    for s in range(1, seqs):
        past = k >= starts[s]
        source = jnp.where(past, k - starts[s] + s * (seq // GRANULE), source)
        left = jnp.where(past, length(len_ref, s) - (k - starts[s]) * GRANULE, left)
    inside = k < starts[seqs]
    table_ref[0:2, :] = jnp.where(inside, source, 0)
    table_ref[2:4, :] = jnp.where(inside, left, 0)
    best[...] = largest_of(first, mine, plane)
    largest = largest_of(exchange(best, depth, far, len(near)), best, depth)
    out_ref[0, 0] = jnp.max(sum((largest > size).astype(jnp.int32) for size in sizes[:-1]))


def most_call(lens, seq, sizes):
    tile = (8, 128)
    dma = pltpu.SemaphoreType.DMA
    return pl.pallas_call(
        functools.partial(most_kernel, lens.size, seq, sizes),
        out_shape=[jax.ShapeDtypeStruct((1, 1), jnp.int32), jax.ShapeDtypeStruct((4, 128), jnp.int32)],
        in_specs=[SMEM],
        out_specs=[SMEM, pl.BlockSpec(memory_space=pltpu.VMEM)],
        scratch_shapes=[pltpu.VMEM(tile, f32), pltpu.VMEM((7, *tile), f32), pltpu.VMEM(tile, f32), pltpu.VMEM((3, *tile), f32), dma((10,)), dma((10,))],
        compiler_params=pltpu.CompilerParams(collective_id=0, has_side_effects=True),
        name="most",
    )(lens)


def grads_kernel(dims, table_ref, x_hbm, dy_hbm, w1_hbm, w2_hbm, o1_hbm, o2_hbm, du_hbm, dx_hbm, *scratch):
    tokens, d_model, d_ff, seq, packed, dx_block = dims
    seqs = tokens // seq
    chunks = d_ff // CHUNK
    block = packed // BLOCKS
    dx_blocks = packed // dx_block
    span = BLOCKS // 2 if packed < tokens else 2
    cuts = 1 if packed < tokens else 2
    parts = part_table(d_model)
    (x_v, g_v, w1_v, w2_v, u0, u1, d0, d1, a_v, du_v, p1, p2, dub_v, dx_v) = scratch[:14]
    recv = [scratch[14 + 5 * k : 19 + 5 * k] for k in range(4)]
    (x_sem, g_sem, w_sem, du_sem, own_sem, dub_sem, dx_sem, rs_send, rs_recv, ag_send, ag_recv) = scratch[34:]

    _, bit, peer = place()
    for s in range(seqs):
        at = pl.ds(s * seq, seq)
        pltpu.make_async_copy(x_hbm.at[at, :], x_v.at[at, :], x_sem.at[s]).start()

    barrier = pltpu.get_barrier_semaphore()
    for k in WEIGHT:
        pl.semaphore_signal(barrier, inc=1, device_id=(peer[k],), device_id_type=MESH)
    for s in range(seqs):
        at = pl.ds(s * seq, seq)
        pltpu.make_async_copy(dy_hbm.at[at, :], g_v.at[at, :], g_sem.at[s]).start()
    pl.semaphore_wait(barrier, STAGES)

    region, given = [], []
    for (_, r0, nr, c0, nc, order) in parts:
        mine, away = [(r0, nr, c0, nc)], []
        for s, name in enumerate(order):
            row, rows, col, cols = mine[-1]
            if s < STAGES - 1:
                half = rows // 2
                mine.append((row + bit[name] * half, half, col, cols))
                away.append((row + (1 - bit[name]) * half, half, col, cols))
            else:
                half = cols // 2
                mine.append((row, rows, col + bit[name] * half, half))
                away.append((row, rows, col + (1 - bit[name]) * half, half))
        region.append(mine)
        given.append(away)

    def cut(r):
        row, rows, col, cols = r
        row = row if isinstance(row, int) else pl.multiple_of(row, 16)
        col = col if isinstance(col, int) else pl.multiple_of(col, 128)
        return pl.ds(row, rows), pl.ds(col, cols)

    def partial(k, i, r):
        rows, cols = cut(r)
        return (p1, p2)[parts[k][0]].at[lax.rem(i, HELD), rows, cols]

    def whole(k, i, r):
        row, rows, col, cols = r
        if parts[k][0] == 0:
            return o1_hbm.at[cut((row, rows, i * CHUNK + col, cols))]
        return o2_hbm.at[cut((i * CHUNK + row, rows, col, cols))]

    def reduce_copy(k, s, i):
        slot = lax.rem(i, 2)
        return pltpu.make_async_remote_copy(
            src_ref=partial(k, i, given[k][s]), dst_ref=recv[k][s].at[slot],
            send_sem=rs_send.at[slot, s, k], recv_sem=rs_recv.at[slot, s, k],
            device_id=(peer[parts[k][5][s]],), device_id_type=MESH)

    def gather_copy(k, s, i):
        slot = lax.rem(i, 2)
        r = region[k][s + 1]
        return pltpu.make_async_remote_copy(
            src_ref=partial(k, i, r) if s == STAGES - 1 else whole(k, i, r), dst_ref=whole(k, i, r),
            send_sem=ag_send.at[slot, s, k], recv_sem=ag_recv.at[slot, s, k],
            device_id=(peer[parts[k][5][s]],), device_id_type=MESH)

    def own_copy(k, i):
        r = region[k][STAGES]
        return pltpu.make_async_copy(partial(k, i, r), whole(k, i, r), own_sem.at[k])

    def event(e, i):
        for k in range(4):
            if 1 <= e <= STAGES:
                reduce_copy(k, e - 1, i).wait()
                rows, cols = cut(region[k][e])
                ref, slot = (p1, p2)[parts[k][0]], lax.rem(i, HELD)
                ref[slot, rows, cols] = ref[slot, rows, cols] + recv[k][e - 1][lax.rem(i, 2)]
            if e < STAGES:
                reduce_copy(k, e, i).start()
            if e == STAGES:
                own_copy(k, i).start()
            if e > STAGES:
                gather_copy(k, 2 * STAGES - e, i).wait()
                if e == STAGES + 1:
                    own_copy(k, i).wait()
            if STAGES <= e < 2 * STAGES:
                gather_copy(k, 2 * STAGES - 1 - e, i).start()

    def weights(i):
        slot = lax.rem(i, 2)
        at = pl.ds(pl.multiple_of(i * CHUNK, CHUNK), CHUNK)
        return (pltpu.make_async_copy(w1_hbm.at[:, at], w1_v.at[:, at], w_sem.at[slot, 0]),
                pltpu.make_async_copy(w2_hbm.at[at, :], w2_v.at[slot], w_sem.at[slot, 1]))

    def rows_of(b):
        return pl.ds(pl.multiple_of(b * block, 16), block)

    def dots(b, i, u, d):
        w1 = w1_v[:, pl.ds(pl.multiple_of(i * CHUNK, CHUNK), CHUNK)]
        u[...] = jnp.dot(x_v[rows_of(b), :], w1, preferred_element_type=f32).astype(bf16)
        d[...] = lax.dot_general(g_v[rows_of(b), :], w2_v[lax.rem(i, 2)], NT, preferred_element_type=f32)

    def pointwise(b, u, d):
        a, slope = gelu_both(u[...].astype(f32))
        a_v[rows_of(b), :] = a.astype(bf16)
        du_v[rows_of(b), :] = (d[...] * slope).astype(bf16)

    def du_out(i):
        return pltpu.make_async_copy(du_v, du_hbm.at[pl.ds(0, packed), pl.ds(pl.multiple_of(i * CHUNK, CHUNK), CHUNK)], du_sem)

    def dx_rows(q):
        return pl.ds(pl.multiple_of(q * dx_block, 16), dx_block)

    def du_in(q):
        slot = lax.rem(q, 2)
        return pltpu.make_async_copy(du_hbm.at[dx_rows(q), :], dub_v.at[slot], dub_sem.at[slot])

    def du_first():
        ready = pl.ds(0, (chunks - 1) * CHUNK)
        return pltpu.make_async_copy(du_hbm.at[dx_rows(0), ready], dub_v.at[0, :, ready], dub_sem.at[0])

    def dx_out(q):
        slot = lax.rem(q, 2)
        return pltpu.make_async_copy(dx_v.at[slot], dx_hbm.at[dx_rows(q), :], dx_sem.at[slot])

    for copy in weights(0):
        copy.start()

    with jax.named_scope("wait_x"):
        for s in range(seqs):
            at = pl.ds(s * seq, seq)
            pltpu.make_async_copy(x_hbm.at[at, :], x_v.at[at, :], x_sem.at[s]).wait()

    group = 4 if packed % (4 * GRANULE) == 0 else 2

    def granule_rows(k):
        return pl.ds(pl.multiple_of(k * GRANULE, GRANULE), GRANULE)

    def source_rows(k):
        return pl.ds(table_ref[lax.div(k, 128), lax.rem(k, 128)] * GRANULE, GRANULE)

    @pl.loop(0, packed // GRANULE // group)
    def _(n):
        rows = [x_v[source_rows(n * group + k), :] for k in range(group)]
        for k in range(group):
            x_v[granule_rows(n * group + k), :] = rows[k]

    with jax.named_scope("wait_g"):
        for s in range(seqs):
            at = pl.ds(s * seq, seq)
            pltpu.make_async_copy(dy_hbm.at[at, :], g_v.at[at, :], g_sem.at[s]).wait()

    @pl.loop(0, packed // GRANULE // group)
    def _(n):
        rows = [g_v[source_rows(n * group + k), :] for k in range(group)]
        for k in range(group):
            at = n * group + k
            keep = lax.broadcasted_iota(jnp.int32, (GRANULE, d_model), 0) < table_ref[2 + lax.div(at, 128), lax.rem(at, 128)]
            g_v[granule_rows(at), :] = jnp.where(keep, rows[k], jnp.zeros((), bf16))

    with jax.named_scope("wait_w"):
        for copy in weights(0):
            copy.wait()

    @pl.loop(0, 2)
    def _(n):
        at = pl.ds(pl.multiple_of(n * (block // 2), 16), block // 2)
        u0[at, :] = jnp.dot(x_v[at, :], w1_v[:, 0:CHUNK], preferred_element_type=f32).astype(bf16)
        d0[at, :] = lax.dot_general(g_v[at, :], w2_v[0], NT, preferred_element_type=f32)


    def events(i, which):
        for e, lag in which:
            j = i - lag

            @pl.when((j >= 0) & (j < chunks))
            def _():
                with jax.named_scope(f"event{e}"):
                    event(e, j)

    @pl.loop(0, chunks)
    def _(i):
        @pl.when(i + 1 < chunks)
        def _():
            for copy in weights(i + 1):
                copy.start()

        @pl.when(i > 0)
        def _():
            du_out(i - 1).wait()

        @pl.loop(0, BLOCKS // span)
        def _(n):
            last = n == BLOCKS // span - 1

            @pl.when(last & (i + 1 < chunks))
            def _():
                for copy in weights(i + 1):
                    copy.wait()

            b = n * span
            after = jnp.minimum(i + last.astype(jnp.int32), chunks - 1)
            sets = ((u0, d0), (u1, d1))
            with jax.named_scope("tokens"):
                for k in range(span):
                    pointwise(b + k, *sets[k % 2])
                    if k < span - 1:
                        dots(b + k + 1, i, *sets[(k + 1) % 2])
                    else:
                        dots(lax.rem(b + span, BLOCKS), after, *sets[0])

            @pl.when(n == BLOCKS // span // 2 - 1)
            def _():
                events(i, EARLY)

        du_out(i).start()
        events(i, MIDDLE)

        @pl.when(i == chunks - 1)
        def _():
            du_first().start()

        slot = lax.rem(i, HELD)
        with jax.named_scope("dw"):
            @pl.loop(0, cuts)
            def _(n):
                n2, n1 = CHUNK // cuts, d_model // cuts
                at2, at1 = pl.ds(pl.multiple_of(n * n2, n2), n2), pl.ds(pl.multiple_of(n * n1, n1), n1)
                p2[slot, at2, :] = lax.dot_general(a_v[:, at2], g_v[:packed, :], TN, preferred_element_type=f32).astype(bf16)
                p1[slot, at1, :] = lax.dot_general(x_v[:packed, at1], du_v[...], TN, preferred_element_type=f32).astype(bf16)

        events(i, LATE)

    @pl.loop(0, max(TAIL, dx_blocks))
    def _(q):
        @pl.when(q < dx_blocks)
        def _():
            slot = lax.rem(q, 2)

            @pl.when(q == 0)
            def _():
                du_out(chunks - 1).wait()
                du_first().wait()
                dub_v[0, :, pl.ds((chunks - 1) * CHUNK, CHUNK)] = du_v[dx_rows(0), :]

            @pl.when(q + 1 < dx_blocks)
            def _():
                du_in(q + 1).start()

            @pl.when(q > 0)
            def _():
                du_in(q).wait()

            @pl.when(q > 1)
            def _():
                dx_out(q - 2).wait()

            with jax.named_scope("dx"):
                dx_v[slot] = (g_v[dx_rows(q), :].astype(f32) + lax.dot_general(dub_v[slot], w1_v[...], NT, preferred_element_type=f32)).astype(bf16)
            dx_out(q).start()

        for e in (1, *reversed(range(2, TAIL + 1))):
            lag = sum(jnp.where(q == step, behind, 0) for behind, step in TAIL_STEPS[e])
            j = chunks - 1 - lag

            @pl.when(functools.reduce(jnp.logical_or, [q == step for _, step in TAIL_STEPS[e]]) & (j >= 0))
            def _():
                with jax.named_scope(f"event{e}"):
                    event(e, j)

    dx_out(dx_blocks - 2).wait()
    dx_out(dx_blocks - 1).wait()


def grads_call(dims, ident, table, x, dy, w1, w2):
    tokens, d_model, d_ff, seq, packed, dx_block = dims
    scratch = [
        pltpu.VMEM((tokens, d_model), bf16), pltpu.VMEM((tokens, d_model), bf16),
        pltpu.VMEM((d_model, d_ff), bf16), pltpu.VMEM((2, CHUNK, d_model), bf16),
        pltpu.VMEM((packed // BLOCKS, CHUNK), bf16), pltpu.VMEM((packed // BLOCKS, CHUNK), bf16),
        pltpu.VMEM((packed // BLOCKS, CHUNK), f32), pltpu.VMEM((packed // BLOCKS, CHUNK), f32),
        pltpu.VMEM((packed, CHUNK), bf16), pltpu.VMEM((packed, CHUNK), bf16),
        pltpu.VMEM((HELD, d_model, CHUNK), bf16), pltpu.VMEM((HELD, CHUNK, d_model), bf16),
        pltpu.VMEM((2, dx_block, d_ff), bf16), pltpu.VMEM((2, dx_block, d_model), bf16),
    ]
    for (_, _, rows, _, cols, _) in part_table(d_model):
        for s in range(STAGES):
            last = s == STAGES - 1
            scratch.append(pltpu.VMEM((2, rows >> (4 if last else s + 1), cols // 2 if last else cols), bf16))
    dma = pltpu.SemaphoreType.DMA
    scratch += [dma((tokens // seq,)), dma((tokens // seq,)), dma((2, 2)), dma, dma((4,)), dma((2,)), dma((2,))]
    scratch += [dma((2, STAGES, 4))] * 4
    return pl.pallas_call(
        functools.partial(grads_kernel, dims),
        out_shape=[jax.ShapeDtypeStruct((d_model, d_ff), bf16), jax.ShapeDtypeStruct((d_ff, d_model), bf16),
                   jax.ShapeDtypeStruct((tokens, d_ff), bf16), jax.ShapeDtypeStruct((tokens + seq, d_model), bf16)],
        in_specs=[SMEM] + [ANY] * 4,
        out_specs=[ANY] * 4,
        scratch_shapes=scratch,
        compiler_params=pltpu.CompilerParams(collective_id=ident, has_side_effects=True, vmem_limit_bytes=62 * 2**20),
        cost_estimate=pl.CostEstimate(flops=10 * packed * d_model * d_ff, bytes_accessed=4 * packed * d_ff, transcendentals=packed * d_ff),
        name=f"grads{packed}",
    )(table, x, dy, w1, w2)


def finish_kernel(dims, len_ref, o1_hbm, o2_hbm, dxp_hbm, g1_hbm, g2_hbm, dx_hbm, c1_v, c2_v, dx_v, starts, c_in, c_out, dx_in, dx_out):
    tokens, d_model, d_ff, seq = dims
    seqs = tokens // seq
    steps, slots, ahead = 4 * seqs, 12, 6
    n1, n2 = d_model // steps, d_ff // steps

    def rows(b, n):
        return pl.ds(pl.multiple_of(b * n, 8), n)

    def carry_in(b):
        slot = lax.rem(b, slots)
        return (pltpu.make_async_copy(o1_hbm.at[rows(b, n1), :], c1_v.at[slot], c_in.at[slot, 0]),
                pltpu.make_async_copy(o2_hbm.at[rows(b, n2), :], c2_v.at[slot], c_in.at[slot, 1]))

    def carry_out(b):
        slot = lax.rem(b, slots)
        return (pltpu.make_async_copy(c1_v.at[slot], g1_hbm.at[rows(b, n1), :], c_out.at[slot, 0]),
                pltpu.make_async_copy(c2_v.at[slot], g2_hbm.at[rows(b, n2), :], c_out.at[slot, 1]))

    starts[0] = jnp.int32(0)
    for s in range(1, seqs):
        starts[s] = starts[s - 1] + granules(len_ref, s - 1)

    def unpack_in(s, act):
        slot, half = lax.rem(s, 4), seq // 2
        for n in range(2):
            at = pl.ds(pl.multiple_of(starts[s] * GRANULE, GRANULE) + n * half, half)

            @pl.when(length(len_ref, s) > n * half)
            def _():
                act(pltpu.make_async_copy(dxp_hbm.at[at, :], dx_v.at[slot, pl.ds(n * half, half), :], dx_in.at[slot, n]))

    def unpack_out(s):
        slot = lax.rem(s, 4)
        return pltpu.make_async_copy(dx_v.at[slot], dx_hbm.at[rows(s, seq), :], dx_out.at[slot])

    for b in range(ahead):
        for copy in carry_in(b):
            copy.start()
    for s in range(2):
        unpack_in(s, lambda copy: copy.start())

    @pl.loop(0, steps)
    def _(b):
        with jax.named_scope("carry_in_wait"):
            for copy in carry_in(b):
                copy.wait()
        for copy in carry_out(b):
            copy.start()

        @pl.when(b >= ahead)
        def _():
            for copy in carry_out(b - ahead):
                copy.wait()

        @pl.when(b + ahead < steps)
        def _():
            for copy in carry_in(b + ahead):
                copy.start()

        s = lax.div(b, 4)

        @pl.when(lax.rem(b, 4) == 3)
        def _():
            unpack_in(s, lambda copy: copy.wait())
            slot = lax.rem(s, 4)
            keep = lax.broadcasted_iota(jnp.int32, (seq, d_model), 0) < length(len_ref, s)
            dx_v[slot] = jnp.where(keep, dx_v[slot], jnp.zeros((), bf16))
            unpack_out(s).start()

            @pl.when(s >= 2)
            def _():
                unpack_out(s - 2).wait()

            @pl.when(s + 2 < seqs)
            def _():
                unpack_in(s + 2, lambda copy: copy.start())

    for b in range(steps - ahead, steps):
        for copy in carry_out(b):
            copy.wait()
    for s in (seqs - 2, seqs - 1):
        unpack_out(s).wait()


def finish_call(dims, lens, o1, o2, dxp):
    tokens, d_model, d_ff, seq = dims
    steps = 4 * (tokens // seq)
    dma = pltpu.SemaphoreType.DMA
    return pl.pallas_call(
        functools.partial(finish_kernel, dims),
        out_shape=[jax.ShapeDtypeStruct((d_model, d_ff), bf16), jax.ShapeDtypeStruct((d_ff, d_model), bf16),
                   jax.ShapeDtypeStruct((tokens, d_model), bf16)],
        in_specs=[SMEM] + [ANY] * 3,
        out_specs=[ANY] * 3,
        scratch_shapes=[
            pltpu.VMEM((12, d_model // steps, d_ff), bf16), pltpu.VMEM((12, d_ff // steps, d_model), bf16), pltpu.VMEM((4, seq, d_model), bf16),
            pltpu.SMEM((tokens // seq,), jnp.int32), dma((12, 2)), dma((12, 2)), dma((4, 2)), dma((4,))],
        compiler_params=pltpu.CompilerParams(vmem_limit_bytes=63 * 2**20),
        cost_estimate=pl.CostEstimate(flops=tokens * d_model, bytes_accessed=8 * d_model * d_ff, transcendentals=0),
        name="finish",
    )(lens, o1, o2, dxp)


def solution(mesh):
    def local_step(x_loc, dy_loc, len_loc, w_in, w_out):
        layers, d_model, d_ff = w_in.shape
        rows, seq, _ = x_loc.shape
        tokens = rows * seq
        lens = len_loc.T
        x, dy = x_loc.reshape(tokens, d_model), dy_loc.reshape(tokens, d_model)
        w1, w2 = w_in.reshape(d_model, d_ff), w_out.reshape(d_ff, d_model)
        sizes = tuple(tokens * n // 16 for n in (12, 13, 16))

        def branch(n):
            def run(table, x, dy, w1, w2):
                return grads_call((tokens, d_model, d_ff, seq, sizes[n], tokens // 16), n + 1, table, x, dy, w1, w2)

            return run

        size, table = most_call(lens, seq, sizes)
        o1, o2, _, dxp = lax.switch(size[0, 0], [branch(n) for n in range(len(sizes))], table, x, dy, w1, w2)
        g1, g2, dx = finish_call((tokens, d_model, d_ff, seq), lens, o1, o2, dxp)
        return g1.reshape(layers, d_model, d_ff), g2.reshape(layers, d_ff, d_model), dx.reshape(rows, seq, d_model)

    return jax.shard_map(local_step, mesh=mesh, in_specs=(P("data"), P("data"), P("data"), P(), P()), out_specs=(P(), P(), P("data")), check_vma=False)
```

```python
import functools
import math
import jax
import jax.numpy as jnp
from jax import lax
from jax.experimental import pallas as pl
from jax.experimental.pallas import tpu as pltpu
from jax.sharding import PartitionSpec as P

GELU_SCALE = math.sqrt(2.0 / math.pi)
GELU_CUBIC = 0.044715
MESH = pl.DeviceIdType.MESH
NT = (((1,), (1,)), ((), ()))
TN = (((0,), (0,)), ((), ()))
f32 = jnp.float32
bf16 = jnp.bfloat16
ANY = pl.BlockSpec(memory_space=pl.ANY)
SMEM = pl.BlockSpec(memory_space=pltpu.SMEM)

CHUNK = 256
GRANULE = 16
BLOCKS = 8
STAGES = 5
WEIGHT = {"c": 1, "x": 2, "y": 4, "z": 8, "w": 16}
EARLY = ((1, 1), (9, 6))
MIDDLE = ((3, 2), (5, 3), (8, 5), (7, 4), (10, 6))
LATE = ((0, 0), (2, 1), (4, 2), (6, 3))
TAIL = 2 * STAGES
TAIL_STEPS = {e: tuple((lag, step) for lag, seen in enumerate((
    {n: n - 1 for n in range(1, 11)}, {n: n - 2 for n in range(3, 11)}, {n: n - 4 for n in range(5, 11)},
    {n: n - 6 for n in range(7, 11)}, {8: 0, 9: 2, 10: 3}, {9: 0, 10: 1})) for n, step in seen.items() if n == e) for e in range(1, TAIL + 1)}
WEIGHT = {"c": 1, "x": 2, "y": 4, "z": 8, "w": 16}
EARLY = ((1, 1), (9, 6))
MIDDLE = ((3, 2), (5, 3), (8, 5), (7, 4), (10, 6))
LATE = ((0, 0), (2, 1), (4, 2), (6, 3))
TAIL = 2 * STAGES
HELD = 4


def gelu_both(u):
    sq = u * u
    half = 0.5 + 0.5 * jnp.tanh(u * (GELU_SCALE + (GELU_SCALE * GELU_CUBIC) * sq))
    value = u * half
    return value, half + (value * (1.0 - half)) * (2.0 * GELU_SCALE + (6.0 * GELU_SCALE * GELU_CUBIC) * sq)


def part_table(d_model):
    rows = 1024 if d_model == 1280 else d_model // 2
    cols = 768 if d_model == 1280 else d_model // 2
    return (
        (0, 0, rows, 0, CHUNK, "cxyzw"),
        (0, rows, d_model - rows, 0, CHUNK, "czxyw"),
        (1, 0, CHUNK, 0, cols, "cyxzw"),
        (1, 0, CHUNK, cols, d_model - cols, "czyxw"),
    )


def place():
    me = lax.axis_index("data")
    bit = {k: lax.rem(lax.div(me, v), 2) for k, v in WEIGHT.items()}
    return me, bit, {k: me + v * (1 - 2 * bit[k]) for k, v in WEIGHT.items()}


def granules(len_ref, s):
    return lax.div(length(len_ref, s) + (GRANULE - 1), GRANULE)


def length(len_ref, s):
    return len_ref[lax.rem(s, 2), lax.div(s, 2)]


def most_kernel(seqs, seq, sizes, len_ref, out_ref, table_ref, mine, plane, best, depth, send, recv):
    me, bit, _ = place()

    def other(d, names):
        return me + sum(WEIGHT[k] * (1 - 2 * bit[k]) for n, k in enumerate(names) if d >> n & 1)

    counts = [granules(len_ref, s) for s in range(seqs)]
    starts = [sum(counts[:s], jnp.int32(0)) for s in range(seqs + 1)]
    mine[...] = jnp.full(mine.shape, (starts[seqs] * GRANULE).astype(f32))
    barrier = pltpu.get_barrier_semaphore()
    near = [other(d, "cxy") for d in range(1, 8)]
    far = [other(d, "zw") for d in range(1, 4)]
    for device in near + far:
        pl.semaphore_signal(barrier, inc=1, device_id=(device,), device_id_type=MESH)
    pl.semaphore_wait(barrier, len(near) + len(far))

    def exchange(source, slots, devices, first):
        copies = [pltpu.make_async_remote_copy(source, slots.at[n], send.at[first + n], recv.at[first + n], device_id=(device,), device_id_type=MESH)
                  for n, device in enumerate(devices)]
        for copy in copies:
            copy.start()
        return copies

    def largest_of(copies, source, slots):
        for copy in copies:
            copy.wait()
        return functools.reduce(jnp.maximum, [slots[n] for n in range(len(copies))], source[...])

    first = exchange(mine, plane, near, 0)
    k = lax.broadcasted_iota(jnp.int32, (2, 128), 0) * 128 + lax.broadcasted_iota(jnp.int32, (2, 128), 1)
    source, left = k, length(len_ref, 0) - k * GRANULE
    for s in range(1, seqs):
        past = k >= starts[s]
        source = jnp.where(past, k - starts[s] + s * (seq // GRANULE), source)
        left = jnp.where(past, length(len_ref, s) - (k - starts[s]) * GRANULE, left)
    inside = k < starts[seqs]
    table_ref[0:2, :] = jnp.where(inside, source, 0)
    table_ref[2:4, :] = jnp.where(inside, left, 0)
    best[...] = largest_of(first, mine, plane)
    largest = largest_of(exchange(best, depth, far, len(near)), best, depth)
    out_ref[0, 0] = jnp.max(sum((largest > size).astype(jnp.int32) for size in sizes[:-1]))


def most_call(lens, seq, sizes):
    tile = (8, 128)
    dma = pltpu.SemaphoreType.DMA
    return pl.pallas_call(
        functools.partial(most_kernel, lens.size, seq, sizes),
        out_shape=[jax.ShapeDtypeStruct((1, 1), jnp.int32), jax.ShapeDtypeStruct((4, 128), jnp.int32)],
        in_specs=[SMEM],
        out_specs=[SMEM, pl.BlockSpec(memory_space=pltpu.VMEM)],
        scratch_shapes=[pltpu.VMEM(tile, f32), pltpu.VMEM((7, *tile), f32), pltpu.VMEM(tile, f32), pltpu.VMEM((3, *tile), f32), dma((10,)), dma((10,))],
        compiler_params=pltpu.CompilerParams(collective_id=0, has_side_effects=True),
        name="most",
    )(lens)


def grads_kernel(dims, table_ref, x_hbm, dy_hbm, w1_hbm, w2_hbm, o1_hbm, o2_hbm, du_hbm, dx_hbm, *scratch):
    tokens, d_model, d_ff, seq, packed, dx_block = dims
    seqs = tokens // seq
    chunks = d_ff // CHUNK
    block = packed // BLOCKS
    dx_blocks = packed // dx_block
    span = BLOCKS // 2 if packed < tokens else 2
    cuts = 1 if packed < tokens else 2
    parts = part_table(d_model)
    (x_v, g_v, w1_v, w2_v, u0, u1, d0, d1, a_v, du_v, p1, p2, dub_v, dx_v) = scratch[:14]
    recv = [scratch[14 + 5 * k : 19 + 5 * k] for k in range(4)]
    (x_sem, g_sem, w_sem, du_sem, own_sem, dub_sem, dx_sem, rs_send, rs_recv, ag_send, ag_recv) = scratch[34:]

    _, bit, peer = place()
    for s in range(seqs):
        at = pl.ds(s * seq, seq)
        pltpu.make_async_copy(x_hbm.at[at, :], x_v.at[at, :], x_sem.at[s]).start()

    barrier = pltpu.get_barrier_semaphore()
    for k in WEIGHT:
        pl.semaphore_signal(barrier, inc=1, device_id=(peer[k],), device_id_type=MESH)
    for s in range(seqs):
        at = pl.ds(s * seq, seq)
        pltpu.make_async_copy(dy_hbm.at[at, :], g_v.at[at, :], g_sem.at[s]).start()
    pl.semaphore_wait(barrier, STAGES)

    region, given = [], []
    for (_, r0, nr, c0, nc, order) in parts:
        mine, away = [(r0, nr, c0, nc)], []
        for s, name in enumerate(order):
            row, rows, col, cols = mine[-1]
            if s < STAGES - 1:
                half = rows // 2
                mine.append((row + bit[name] * half, half, col, cols))
                away.append((row + (1 - bit[name]) * half, half, col, cols))
            else:
                half = cols // 2
                mine.append((row, rows, col + bit[name] * half, half))
                away.append((row, rows, col + (1 - bit[name]) * half, half))
        region.append(mine)
        given.append(away)

    def cut(r):
        row, rows, col, cols = r
        row = row if isinstance(row, int) else pl.multiple_of(row, 16)
        col = col if isinstance(col, int) else pl.multiple_of(col, 128)
        return pl.ds(row, rows), pl.ds(col, cols)

    def partial(k, i, r):
        rows, cols = cut(r)
        return (p1, p2)[parts[k][0]].at[lax.rem(i, HELD), rows, cols]

    def whole(k, i, r):
        row, rows, col, cols = r
        if parts[k][0] == 0:
            return o1_hbm.at[cut((row, rows, i * CHUNK + col, cols))]
        return o2_hbm.at[cut((i * CHUNK + row, rows, col, cols))]

    def reduce_copy(k, s, i):
        slot = lax.rem(i, 2)
        return pltpu.make_async_remote_copy(
            src_ref=partial(k, i, given[k][s]), dst_ref=recv[k][s].at[slot],
            send_sem=rs_send.at[slot, s, k], recv_sem=rs_recv.at[slot, s, k],
            device_id=(peer[parts[k][5][s]],), device_id_type=MESH)

    def gather_copy(k, s, i):
        slot = lax.rem(i, 2)
        r = region[k][s + 1]
        return pltpu.make_async_remote_copy(
            src_ref=partial(k, i, r) if s == STAGES - 1 else whole(k, i, r), dst_ref=whole(k, i, r),
            send_sem=ag_send.at[slot, s, k], recv_sem=ag_recv.at[slot, s, k],
            device_id=(peer[parts[k][5][s]],), device_id_type=MESH)

    def own_copy(k, i):
        r = region[k][STAGES]
        return pltpu.make_async_copy(partial(k, i, r), whole(k, i, r), own_sem.at[k])

    def event(e, i):
        for k in range(4):
            if 1 <= e <= STAGES:
                reduce_copy(k, e - 1, i).wait()
                rows, cols = cut(region[k][e])
                ref, slot = (p1, p2)[parts[k][0]], lax.rem(i, HELD)
                ref[slot, rows, cols] = ref[slot, rows, cols] + recv[k][e - 1][lax.rem(i, 2)]
            if e < STAGES:
                reduce_copy(k, e, i).start()
            if e == STAGES:
                own_copy(k, i).start()
            if e > STAGES:
                gather_copy(k, 2 * STAGES - e, i).wait()
                if e == STAGES + 1:
                    own_copy(k, i).wait()
            if STAGES <= e < 2 * STAGES:
                gather_copy(k, 2 * STAGES - 1 - e, i).start()

    def weights(i):
        slot = lax.rem(i, 2)
        at = pl.ds(pl.multiple_of(i * CHUNK, CHUNK), CHUNK)
        return (pltpu.make_async_copy(w1_hbm.at[:, at], w1_v.at[:, at], w_sem.at[slot, 0]),
                pltpu.make_async_copy(w2_hbm.at[at, :], w2_v.at[slot], w_sem.at[slot, 1]))

    def rows_of(b):
        return pl.ds(pl.multiple_of(b * block, 16), block)

    def dots(b, i, u, d):
        w1 = w1_v[:, pl.ds(pl.multiple_of(i * CHUNK, CHUNK), CHUNK)]
        u[...] = jnp.dot(x_v[rows_of(b), :], w1, preferred_element_type=f32).astype(bf16)
        d[...] = lax.dot_general(g_v[rows_of(b), :], w2_v[lax.rem(i, 2)], NT, preferred_element_type=f32)

    def pointwise(b, u, d):
        a, slope = gelu_both(u[...].astype(f32))
        a_v[rows_of(b), :] = a.astype(bf16)
        du_v[rows_of(b), :] = (d[...] * slope).astype(bf16)

    def du_out(i):
        return pltpu.make_async_copy(du_v, du_hbm.at[pl.ds(0, packed), pl.ds(pl.multiple_of(i * CHUNK, CHUNK), CHUNK)], du_sem)

    def dx_rows(q):
        return pl.ds(pl.multiple_of(q * dx_block, 16), dx_block)

    def du_in(q):
        slot = lax.rem(q, 2)
        return pltpu.make_async_copy(du_hbm.at[dx_rows(q), :], dub_v.at[slot], dub_sem.at[slot])

    def du_first():
        ready = pl.ds(0, (chunks - 1) * CHUNK)
        return pltpu.make_async_copy(du_hbm.at[dx_rows(0), ready], dub_v.at[0, :, ready], dub_sem.at[0])

    def dx_out(q):
        slot = lax.rem(q, 2)
        return pltpu.make_async_copy(dx_v.at[slot], dx_hbm.at[dx_rows(q), :], dx_sem.at[slot])

    for copy in weights(0):
        copy.start()

    with jax.named_scope("wait_x"):
        for s in range(seqs):
            at = pl.ds(s * seq, seq)
            pltpu.make_async_copy(x_hbm.at[at, :], x_v.at[at, :], x_sem.at[s]).wait()

    group = 4 if packed % (4 * GRANULE) == 0 else 2

    def granule_rows(k):
        return pl.ds(pl.multiple_of(k * GRANULE, GRANULE), GRANULE)

    def source_rows(k):
        return pl.ds(table_ref[lax.div(k, 128), lax.rem(k, 128)] * GRANULE, GRANULE)

    @pl.loop(0, packed // GRANULE // group)
    def _(n):
        rows = [x_v[source_rows(n * group + k), :] for k in range(group)]
        for k in range(group):
            x_v[granule_rows(n * group + k), :] = rows[k]

    with jax.named_scope("wait_g"):
        for s in range(seqs):
            at = pl.ds(s * seq, seq)
            pltpu.make_async_copy(dy_hbm.at[at, :], g_v.at[at, :], g_sem.at[s]).wait()

    @pl.loop(0, packed // GRANULE // group)
    def _(n):
        rows = [g_v[source_rows(n * group + k), :] for k in range(group)]
        for k in range(group):
            at = n * group + k
            keep = lax.broadcasted_iota(jnp.int32, (GRANULE, d_model), 0) < table_ref[2 + lax.div(at, 128), lax.rem(at, 128)]
            g_v[granule_rows(at), :] = jnp.where(keep, rows[k], jnp.zeros((), bf16))

    with jax.named_scope("wait_w"):
        for copy in weights(0):
            copy.wait()

    @pl.loop(0, 2)
    def _(n):
        at = pl.ds(pl.multiple_of(n * (block // 2), 16), block // 2)
        u0[at, :] = jnp.dot(x_v[at, :], w1_v[:, 0:CHUNK], preferred_element_type=f32).astype(bf16)
        d0[at, :] = lax.dot_general(g_v[at, :], w2_v[0], NT, preferred_element_type=f32)


    def events(i, which):
        for e, lag in which:
            j = i - lag

            @pl.when((j >= 0) & (j < chunks))
            def _():
                with jax.named_scope(f"event{e}"):
                    event(e, j)

    @pl.loop(0, chunks)
    def _(i):
        @pl.when(i + 1 < chunks)
        def _():
            for copy in weights(i + 1):
                copy.start()

        @pl.when(i > 0)
        def _():
            du_out(i - 1).wait()

        @pl.loop(0, BLOCKS // span)
        def _(n):
            last = n == BLOCKS // span - 1

            @pl.when(last & (i + 1 < chunks))
            def _():
                for copy in weights(i + 1):
                    copy.wait()

            b = n * span
            after = jnp.minimum(i + last.astype(jnp.int32), chunks - 1)
            sets = ((u0, d0), (u1, d1))
            with jax.named_scope("tokens"):
                for k in range(span):
                    pointwise(b + k, *sets[k % 2])
                    if k < span - 1:
                        dots(b + k + 1, i, *sets[(k + 1) % 2])
                    else:
                        dots(lax.rem(b + span, BLOCKS), after, *sets[0])

            @pl.when(n == BLOCKS // span // 2 - 1)
            def _():
                events(i, EARLY)

        du_out(i).start()
        events(i, MIDDLE)

        @pl.when(i == chunks - 1)
        def _():
            du_first().start()

        slot = lax.rem(i, HELD)
        with jax.named_scope("dw"):
            @pl.loop(0, cuts)
            def _(n):
                n2, n1 = CHUNK // cuts, d_model // cuts
                at2, at1 = pl.ds(pl.multiple_of(n * n2, n2), n2), pl.ds(pl.multiple_of(n * n1, n1), n1)
                p2[slot, at2, :] = lax.dot_general(a_v[:, at2], g_v[:packed, :], TN, preferred_element_type=f32).astype(bf16)
                p1[slot, at1, :] = lax.dot_general(x_v[:packed, at1], du_v[...], TN, preferred_element_type=f32).astype(bf16)

        events(i, LATE)

    @pl.loop(0, max(TAIL, dx_blocks))
    def _(q):
        @pl.when(q < dx_blocks)
        def _():
            slot = lax.rem(q, 2)

            @pl.when(q == 0)
            def _():
                du_out(chunks - 1).wait()
                du_first().wait()
                dub_v[0, :, pl.ds((chunks - 1) * CHUNK, CHUNK)] = du_v[dx_rows(0), :]

            @pl.when(q + 1 < dx_blocks)
            def _():
                du_in(q + 1).start()

            @pl.when(q > 0)
            def _():
                du_in(q).wait()

            @pl.when(q > 1)
            def _():
                dx_out(q - 2).wait()

            with jax.named_scope("dx"):
                dx_v[slot] = (g_v[dx_rows(q), :].astype(f32) + lax.dot_general(dub_v[slot], w1_v[...], NT, preferred_element_type=f32)).astype(bf16)
            dx_out(q).start()

        for e in (1, *reversed(range(2, TAIL + 1))):
            lag = sum(jnp.where(q == step, behind, 0) for behind, step in TAIL_STEPS[e])
            j = chunks - 1 - lag

            @pl.when(functools.reduce(jnp.logical_or, [q == step for _, step in TAIL_STEPS[e]]) & (j >= 0))
            def _():
                with jax.named_scope(f"event{e}"):
                    event(e, j)

    dx_out(dx_blocks - 2).wait()
    dx_out(dx_blocks - 1).wait()


def grads_call(dims, ident, table, x, dy, w1, w2):
    tokens, d_model, d_ff, seq, packed, dx_block = dims
    scratch = [
        pltpu.VMEM((tokens, d_model), bf16), pltpu.VMEM((tokens, d_model), bf16),
        pltpu.VMEM((d_model, d_ff), bf16), pltpu.VMEM((2, CHUNK, d_model), bf16),
        pltpu.VMEM((packed // BLOCKS, CHUNK), bf16), pltpu.VMEM((packed // BLOCKS, CHUNK), bf16),
        pltpu.VMEM((packed // BLOCKS, CHUNK), f32), pltpu.VMEM((packed // BLOCKS, CHUNK), f32),
        pltpu.VMEM((packed, CHUNK), bf16), pltpu.VMEM((packed, CHUNK), bf16),
        pltpu.VMEM((HELD, d_model, CHUNK), bf16), pltpu.VMEM((HELD, CHUNK, d_model), bf16),
        pltpu.VMEM((2, dx_block, d_ff), bf16), pltpu.VMEM((2, dx_block, d_model), bf16),
    ]
    for (_, _, rows, _, cols, _) in part_table(d_model):
        for s in range(STAGES):
            last = s == STAGES - 1
            scratch.append(pltpu.VMEM((2, rows >> (4 if last else s + 1), cols // 2 if last else cols), bf16))
    dma = pltpu.SemaphoreType.DMA
    scratch += [dma((tokens // seq,)), dma((tokens // seq,)), dma((2, 2)), dma, dma((4,)), dma((2,)), dma((2,))]
    scratch += [dma((2, STAGES, 4))] * 4
    return pl.pallas_call(
        functools.partial(grads_kernel, dims),
        out_shape=[jax.ShapeDtypeStruct((d_model, d_ff), bf16), jax.ShapeDtypeStruct((d_ff, d_model), bf16),
                   jax.ShapeDtypeStruct((tokens, d_ff), bf16), jax.ShapeDtypeStruct((tokens + seq, d_model), bf16)],
        in_specs=[SMEM] + [ANY] * 4,
        out_specs=[ANY] * 4,
        scratch_shapes=scratch,
        compiler_params=pltpu.CompilerParams(collective_id=ident, has_side_effects=True, vmem_limit_bytes=62 * 2**20),
        cost_estimate=pl.CostEstimate(flops=10 * packed * d_model * d_ff, bytes_accessed=4 * packed * d_ff, transcendentals=packed * d_ff),
        name=f"grads{packed}",
    )(table, x, dy, w1, w2)


def finish_kernel(dims, len_ref, o1_hbm, o2_hbm, dxp_hbm, g1_hbm, g2_hbm, dx_hbm, c1_v, c2_v, dx_v, starts, c_in, c_out, dx_in, dx_out):
    tokens, d_model, d_ff, seq = dims
    seqs = tokens // seq
    steps, slots, ahead = 2 * seqs, 6, 3
    n1, n2 = d_model // steps, d_ff // steps

    def rows(b, n):
        return pl.ds(pl.multiple_of(b * n, 8), n)

    def carry_in(b):
        slot = lax.rem(b, slots)
        return (pltpu.make_async_copy(o1_hbm.at[rows(b, n1), :], c1_v.at[slot], c_in.at[slot, 0]),
                pltpu.make_async_copy(o2_hbm.at[rows(b, n2), :], c2_v.at[slot], c_in.at[slot, 1]))

    def carry_out(b):
        slot = lax.rem(b, slots)
        return (pltpu.make_async_copy(c1_v.at[slot], g1_hbm.at[rows(b, n1), :], c_out.at[slot, 0]),
                pltpu.make_async_copy(c2_v.at[slot], g2_hbm.at[rows(b, n2), :], c_out.at[slot, 1]))

    starts[0] = jnp.int32(0)
    for s in range(1, seqs):
        starts[s] = starts[s - 1] + granules(len_ref, s - 1)

    def unpack_in(s, act):
        slot, half = lax.rem(s, 4), seq // 2
        for n in range(2):
            at = pl.ds(pl.multiple_of(starts[s] * GRANULE, GRANULE) + n * half, half)

            @pl.when(length(len_ref, s) > n * half)
            def _():
                act(pltpu.make_async_copy(dxp_hbm.at[at, :], dx_v.at[slot, pl.ds(n * half, half), :], dx_in.at[slot, n]))

    def unpack_out(s):
        slot = lax.rem(s, 4)
        return pltpu.make_async_copy(dx_v.at[slot], dx_hbm.at[rows(s, seq), :], dx_out.at[slot])

    for b in range(ahead):
        for copy in carry_in(b):
            copy.start()
    for s in range(2):
        unpack_in(s, lambda copy: copy.start())

    @pl.loop(0, steps)
    def _(b):
        with jax.named_scope("carry_in_wait"):
            for copy in carry_in(b):
                copy.wait()
        for copy in carry_out(b):
            copy.start()

        @pl.when(b >= ahead)
        def _():
            for copy in carry_out(b - ahead):
                copy.wait()

        @pl.when(b + ahead < steps)
        def _():
            for copy in carry_in(b + ahead):
                copy.start()

        s = lax.div(b, 2)

        @pl.when(lax.rem(b, 2) == 1)
        def _():
            unpack_in(s, lambda copy: copy.wait())
            slot = lax.rem(s, 4)
            keep = lax.broadcasted_iota(jnp.int32, (seq, d_model), 0) < length(len_ref, s)
            dx_v[slot] = jnp.where(keep, dx_v[slot], jnp.zeros((), bf16))
            unpack_out(s).start()

            @pl.when(s >= 2)
            def _():
                unpack_out(s - 2).wait()

            @pl.when(s + 2 < seqs)
            def _():
                unpack_in(s + 2, lambda copy: copy.start())

    for b in range(steps - ahead, steps):
        for copy in carry_out(b):
            copy.wait()
    for s in (seqs - 2, seqs - 1):
        unpack_out(s).wait()


def finish_call(dims, lens, o1, o2, dxp):
    tokens, d_model, d_ff, seq = dims
    steps = 2 * (tokens // seq)
    dma = pltpu.SemaphoreType.DMA
    return pl.pallas_call(
        functools.partial(finish_kernel, dims),
        out_shape=[jax.ShapeDtypeStruct((d_model, d_ff), bf16), jax.ShapeDtypeStruct((d_ff, d_model), bf16),
                   jax.ShapeDtypeStruct((tokens, d_model), bf16)],
        in_specs=[SMEM] + [ANY] * 3,
        out_specs=[ANY] * 3,
        scratch_shapes=[
            pltpu.VMEM((6, d_model // steps, d_ff), bf16), pltpu.VMEM((6, d_ff // steps, d_model), bf16), pltpu.VMEM((4, seq, d_model), bf16),
            pltpu.SMEM((tokens // seq,), jnp.int32), dma((6, 2)), dma((6, 2)), dma((4, 2)), dma((4,))],
        compiler_params=pltpu.CompilerParams(vmem_limit_bytes=63 * 2**20),
        cost_estimate=pl.CostEstimate(flops=tokens * d_model, bytes_accessed=8 * d_model * d_ff, transcendentals=0),
        name="finish",
    )(lens, o1, o2, dxp)


def solution(mesh):
    def local_step(x_loc, dy_loc, len_loc, w_in, w_out):
        layers, d_model, d_ff = w_in.shape
        rows, seq, _ = x_loc.shape
        tokens = rows * seq
        lens = len_loc.T
        x, dy = x_loc.reshape(tokens, d_model), dy_loc.reshape(tokens, d_model)
        w1, w2 = w_in.reshape(d_model, d_ff), w_out.reshape(d_ff, d_model)
        sizes = tuple(tokens * n // 16 for n in (12, 13, 16))

        def branch(n):
            def run(table, x, dy, w1, w2):
                return grads_call((tokens, d_model, d_ff, seq, sizes[n], tokens // 16), n + 1, table, x, dy, w1, w2)

            return run

        size, table = most_call(lens, seq, sizes)
        o1, o2, _, dxp = lax.switch(size[0, 0], [branch(n) for n in range(len(sizes))], table, x, dy, w1, w2)
        g1, g2, dx = finish_call((tokens, d_model, d_ff, seq), lens, o1, o2, dxp)
        return g1.reshape(layers, d_model, d_ff), g2.reshape(layers, d_ff, d_model), dx.reshape(rows, seq, d_model)

    return jax.shard_map(local_step, mesh=mesh, in_specs=(P("data"), P("data"), P("data"), P(), P()), out_specs=(P(), P(), P("data")), check_vma=False)
```
